32 devices in a mesh: dp: 1 (over z), cy: 4 (over y), cx: 4 (over x), core: 2 (over core).
Axes of the slice: x: 4, y: 4, z: 1, core: 2. Of those that a mesh axis runs over, the one named last changes fastest.
The devices are a block of a 4x4x8 slice.
Arguments:
- x_in: bfloat16 [1, 3072, 2048], P('dp', ('cy', 'cx', 'core'))
- w_qkv: bfloat16 [2048, 48, 64], replicated
- w_out: bfloat16 [32, 64, 2048], replicated
Outputs:
- output: bfloat16 [1, 3072, 2048], P('dp', ('cy', 'cx', 'core'))
All inputs are finite; a program needn't handle non-finite values.
Results may differ from the reference program's by a relative error of at most 0.00796281.
Values are sent between devices in bfloat16 or wider.
A program may use at most 768 MiB of HBM per device.

```python
import math
import jax
import jax.numpy as jnp
from jax import lax

TOKENS_DEV = 96
GROUP_DEVICES = 32
HEADS = 32
KV_HEADS = 8
HEAD_DIM = 64

TOKENS = TOKENS_DEV * GROUP_DEVICES
WIDTH = HEADS * HEAD_DIM
GROUP_SIZE = HEADS // KV_HEADS
QUERY_GAIN = 2.0
OUT_GAIN = math.sqrt(TOKENS) * math.exp(-0.5 * QUERY_GAIN ** 2)


def setup_inputs(seed: int = 0, part: int = 0) -> dict:
    root_key = jax.random.key(seed)
    key_act = jax.random.fold_in(jax.random.fold_in(root_key, 1), part)
    key_qkv = jax.random.fold_in(root_key, 2)
    key_out = jax.random.fold_in(root_key, 3)
    act_rows = jax.random.normal(key_act, (1, TOKENS, WIDTH), jnp.float32)
    head_gain = jnp.concatenate([jnp.full((HEADS,), QUERY_GAIN, jnp.float32), jnp.ones((2 * KV_HEADS,), jnp.float32)])
    w_qkv = jax.random.normal(key_qkv, (WIDTH, HEADS + 2 * KV_HEADS, HEAD_DIM), jnp.float32) * (WIDTH ** -0.5) * head_gain[None, :, None]
    w_out = jax.random.normal(key_out, (HEADS, HEAD_DIM, WIDTH), jnp.float32) * (OUT_GAIN * WIDTH ** -0.5)
    return {"x_in": act_rows.astype(jnp.bfloat16), "w_qkv": w_qkv.astype(jnp.bfloat16), "w_out": w_out.astype(jnp.bfloat16)}


def reference(x_in, w_qkv, w_out):
    qkv_rows = jnp.dot(x_in[0], w_qkv.reshape(WIDTH, -1), preferred_element_type=jnp.float32)
    qkv_rows = qkv_rows.astype(jnp.bfloat16).reshape(TOKENS, HEADS + 2 * KV_HEADS, HEAD_DIM)
    queries = qkv_rows[:, :HEADS].reshape(GROUP_DEVICES, TOKENS_DEV, KV_HEADS, GROUP_SIZE, HEAD_DIM)
    queries = jnp.transpose(queries, (2, 0, 1, 3, 4))
    key_heads = jnp.transpose(qkv_rows[:, HEADS:HEADS + KV_HEADS], (1, 0, 2))
    value_heads = jnp.transpose(qkv_rows[:, HEADS + KV_HEADS:], (1, 0, 2))
    logit_scale = HEAD_DIM ** -0.5

    def head_attend(operands):
        q_head, k_head, v_head = operands
        k_wide = k_head.astype(jnp.float32)
        v_wide = v_head.astype(jnp.float32)

        def tile_attend(q_tile):
            scores = jnp.einsum("qgd,sd->gqs", q_tile.astype(jnp.float32), k_wide) * logit_scale
            weights = jax.nn.softmax(scores, axis=-1)
            return jnp.einsum("gqs,sd->qgd", weights, v_wide)

        return lax.map(tile_attend, q_head)

    attn_out = lax.map(head_attend, (queries, key_heads, value_heads))
    attn_out = jnp.transpose(attn_out, (1, 2, 0, 3, 4)).reshape(TOKENS, WIDTH).astype(jnp.bfloat16)
    y_rows = jnp.dot(attn_out, w_out.reshape(WIDTH, WIDTH), preferred_element_type=jnp.float32)
    return y_rows.astype(jnp.bfloat16)[None]
```

```python
import functools
import math

import jax
import jax.numpy as jnp
from jax import lax
from jax.experimental import pallas as pl
from jax.experimental.pallas import tpu as pltpu
from jax.sharding import PartitionSpec as P

MESH = pl.DeviceIdType.MESH
LANES = 128
TILE = 256
NT = (((1,), (1,)), ((), ()))

ORDER = (
    (0, 0),
    (1, 0), (3, 0), (0, 1), (0, 3),
    (2, 0), (0, 2), (1, 1), (3, 3), (1, 3), (3, 1),
    (2, 1), (1, 2), (2, 3), (3, 2),
    (2, 2),
)


def kernel(dims, x_hbm, wqkv_hbm, wout_hbm, y_ref,
           x_ext, w_kv, w_q, w_o, kv_buf, q_t, acc, stat, o_buf, o_recv,
           load_sem, x_sem, kv_send, kv_recv, o_sem):
    nx, ny, heads, kv_heads, head_dim = dims
    chip_tokens = o_buf.shape[0]
    dev_tokens = chip_tokens // 2
    kv_local = kv_heads // 2
    group = heads // kv_heads
    q_rows = group * head_dim
    feat = kv_local * q_rows
    rows = q_t.shape[2]
    main = LANES
    tail = chip_tokens - main
    cx, cy, core = lax.axis_index("cx"), lax.axis_index("cy"), lax.axis_index("core")
    other = 1 - core
    own_rows = pl.ds(pl.multiple_of(core * dev_tokens, 32), dev_tokens)
    other_rows = pl.ds(pl.multiple_of(other * dev_tokens, 32), dev_tokens)

    x_load = pltpu.make_async_copy(x_hbm, x_ext.at[own_rows], load_sem.at[0])
    x_load.start()
    kv_loads = []
    for h in range(kv_local):
        head = core * kv_local + h
        for part in range(2):
            src = pl.multiple_of((heads + part * kv_heads + head) * head_dim, head_dim)
            copy = pltpu.make_async_copy(
                wqkv_hbm.at[pl.ds(src, head_dim)],
                w_kv.at[pl.ds(h * 2 * head_dim + part * head_dim, head_dim)],
                load_sem.at[1 + 2 * h + part])
            copy.start()
            kv_loads.append(copy)
    q_load = pltpu.make_async_copy(
        wqkv_hbm.at[pl.ds(pl.multiple_of(core * feat, feat), feat)], w_q, load_sem.at[1 + 2 * kv_local])
    q_load.start()

    def chip(dx, dy):
        return {"cx": lax.rem(cx + dx, nx), "cy": lax.rem(cy + dy, ny)}

    barrier = pltpu.get_barrier_semaphore()
    for target in ({"core": other}, chip(1, 0), chip(nx - 1, 0), chip(0, 1), chip(0, ny - 1)):
        pl.semaphore_signal(barrier, inc=1, device_id=target, device_id_type=MESH)
    pl.semaphore_wait(barrier, 5)

    x_load.wait()
    x_copy = pltpu.make_async_remote_copy(
        src_ref=x_ext.at[own_rows], dst_ref=x_ext.at[own_rows], send_sem=x_sem.at[0], recv_sem=x_sem.at[1],
        device_id={"core": other}, device_id_type=MESH)
    x_copy.start()
    q_t[:, head_dim:, :] = jnp.zeros((kv_local, LANES - head_dim, rows), jnp.bfloat16)
    x_copy.wait()
    x_ext[chip_tokens:chip_tokens + tail] = x_ext[main:chip_tokens]

    def send(slot, kind, half, target):
        width = kv_local // 2
        first = kind * width
        if half is not None:
            width //= 2
            first = first + half * width
        ref = kv_buf.at[slot, pl.ds(first, width)]
        pltpu.make_async_remote_copy(
            src_ref=ref, dst_ref=ref, send_sem=kv_send, recv_sem=kv_recv.at[slot, kind],
            device_id=target, device_id_type=MESH).start()

    def slot_of(dx, dy):
        return lax.rem(cy + dy, ny) * nx + lax.rem(cx + dx, nx)

    mine = slot_of(0, 0)
    for kind in range(2):
        for copy in kv_loads[kind * kv_local:(kind + 1) * kv_local]:
            copy.wait()
        part = lax.dot_general(
            x_ext[:chip_tokens], w_kv[kind * TILE:(kind + 1) * TILE], NT, preferred_element_type=jnp.float32)
        for h in range(2):
            kv_buf[mine, kind * 2 + h] = part[:, h * LANES:(h + 1) * LANES].astype(jnp.bfloat16)
        for target in (chip(1, 0), chip(nx - 1, 0), chip(0, 1), chip(0, ny - 1)):
            send(mine, kind, None, target)

    o_load = pltpu.make_async_copy(wout_hbm, w_o, load_sem.at[2 + 2 * kv_local])
    o_load.start()

    q_load.wait()
    lane = lax.broadcasted_iota(jnp.int32, (head_dim, LANES), 1)
    for h in range(kv_local):
        res = lax.dot_general(
            w_q[h * q_rows:(h + 1) * q_rows], x_ext[...], NT, preferred_element_type=jnp.float32)
        for g in range(group):
            q_t[h, :head_dim, g * LANES:(g + 1) * LANES] = (
                res[g * head_dim:(g + 1) * head_dim, :main].astype(jnp.bfloat16))
        for pair in range(group // 2):
            lo = res[2 * pair * head_dim:(2 * pair + 1) * head_dim, main:]
            hi = res[(2 * pair + 1) * head_dim:(2 * pair + 2) * head_dim, main:]
            q_t[h, :head_dim, (group + pair) * LANES:(group + pair + 1) * LANES] = (
                jnp.where(lane < tail, lo, hi).astype(jnp.bfloat16))

    acc[...] = jnp.zeros_like(acc)
    stat[:kv_local] = jnp.full((kv_local, rows), -jnp.inf, jnp.float32)
    stat[kv_local:] = jnp.zeros((kv_local, rows), jnp.float32)
    scale = head_dim ** -0.5 * math.log2(math.e)

    def receive_and_forward(dx, dy):
        slot = slot_of(dx, dy)
        for kind in range(2):
            ref = kv_buf.at[slot, pl.ds(kind * (kv_local // 2), kv_local // 2)]
            pltpu.make_async_remote_copy(
                src_ref=ref, dst_ref=ref, send_sem=kv_send, recv_sem=kv_recv.at[slot, kind],
                device_id={"core": other}, device_id_type=MESH).wait_recv()
            along, across = (dx, dy) if kind == 0 else (dy, dx)

            def step(sign, first_axis):
                on_x = (kind == 0) == first_axis
                return chip(sign % nx, 0) if on_x else chip(0, sign % ny)

            if across == 0:
                send(slot, kind, None, step(1, False))
                send(slot, kind, None, step(-1, False))
                if along == 3:
                    send(slot, kind, 0, step(1, True))
                if along == 1:
                    send(slot, kind, 1, step(-1, True))
            if across == 3:
                send(slot, kind, 0, step(1, False))
            if across == 1:
                send(slot, kind, 1, step(-1, False))

    def block_step(n, carry):
        slot = mine
        for k, (dx, dy) in enumerate(ORDER):
            if k == 0:
                continue
            slot = jnp.where(n == k, slot_of(dx, dy), slot)

            @pl.when(n + 1 == k)
            def _():
                receive_and_forward(dx, dy)

        for h in range(kv_local):
            kv = kv_buf[slot, h]
            v_t = jnp.transpose(kv.astype(jnp.float32), (1, 0))[head_dim:].astype(jnp.bfloat16)
            for t in range(rows // TILE):
                cols = slice(t * TILE, (t + 1) * TILE)
                scores = jnp.dot(kv, q_t[h, :, cols], preferred_element_type=jnp.float32)
                old_max = stat[h:h + 1, cols]
                new_max = jnp.maximum(old_max, jnp.max(scores, axis=0, keepdims=True))
                rescale = jnp.exp2((old_max - new_max) * scale)
                weights = jnp.exp2((scores - new_max) * scale)
                stat[h:h + 1, cols] = new_max
                stat[kv_local + h:kv_local + h + 1, cols] = (
                    stat[kv_local + h:kv_local + h + 1, cols] * rescale + jnp.sum(weights, axis=0, keepdims=True))
                acc[h, :, cols] = acc[h, :, cols] * rescale + jnp.dot(
                    v_t, weights.astype(jnp.bfloat16), preferred_element_type=jnp.float32)
        return carry

    lax.fori_loop(0, len(ORDER), block_step, 0)

    for h in range(kv_local):
        out = acc[h] / stat[kv_local + h:kv_local + h + 1, :]
        for pair in range(group // 2):
            cols = slice(h * q_rows + pair * LANES, h * q_rows + (pair + 1) * LANES)
            first = 2 * pair * LANES
            both = jnp.concatenate([out[:, first:first + LANES], out[:, first + LANES:first + 2 * LANES]], axis=0)
            o_buf[:main, cols] = jnp.transpose(both, (1, 0)).astype(jnp.bfloat16)
            ends = out[:, (group + pair) * LANES:(group + pair + 1) * LANES]
            both = jnp.concatenate([ends, pltpu.roll(ends, tail, 1)], axis=0)
            o_buf[main:, cols] = jnp.transpose(both, (1, 0))[:tail].astype(jnp.bfloat16)

    o_copy = pltpu.make_async_remote_copy(
        src_ref=o_buf.at[other_rows], dst_ref=o_recv, send_sem=o_sem.at[0], recv_sem=o_sem.at[1],
        device_id={"core": other}, device_id_type=MESH)
    o_copy.start()
    o_load.wait()
    y = jnp.dot(o_buf[own_rows], w_o[pl.ds(pl.multiple_of(core * feat, feat), feat)],
                preferred_element_type=jnp.float32)
    o_copy.wait()
    y = y + jnp.dot(o_recv[...], w_o[pl.ds(pl.multiple_of(other * feat, feat), feat)],
                    preferred_element_type=jnp.float32)
    y_ref[...] = y.astype(jnp.bfloat16)

    sent = kv_buf.at[pl.ds(0, nx * ny - 1)]
    pltpu.make_async_remote_copy(
        src_ref=sent, dst_ref=sent, send_sem=kv_send, recv_sem=o_sem.at[1],
        device_id={"core": other}, device_id_type=MESH).wait_send()


def solution(mesh):
    nx, ny = mesh.shape["cx"], mesh.shape["cy"]
    seq_spec = P("dp", ("cy", "cx", "core"))

    def local_layer(x_loc, w_qkv, w_out):
        heads, head_dim, width = w_out.shape
        kv_heads = (w_qkv.shape[1] - heads) // 2
        tokens = x_loc.shape[1]
        kv_local = kv_heads // 2
        group = heads // kv_heads
        feat = kv_local * group * head_dim
        rows = group * 2 * tokens
        dims = (nx, ny, heads, kv_heads, head_dim)
        w_rows = jnp.transpose(w_qkv, (1, 2, 0)).reshape(-1, width)
        hbm = pl.BlockSpec(memory_space=pl.ANY)
        y = pl.pallas_call(
            functools.partial(kernel, dims),
            out_shape=jax.ShapeDtypeStruct((tokens, width), jnp.bfloat16),
            in_specs=[hbm] * 3,
            out_specs=pl.BlockSpec(memory_space=pltpu.VMEM),
            scratch_shapes=[
                pltpu.VMEM((TILE, width), jnp.bfloat16),
                pltpu.VMEM((2 * kv_local * head_dim, width), jnp.bfloat16),
                pltpu.VMEM((feat, width), jnp.bfloat16),
                pltpu.VMEM((heads * head_dim, width), jnp.bfloat16),
                pltpu.VMEM((nx * ny, kv_local, 2 * tokens, LANES), jnp.bfloat16),
                pltpu.VMEM((kv_local, LANES, rows), jnp.bfloat16),
                pltpu.VMEM((kv_local, head_dim, rows), jnp.float32),
                pltpu.VMEM((2 * kv_local, rows), jnp.float32),
                pltpu.VMEM((2 * tokens, feat), jnp.bfloat16),
                pltpu.VMEM((tokens, feat), jnp.bfloat16),
                pltpu.SemaphoreType.DMA((3 + 2 * kv_local,)),
                pltpu.SemaphoreType.DMA((2,)),
                pltpu.SemaphoreType.DMA,
                pltpu.SemaphoreType.DMA((nx * ny, 2)),
                pltpu.SemaphoreType.DMA((2,)),
            ],
            compiler_params=pltpu.CompilerParams(collective_id=0, has_side_effects=True),
        )(x_loc[0], w_rows, w_out.reshape(heads * head_dim, width))
        return y[None]

    return jax.shard_map(local_layer, mesh=mesh, in_specs=(seq_spec, P(), P()), out_specs=seq_spec, check_vma=False)
```

```python
import functools
import math

import jax
import jax.numpy as jnp
from jax import lax
from jax.experimental import pallas as pl
from jax.experimental.pallas import tpu as pltpu
from jax.sharding import PartitionSpec as P

MESH = pl.DeviceIdType.MESH
LANES = 128
TILE = 256
NT = (((1,), (1,)), ((), ()))

ORDER = (
    (0, 0),
    (1, 0), (3, 0), (0, 1), (0, 3),
    (2, 0), (0, 2), (1, 1), (3, 3), (1, 3), (3, 1),
    (2, 1), (1, 2), (2, 3), (3, 2),
    (2, 2),
)


def kernel(dims, x_hbm, wqkv_hbm, wout_hbm, y_ref,
           x_ext, w_kv, w_q, w_o, kv_buf, q_t, v_t, s_buf, acc, stat, o_buf, o_recv,
           load_sem, x_sem, kv_send, kv_recv, o_sem):
    nx, ny, heads, kv_heads, head_dim = dims
    chip_tokens = o_buf.shape[0]
    dev_tokens = chip_tokens // 2
    kv_local = kv_heads // 2
    group = heads // kv_heads
    q_rows = group * head_dim
    feat = kv_local * q_rows
    rows = q_t.shape[2]
    main = LANES
    tail = chip_tokens - main
    cx, cy, core = lax.axis_index("cx"), lax.axis_index("cy"), lax.axis_index("core")
    other = 1 - core
    own_rows = pl.ds(pl.multiple_of(core * dev_tokens, 32), dev_tokens)
    other_rows = pl.ds(pl.multiple_of(other * dev_tokens, 32), dev_tokens)

    x_load = pltpu.make_async_copy(x_hbm, x_ext.at[own_rows], load_sem.at[0])
    x_load.start()
    kv_loads = []
    for h in range(kv_local):
        head = core * kv_local + h
        for part in range(2):
            src = pl.multiple_of((heads + part * kv_heads + head) * head_dim, head_dim)
            copy = pltpu.make_async_copy(
                wqkv_hbm.at[pl.ds(src, head_dim)],
                w_kv.at[pl.ds(h * 2 * head_dim + part * head_dim, head_dim)],
                load_sem.at[1 + 2 * h + part])
            copy.start()
            kv_loads.append(copy)
    q_load = pltpu.make_async_copy(
        wqkv_hbm.at[pl.ds(pl.multiple_of(core * feat, feat), feat)], w_q, load_sem.at[1 + 2 * kv_local])
    q_load.start()

    def chip(dx, dy):
        return {"cx": lax.rem(cx + dx, nx), "cy": lax.rem(cy + dy, ny)}

    barrier = pltpu.get_barrier_semaphore()
    for target in ({"core": other}, chip(1, 0), chip(nx - 1, 0), chip(0, 1), chip(0, ny - 1)):
        pl.semaphore_signal(barrier, inc=1, device_id=target, device_id_type=MESH)
    pl.semaphore_wait(barrier, 5)

    x_load.wait()
    x_copy = pltpu.make_async_remote_copy(
        src_ref=x_ext.at[own_rows], dst_ref=x_ext.at[own_rows], send_sem=x_sem.at[0], recv_sem=x_sem.at[1],
        device_id={"core": other}, device_id_type=MESH)
    x_copy.start()
    q_t[:, head_dim:, :] = jnp.zeros((kv_local, LANES - head_dim, rows), jnp.bfloat16)
    x_copy.wait()
    x_ext[chip_tokens:chip_tokens + tail] = x_ext[main:chip_tokens]

    def send(slot, kind, half, target):
        width = kv_local // 2
        first = kind * width
        if half is not None:
            width //= 2
            first = first + half * width
        ref = kv_buf.at[slot, pl.ds(first, width)]
        pltpu.make_async_remote_copy(
            src_ref=ref, dst_ref=ref, send_sem=kv_send, recv_sem=kv_recv.at[slot, kind],
            device_id=target, device_id_type=MESH).start()

    def slot_of(dx, dy):
        return lax.rem(cy + dy, ny) * nx + lax.rem(cx + dx, nx)

    mine = slot_of(0, 0)
    for kind in range(2):
        for copy in kv_loads[kind * kv_local:(kind + 1) * kv_local]:
            copy.wait()
        part = lax.dot_general(
            x_ext[:chip_tokens], w_kv[kind * TILE:(kind + 1) * TILE], NT, preferred_element_type=jnp.float32)
        for h in range(2):
            kv_buf[mine, kind * 2 + h] = part[:, h * LANES:(h + 1) * LANES].astype(jnp.bfloat16)
        for target in (chip(1, 0), chip(nx - 1, 0), chip(0, 1), chip(0, ny - 1)):
            send(mine, kind, None, target)

    o_load = pltpu.make_async_copy(wout_hbm, w_o, load_sem.at[2 + 2 * kv_local])
    o_load.start()

    q_load.wait()
    lane = lax.broadcasted_iota(jnp.int32, (head_dim, LANES), 1)
    for h in range(kv_local):
        res = lax.dot_general(
            w_q[h * q_rows:(h + 1) * q_rows], x_ext[...], NT, preferred_element_type=jnp.float32)
        for g in range(group):
            q_t[h, :head_dim, g * LANES:(g + 1) * LANES] = (
                res[g * head_dim:(g + 1) * head_dim, :main].astype(jnp.bfloat16))
        for pair in range(group // 2):
            lo = res[2 * pair * head_dim:(2 * pair + 1) * head_dim, main:]
            hi = res[(2 * pair + 1) * head_dim:(2 * pair + 2) * head_dim, main:]
            q_t[h, :head_dim, (group + pair) * LANES:(group + pair + 1) * LANES] = (
                jnp.where(lane < tail, lo, hi).astype(jnp.bfloat16))

    acc[...] = jnp.zeros_like(acc)
    stat[:kv_local] = jnp.full((kv_local, rows), -jnp.inf, jnp.float32)
    stat[kv_local:2 * kv_local] = jnp.zeros((kv_local, rows), jnp.float32)
    scale = head_dim ** -0.5 * math.log2(math.e)

    def receive_and_forward(dx, dy):
        slot = slot_of(dx, dy)
        for kind in range(2):
            ref = kv_buf.at[slot, pl.ds(kind * (kv_local // 2), kv_local // 2)]
            pltpu.make_async_remote_copy(
                src_ref=ref, dst_ref=ref, send_sem=kv_send, recv_sem=kv_recv.at[slot, kind],
                device_id={"core": other}, device_id_type=MESH).wait_recv()
            along, across = (dx, dy) if kind == 0 else (dy, dx)

            def step(sign, first_axis):
                on_x = (kind == 0) == first_axis
                return chip(sign % nx, 0) if on_x else chip(0, sign % ny)

            if across == 0:
                send(slot, kind, None, step(1, False))
                send(slot, kind, None, step(-1, False))
                if along == 3:
                    send(slot, kind, 0, step(1, True))
                if along == 1:
                    send(slot, kind, 1, step(-1, True))
            if across == 3:
                send(slot, kind, 0, step(1, False))
            if across == 1:
                send(slot, kind, 1, step(-1, False))

    tiles = rows // TILE

    def score(slot):
        def head_tile(h, t):
            cols = slice(t * TILE, (t + 1) * TILE)
            if t == 0:
                v_t[h] = jnp.transpose(kv_buf[slot, h].astype(jnp.float32), (1, 0))[head_dim:].astype(jnp.bfloat16)
            scores = jnp.dot(kv_buf[slot, h], q_t[h, :, cols], preferred_element_type=jnp.float32)
            old_max = stat[h:h + 1, cols]
            new_max = jnp.maximum(old_max, jnp.max(scores, axis=0, keepdims=True))
            stat[h:h + 1, cols] = new_max
            stat[2 * kv_local + h:2 * kv_local + h + 1, cols] = jnp.exp2((old_max - new_max) * scale)
            s_buf[h * tiles + t] = scores
        return head_tile

    def absorb(h, t):
        cols = slice(t * TILE, (t + 1) * TILE)
        rescale = stat[2 * kv_local + h:2 * kv_local + h + 1, cols]
        weights = jnp.exp2((s_buf[h * tiles + t] - stat[h:h + 1, cols]) * scale)
        stat[kv_local + h:kv_local + h + 1, cols] = (
            stat[kv_local + h:kv_local + h + 1, cols] * rescale + jnp.sum(weights, axis=0, keepdims=True))
        acc[h, :, cols] = acc[h, :, cols] * rescale + jnp.dot(
            v_t[h], weights.astype(jnp.bfloat16), preferred_element_type=jnp.float32)

    pieces = [(h, t) for h in range(kv_local) for t in range(tiles)]

    first_score = score(mine)
    for h, t in pieces:
        first_score(h, t)

    def block_step(n, carry):
        slot = mine
        for k, (dx, dy) in enumerate(ORDER):
            if k == 0:
                continue
            slot = jnp.where(n == k, slot_of(dx, dy), slot)

            @pl.when(n == k)
            def _():
                receive_and_forward(dx, dy)

        next_score = score(slot)
        for i, (h, t) in enumerate(pieces):
            absorb(h, t)
            if t == tiles - 1:
                for u in range(tiles):
                    next_score(h, u)
        return carry

    lax.fori_loop(1, len(ORDER), block_step, 0)
    for h, t in pieces:
        absorb(h, t)

    for h in range(kv_local):
        out = acc[h] / stat[kv_local + h:kv_local + h + 1, :]
        for pair in range(group // 2):
            cols = slice(h * q_rows + pair * LANES, h * q_rows + (pair + 1) * LANES)
            first = 2 * pair * LANES
            both = jnp.concatenate([out[:, first:first + LANES], out[:, first + LANES:first + 2 * LANES]], axis=0)
            o_buf[:main, cols] = jnp.transpose(both, (1, 0)).astype(jnp.bfloat16)
            ends = out[:, (group + pair) * LANES:(group + pair + 1) * LANES]
            both = jnp.concatenate([ends, pltpu.roll(ends, tail, 1)], axis=0)
            o_buf[main:, cols] = jnp.transpose(both, (1, 0))[:tail].astype(jnp.bfloat16)

    o_copy = pltpu.make_async_remote_copy(
        src_ref=o_buf.at[other_rows], dst_ref=o_recv, send_sem=o_sem.at[0], recv_sem=o_sem.at[1],
        device_id={"core": other}, device_id_type=MESH)
    o_copy.start()
    o_load.wait()
    y = jnp.dot(o_buf[own_rows], w_o[pl.ds(pl.multiple_of(core * feat, feat), feat)],
                preferred_element_type=jnp.float32)
    o_copy.wait()
    y = y + jnp.dot(o_recv[...], w_o[pl.ds(pl.multiple_of(other * feat, feat), feat)],
                    preferred_element_type=jnp.float32)
    y_ref[...] = y.astype(jnp.bfloat16)

    sent = kv_buf.at[pl.ds(0, nx * ny - 1)]
    pltpu.make_async_remote_copy(
        src_ref=sent, dst_ref=sent, send_sem=kv_send, recv_sem=o_sem.at[1],
        device_id={"core": other}, device_id_type=MESH).wait_send()


def solution(mesh):
    nx, ny = mesh.shape["cx"], mesh.shape["cy"]
    seq_spec = P("dp", ("cy", "cx", "core"))

    def local_layer(x_loc, w_qkv, w_out):
        heads, head_dim, width = w_out.shape
        kv_heads = (w_qkv.shape[1] - heads) // 2
        tokens = x_loc.shape[1]
        kv_local = kv_heads // 2
        group = heads // kv_heads
        feat = kv_local * group * head_dim
        rows = group * 2 * tokens
        dims = (nx, ny, heads, kv_heads, head_dim)
        w_rows = jnp.transpose(w_qkv, (1, 2, 0)).reshape(-1, width)
        hbm = pl.BlockSpec(memory_space=pl.ANY)
        y = pl.pallas_call(
            functools.partial(kernel, dims),
            out_shape=jax.ShapeDtypeStruct((tokens, width), jnp.bfloat16),
            in_specs=[hbm] * 3,
            out_specs=pl.BlockSpec(memory_space=pltpu.VMEM),
            scratch_shapes=[
                pltpu.VMEM((TILE, width), jnp.bfloat16),
                pltpu.VMEM((2 * kv_local * head_dim, width), jnp.bfloat16),
                pltpu.VMEM((feat, width), jnp.bfloat16),
                pltpu.VMEM((heads * head_dim, width), jnp.bfloat16),
                pltpu.VMEM((nx * ny, kv_local, 2 * tokens, LANES), jnp.bfloat16),
                pltpu.VMEM((kv_local, LANES, rows), jnp.bfloat16),
                pltpu.VMEM((kv_local, head_dim, 2 * tokens), jnp.bfloat16),
                pltpu.VMEM((kv_local * (rows // TILE), 2 * tokens, TILE), jnp.float32),
                pltpu.VMEM((kv_local, head_dim, rows), jnp.float32),
                pltpu.VMEM((3 * kv_local, rows), jnp.float32),
                pltpu.VMEM((2 * tokens, feat), jnp.bfloat16),
                pltpu.VMEM((tokens, feat), jnp.bfloat16),
                pltpu.SemaphoreType.DMA((3 + 2 * kv_local,)),
                pltpu.SemaphoreType.DMA((2,)),
                pltpu.SemaphoreType.DMA,
                pltpu.SemaphoreType.DMA((nx * ny, 2)),
                pltpu.SemaphoreType.DMA((2,)),
            ],
            compiler_params=pltpu.CompilerParams(collective_id=0, has_side_effects=True),
        )(x_loc[0], w_rows, w_out.reshape(heads * head_dim, width))
        return y[None]

    return jax.shard_map(local_layer, mesh=mesh, in_specs=(seq_spec, P(), P()), out_specs=seq_spec, check_vma=False)
```

```python
import functools
import math

import jax
import jax.numpy as jnp
from jax import lax
from jax.experimental import pallas as pl
from jax.experimental.pallas import tpu as pltpu
from jax.sharding import PartitionSpec as P

MESH = pl.DeviceIdType.MESH
LANES = 128
TILE = 256
NT = (((1,), (1,)), ((), ()))

ORDER = (
    (0, 0),
    (1, 0), (3, 0), (0, 1), (0, 3),
    (2, 0), (1, 1), (3, 1), (1, 3), (0, 2), (3, 3),
    (2, 1), (2, 3), (1, 2), (3, 2),
    (2, 2),
)


def kernel(dims, x_hbm, wqkv_hbm, wout_hbm, y_ref,
           x_ext, w_kv, w_q, w_o, kv_buf, q_t, v_t, s_buf, acc, stat, o_buf, o_recv,
           load_sem, x_sem, kv_send, kv_recv, o_sem):
    nx, ny, heads, kv_heads, head_dim = dims
    chip_tokens = o_buf.shape[0]
    dev_tokens = chip_tokens // 2
    kv_local = kv_heads // 2
    group = heads // kv_heads
    q_rows = group * head_dim
    feat = kv_local * q_rows
    rows = q_t.shape[2]
    main = LANES
    tail = chip_tokens - main
    cx, cy, core = lax.axis_index("cx"), lax.axis_index("cy"), lax.axis_index("core")
    other = 1 - core
    own_rows = pl.ds(pl.multiple_of(core * dev_tokens, 32), dev_tokens)
    other_rows = pl.ds(pl.multiple_of(other * dev_tokens, 32), dev_tokens)

    x_load = pltpu.make_async_copy(x_hbm, x_ext.at[own_rows], load_sem.at[0])
    x_load.start()
    kv_loads = []
    for h in range(kv_local):
        head = core * kv_local + h
        for part in range(2):
            src = pl.multiple_of((heads + part * kv_heads + head) * head_dim, head_dim)
            copy = pltpu.make_async_copy(
                wqkv_hbm.at[pl.ds(src, head_dim)],
                w_kv.at[pl.ds(h * 2 * head_dim + part * head_dim, head_dim)],
                load_sem.at[1 + 2 * h + part])
            copy.start()
            kv_loads.append(copy)
    q_load = pltpu.make_async_copy(
        wqkv_hbm.at[pl.ds(pl.multiple_of(core * feat, feat), feat)], w_q, load_sem.at[1 + 2 * kv_local])
    q_load.start()

    def chip(dx, dy):
        return {"cx": lax.rem(cx + dx, nx), "cy": lax.rem(cy + dy, ny)}

    barrier = pltpu.get_barrier_semaphore()
    for target in ({"core": other}, chip(1, 0), chip(nx - 1, 0), chip(0, 1), chip(0, ny - 1)):
        pl.semaphore_signal(barrier, inc=1, device_id=target, device_id_type=MESH)
    pl.semaphore_wait(barrier, 5)

    x_load.wait()
    x_copy = pltpu.make_async_remote_copy(
        src_ref=x_ext.at[own_rows], dst_ref=x_ext.at[own_rows], send_sem=x_sem.at[0], recv_sem=x_sem.at[1],
        device_id={"core": other}, device_id_type=MESH)
    x_copy.start()
    q_t[:, head_dim:, :] = jnp.zeros((kv_local, LANES - head_dim, rows), jnp.bfloat16)
    x_copy.wait()
    x_ext[chip_tokens:chip_tokens + tail] = x_ext[main:chip_tokens]

    def send(slot, kind, half, target):
        width = kv_local // 2
        first = kind * width
        if half is not None:
            width //= 2
            first = first + half * width
        ref = kv_buf.at[slot, pl.ds(first, width)]
        pltpu.make_async_remote_copy(
            src_ref=ref, dst_ref=ref, send_sem=kv_send, recv_sem=kv_recv.at[slot, kind],
            device_id=target, device_id_type=MESH).start()

    def slot_of(dx, dy):
        return lax.rem(cy + dy, ny) * nx + lax.rem(cx + dx, nx)

    mine = slot_of(0, 0)
    for copy in kv_loads:
        copy.wait()
    part = lax.dot_general(x_ext[:chip_tokens], w_kv[...], NT, preferred_element_type=jnp.float32)
    for h in range(kv_local):
        kv_buf[mine, h] = part[:, h * LANES:(h + 1) * LANES].astype(jnp.bfloat16)
    for kind in range(2):
        for target in (chip(1, 0), chip(nx - 1, 0), chip(0, 1), chip(0, ny - 1)):
            send(mine, kind, None, target)

    o_load = pltpu.make_async_copy(wout_hbm, w_o, load_sem.at[2 + 2 * kv_local])
    o_load.start()

    q_load.wait()
    lane = lax.broadcasted_iota(jnp.int32, (head_dim, LANES), 1)
    for h in range(kv_local):
        res = lax.dot_general(
            w_q[h * q_rows:(h + 1) * q_rows], x_ext[...], NT, preferred_element_type=jnp.float32)
        for g in range(group):
            q_t[h, :head_dim, g * LANES:(g + 1) * LANES] = (
                res[g * head_dim:(g + 1) * head_dim, :main].astype(jnp.bfloat16))
        for pair in range(group // 2):
            lo = res[2 * pair * head_dim:(2 * pair + 1) * head_dim, main:]
            hi = res[(2 * pair + 1) * head_dim:(2 * pair + 2) * head_dim, main:]
            q_t[h, :head_dim, (group + pair) * LANES:(group + pair + 1) * LANES] = (
                jnp.where(lane < tail, lo, hi).astype(jnp.bfloat16))

    acc[...] = jnp.zeros_like(acc)
    stat[:kv_local] = jnp.full((kv_local, rows), -jnp.inf, jnp.float32)
    stat[kv_local:2 * kv_local] = jnp.zeros((kv_local, rows), jnp.float32)
    scale = head_dim ** -0.5 * math.log2(math.e)

    def receive_and_forward(kind, along, across):
        dx, dy = (along, across) if kind == 0 else (across, along)
        slot = slot_of(dx, dy)
        ref = kv_buf.at[slot, pl.ds(kind * (kv_local // 2), kv_local // 2)]
        pltpu.make_async_remote_copy(
            src_ref=ref, dst_ref=ref, send_sem=kv_send, recv_sem=kv_recv.at[slot, kind],
            device_id={"core": other}, device_id_type=MESH).wait_recv()

        def step(sign, first_axis):
            on_x = (kind == 0) == first_axis
            return chip(sign % nx, 0) if on_x else chip(0, sign % ny)

        if across == 0:
            if along == 3:
                send(slot, kind, 0, step(1, True))
            if along == 1:
                send(slot, kind, 1, step(-1, True))
            send(slot, kind, None, step(1, False))
            send(slot, kind, None, step(-1, False))
        if across == 3:
            send(slot, kind, 0, step(1, False))
        if across == 1:
            send(slot, kind, 1, step(-1, False))

    tiles = rows // TILE

    def score(slots):
        def head_tile(h, t):
            slot = slots[h * 2 // kv_local]
            cols = slice(t * TILE, (t + 1) * TILE)
            if t == 0:
                v_t[h] = jnp.transpose(kv_buf[slot, h].astype(jnp.float32), (1, 0))[head_dim:].astype(jnp.bfloat16)
            scores = jnp.dot(kv_buf[slot, h], q_t[h, :, cols], preferred_element_type=jnp.float32)
            old_max = stat[h:h + 1, cols]
            new_max = jnp.maximum(old_max, jnp.max(scores, axis=0, keepdims=True))
            stat[h:h + 1, cols] = new_max
            stat[2 * kv_local + h:2 * kv_local + h + 1, cols] = jnp.exp2((old_max - new_max) * scale)
            s_buf[h * tiles + t] = scores
        return head_tile

    def absorb(h, t):
        cols = slice(t * TILE, (t + 1) * TILE)
        rescale = stat[2 * kv_local + h:2 * kv_local + h + 1, cols]
        weights = jnp.exp2((s_buf[h * tiles + t] - stat[h:h + 1, cols]) * scale)
        stat[kv_local + h:kv_local + h + 1, cols] = (
            stat[kv_local + h:kv_local + h + 1, cols] * rescale + jnp.sum(weights, axis=0, keepdims=True))
        acc[h, :, cols] = acc[h, :, cols] * rescale + jnp.dot(
            v_t[h], weights.astype(jnp.bfloat16), preferred_element_type=jnp.float32)

    pieces = [(h, t) for h in range(kv_local) for t in range(tiles)]

    first_score = score((mine, mine))
    for h, t in pieces:
        first_score(h, t)

    def block_step(n, carry):
        slots = [mine, mine]
        for k, (along, across) in enumerate(ORDER):
            if k == 0:
                continue
            slots[0] = jnp.where(n == k, slot_of(along, across), slots[0])
            slots[1] = jnp.where(n == k, slot_of(across, along), slots[1])

            @pl.when(n == k)
            def _():
                receive_and_forward(0, along, across)
                receive_and_forward(1, along, across)

        next_score = score(slots)
        for i, (h, t) in enumerate(pieces):
            absorb(h, t)
            if t == tiles - 1:
                for u in range(tiles):
                    next_score(h, u)
        return carry

    lax.fori_loop(1, len(ORDER), block_step, 0)
    for h, t in pieces:
        absorb(h, t)

    for h in range(kv_local):
        out = acc[h] / stat[kv_local + h:kv_local + h + 1, :]
        for pair in range(group // 2):
            cols = slice(h * q_rows + pair * LANES, h * q_rows + (pair + 1) * LANES)
            first = 2 * pair * LANES
            both = jnp.concatenate([out[:, first:first + LANES], out[:, first + LANES:first + 2 * LANES]], axis=0)
            o_buf[:main, cols] = jnp.transpose(both, (1, 0)).astype(jnp.bfloat16)
            ends = out[:, (group + pair) * LANES:(group + pair + 1) * LANES]
            both = jnp.concatenate([ends, pltpu.roll(ends, tail, 1)], axis=0)
            o_buf[main:, cols] = jnp.transpose(both, (1, 0))[:tail].astype(jnp.bfloat16)

    o_copy = pltpu.make_async_remote_copy(
        src_ref=o_buf.at[other_rows], dst_ref=o_recv, send_sem=o_sem.at[0], recv_sem=o_sem.at[1],
        device_id={"core": other}, device_id_type=MESH)
    o_copy.start()
    o_load.wait()
    y = jnp.dot(o_buf[own_rows], w_o[pl.ds(pl.multiple_of(core * feat, feat), feat)],
                preferred_element_type=jnp.float32)
    o_copy.wait()
    y = y + jnp.dot(o_recv[...], w_o[pl.ds(pl.multiple_of(other * feat, feat), feat)],
                    preferred_element_type=jnp.float32)
    y_ref[...] = y.astype(jnp.bfloat16)

    sent = kv_buf.at[pl.ds(0, nx * ny - 1)]
    pltpu.make_async_remote_copy(
        src_ref=sent, dst_ref=sent, send_sem=kv_send, recv_sem=o_sem.at[1],
        device_id={"core": other}, device_id_type=MESH).wait_send()


def solution(mesh):
    nx, ny = mesh.shape["cx"], mesh.shape["cy"]
    seq_spec = P("dp", ("cy", "cx", "core"))

    def local_layer(x_loc, w_qkv, w_out):
        heads, head_dim, width = w_out.shape
        kv_heads = (w_qkv.shape[1] - heads) // 2
        tokens = x_loc.shape[1]
        kv_local = kv_heads // 2
        group = heads // kv_heads
        feat = kv_local * group * head_dim
        rows = group * 2 * tokens
        dims = (nx, ny, heads, kv_heads, head_dim)
        w_rows = jnp.transpose(w_qkv, (1, 2, 0)).reshape(-1, width)
        hbm = pl.BlockSpec(memory_space=pl.ANY)
        y = pl.pallas_call(
            functools.partial(kernel, dims),
            out_shape=jax.ShapeDtypeStruct((tokens, width), jnp.bfloat16),
            in_specs=[hbm] * 3,
            out_specs=pl.BlockSpec(memory_space=pltpu.VMEM),
            scratch_shapes=[
                pltpu.VMEM((TILE, width), jnp.bfloat16),
                pltpu.VMEM((2 * kv_local * head_dim, width), jnp.bfloat16),
                pltpu.VMEM((feat, width), jnp.bfloat16),
                pltpu.VMEM((heads * head_dim, width), jnp.bfloat16),
                pltpu.VMEM((nx * ny, kv_local, 2 * tokens, LANES), jnp.bfloat16),
                pltpu.VMEM((kv_local, LANES, rows), jnp.bfloat16),
                pltpu.VMEM((kv_local, head_dim, 2 * tokens), jnp.bfloat16),
                pltpu.VMEM((kv_local * (rows // TILE), 2 * tokens, TILE), jnp.float32),
                pltpu.VMEM((kv_local, head_dim, rows), jnp.float32),
                pltpu.VMEM((3 * kv_local, rows), jnp.float32),
                pltpu.VMEM((2 * tokens, feat), jnp.bfloat16),
                pltpu.VMEM((tokens, feat), jnp.bfloat16),
                pltpu.SemaphoreType.DMA((3 + 2 * kv_local,)),
                pltpu.SemaphoreType.DMA((2,)),
                pltpu.SemaphoreType.DMA,
                pltpu.SemaphoreType.DMA((nx * ny, 2)),
                pltpu.SemaphoreType.DMA((2,)),
            ],
            compiler_params=pltpu.CompilerParams(
                collective_id=0, has_side_effects=True, vmem_limit_bytes=54000 * 1024),
        )(x_loc[0], w_rows, w_out.reshape(heads * head_dim, width))
        return y[None]

    return jax.shard_map(local_layer, mesh=mesh, in_specs=(seq_spec, P(), P()), out_specs=seq_spec, check_vma=False)
```

```python
import functools
import math

import jax
import jax.numpy as jnp
from jax import lax
from jax.experimental import pallas as pl
from jax.experimental.pallas import tpu as pltpu
from jax.sharding import PartitionSpec as P

MESH = pl.DeviceIdType.MESH
LANES = 128
TILE = 256
NT = (((1,), (1,)), ((), ()))

STEPS = (
    (0, 0), (1, 0), (3, 0), (2, 0), (2, 1), (2, 3), (1, 1), (2, 2),
    (1, 3), (1, 2), (3, 1), (3, 3), (3, 2), (0, 1), (0, 3), (0, 2),
)


def kernel(dims, x_hbm, wqkv_hbm, wout_hbm, y_ref,
           x_ext, w_kv, w_q, w_o, kv_all, kv_buf, kv_relay, q_all, q_t, q_relay,
           v_t, s_buf, m_cur, r_cur, m_run, l_run, acc, o_send, o_relay, o_all, y_acc,
           load_sem, x_sem, kv_send, kv_recv, kv_relay_sem, q_send, q_recv, q_relay_sem,
           o_send_sem, o_recv, o_relay_sem):
    nx, ny, heads, kv_heads, head_dim = dims
    chip_tokens = kv_all.shape[1]
    dev_tokens = chip_tokens // 2
    kv_local = kv_heads // 2
    group = heads // kv_heads
    q_rows = group * head_dim
    feat = kv_local * q_rows
    rows = q_t.shape[2]
    tiles = rows // TILE
    main = LANES
    tail = chip_tokens - main
    cx, cy, core = lax.axis_index("cx"), lax.axis_index("cy"), lax.axis_index("core")
    other = 1 - core
    own_rows = pl.ds(pl.multiple_of(core * dev_tokens, 32), dev_tokens)
    other_rows = pl.ds(pl.multiple_of(other * dev_tokens, 32), dev_tokens)
    scale = head_dim ** -0.5 * math.log2(math.e)

    x_load = pltpu.make_async_copy(x_hbm, x_ext.at[own_rows], load_sem.at[0])
    x_load.start()
    kv_loads = []
    for h in range(kv_local):
        head = core * kv_local + h
        for part in range(2):
            src = pl.multiple_of((heads + part * kv_heads + head) * head_dim, head_dim)
            copy = pltpu.make_async_copy(
                wqkv_hbm.at[pl.ds(src, head_dim)],
                w_kv.at[pl.ds(h * 2 * head_dim + part * head_dim, head_dim)],
                load_sem.at[1 + 2 * h + part])
            copy.start()
            kv_loads.append(copy)
    q_load = pltpu.make_async_copy(
        wqkv_hbm.at[pl.ds(pl.multiple_of(core * feat, feat), feat)], w_q, load_sem.at[1 + 2 * kv_local])
    q_load.start()

    east = {"cx": lax.rem(cx + 1, nx)}
    west = {"cx": lax.rem(cx + nx - 1, nx)}
    north = {"cy": lax.rem(cy + 1, ny)}
    south = {"cy": lax.rem(cy + ny - 1, ny)}
    partner = {"core": other}
    targets = (partner, east, west, {**east, **partner}, {**west, **partner}, north, south)
    barrier = pltpu.get_barrier_semaphore()
    for target in targets:
        pl.semaphore_signal(barrier, inc=1, device_id=target, device_id_type=MESH)
    pl.semaphore_wait(barrier, len(targets))

    def remote(src, dst, send_sem, recv_sem, target):
        return pltpu.make_async_remote_copy(
            src_ref=src, dst_ref=dst, send_sem=send_sem, recv_sem=recv_sem, device_id=target, device_id_type=MESH)

    x_load.wait()
    x_copy = remote(x_ext.at[own_rows], x_ext.at[own_rows], x_sem.at[0], x_sem.at[1], partner)
    x_copy.start()
    q_t[:, head_dim:, :] = jnp.zeros((nx, LANES - head_dim, rows), jnp.bfloat16)
    acc[...] = jnp.zeros_like(acc)
    m_run[...] = jnp.full_like(m_run, -jnp.inf)
    l_run[...] = jnp.zeros_like(l_run)
    for copy in kv_loads:
        copy.wait()
    x_copy.wait()

    part = lax.dot_general(x_ext[:chip_tokens], w_kv[...], NT, preferred_element_type=jnp.float32)
    for h in range(kv_local):
        kv_all[h] = part[:, h * LANES:(h + 1) * LANES].astype(jnp.bfloat16)

    def head_at(dx):
        return lax.rem(cx + dx, nx)

    def kv_piece(dx, dy):
        return kv_buf.at[dy, pl.ds(dx * chip_tokens, chip_tokens)]

    def kv_half(dx, half):
        return kv_buf.at[0, pl.ds(dx * chip_tokens + half * dev_tokens, dev_tokens)]

    far = kv_all.at[head_at(2)]
    for half, target in ((0, east), (1, west)):
        remote(far.at[pl.ds(half * dev_tokens, dev_tokens)], kv_relay.at[half],
               kv_send, kv_relay_sem.at[half], target).start()
    remote(kv_all.at[head_at(1)], kv_piece(3, 0), kv_send, kv_recv.at[0, 3], east).start()
    remote(kv_all.at[head_at(3)], kv_piece(1, 0), kv_send, kv_recv.at[0, 1], west).start()

    def spread(src, dx):
        remote(src, kv_piece(dx, 3), kv_send, kv_recv.at[3, dx], north).start()
        remote(src, kv_piece(dx, 1), kv_send, kv_recv.at[1, dx], south).start()

    spread(kv_all.at[cx], 0)
    kv_buf[0, :chip_tokens] = kv_all[cx]
    o_load = pltpu.make_async_copy(wout_hbm, w_o, load_sem.at[2 + 2 * kv_local])
    o_load.start()

    q_load.wait()
    x_ext[chip_tokens:chip_tokens + tail] = x_ext[main:chip_tokens]
    lane = lax.broadcasted_iota(jnp.int32, (head_dim, LANES), 1)
    for dx in (2, 1, 3, 0):
        res = lax.dot_general(
            w_q[pl.ds(pl.multiple_of(head_at(dx) * q_rows, q_rows), q_rows)], x_ext[...], NT,
            preferred_element_type=jnp.float32)
        dst = q_t.at[0, pl.ds(0, head_dim)] if dx == 0 else q_all.at[dx]
        for g in range(group):
            dst[:, g * LANES:(g + 1) * LANES] = res[g * head_dim:(g + 1) * head_dim, :main].astype(jnp.bfloat16)
        for pair in range(group // 2):
            lo = res[2 * pair * head_dim:(2 * pair + 1) * head_dim, main:]
            hi = res[(2 * pair + 1) * head_dim:(2 * pair + 2) * head_dim, main:]
            dst[:, (group + pair) * LANES:(group + pair + 1) * LANES] = (
                jnp.where(lane < tail, lo, hi).astype(jnp.bfloat16))
        half_dim = head_dim // 2
        if dx == 2:
            for half, target in ((0, east), (1, west)):
                remote(q_all.at[2, pl.ds(half * half_dim, half_dim)], q_relay.at[half],
                       q_send, q_relay_sem.at[half], target).start()
        if dx == 1:
            remote(q_all.at[1], q_t.at[3, pl.ds(0, head_dim)], q_send, q_recv.at[3], east).start()
        if dx == 3:
            remote(q_all.at[3], q_t.at[1, pl.ds(0, head_dim)], q_send, q_recv.at[1], west).start()

    def arrive(ref, sem):
        remote(ref, ref, kv_send, sem, partner).wait_recv()

    def kv_relay_on():
        for half, target in ((0, east), (1, west)):
            arrive(kv_relay.at[half], kv_relay_sem.at[half])
            remote(kv_relay.at[half], kv_half(2, half), kv_send, kv_recv.at[0, 2], target).start()

    def kv_row(dx):
        arrive(kv_piece(dx, 0), kv_recv.at[0, dx])
        spread(kv_piece(dx, 0), dx)

    def kv_side(dx, dy):
        arrive(kv_piece(dx, dy), kv_recv.at[dy, dx])
        if dy == 3 and dx % 2 == 0:
            remote(kv_piece(dx, 3), kv_piece(dx, 2), kv_send, kv_recv.at[2, dx], north).start()
        if dy == 1 and dx % 2 == 1:
            remote(kv_piece(dx, 1), kv_piece(dx, 2), kv_send, kv_recv.at[2, dx], south).start()

    def q_relay_on():
        for half, target in ((0, east), (1, west)):
            arrive(q_relay.at[half], q_relay_sem.at[half])
            remote(q_relay.at[half], q_t.at[2, pl.ds(half * half_dim, half_dim)],
                   q_send, q_recv.at[2], target).start()

    def q_arrive(dx):
        arrive(q_t.at[dx, pl.ds(0, head_dim)], q_recv.at[dx])

    def o_relay_on():
        for half, target in ((0, east), (1, {**west, **partner})):
            arrive(o_relay.at[half], o_relay_sem.at[half])
            remote(o_relay.at[half], o_all.at[half, 2], o_send_sem.at[0], o_recv.at[half, 2], target).start()

    def score(q, dy, t):
        cols = slice(t * TILE, (t + 1) * TILE)
        scores = jnp.dot(kv_buf[dy], q_t[q, :, cols], preferred_element_type=jnp.float32)
        old_max = m_run[q, :, cols]
        new_max = jnp.maximum(old_max, jnp.max(scores, axis=0, keepdims=True))
        m_run[q, :, cols] = new_max
        m_cur[:, cols] = new_max
        r_cur[:, cols] = jnp.exp2((old_max - new_max) * scale)
        s_buf[t] = scores

    def absorb(q, dy, t):
        cols = slice(t * TILE, (t + 1) * TILE)
        rescale = r_cur[:, cols]
        weights = jnp.exp2((s_buf[t] - m_cur[:, cols]) * scale)
        l_run[q, :, cols] = l_run[q, :, cols] * rescale + jnp.sum(weights, axis=0, keepdims=True)
        acc[q, :, cols] = acc[q, :, cols] * rescale + jnp.dot(
            v_t[dy], weights.astype(jnp.bfloat16), preferred_element_type=jnp.float32)

    def finish(q):
        out = acc[q] / l_run[q]
        dst = o_send.at[q]
        for pair in range(group // 2):
            cols = slice(pair * LANES, (pair + 1) * LANES)
            first = 2 * pair * LANES
            both = jnp.concatenate([out[:, first:first + LANES], out[:, first + LANES:first + 2 * LANES]], axis=0)
            dst[:main, cols] = jnp.transpose(both, (1, 0)).astype(jnp.bfloat16)
            ends = out[:, (group + pair) * LANES:(group + pair + 1) * LANES]
            both = jnp.concatenate([ends, pltpu.roll(ends, tail, 1)], axis=0)
            dst[main:, cols] = jnp.transpose(both, (1, 0))[:tail].astype(jnp.bfloat16)
        mine, theirs = o_send.at[q, own_rows], o_send.at[q, other_rows]
        if q == 2:
            remote(mine, o_relay.at[0], o_send_sem.at[0], o_relay_sem.at[0], east).start()
            remote(theirs, o_relay.at[1], o_send_sem.at[0], o_relay_sem.at[1], west).start()
        elif q:
            target = east if q == 1 else west
            remote(mine, o_all.at[0, nx - q], o_send_sem.at[0], o_recv.at[0, nx - q], target).start()
            remote(theirs, o_all.at[1, nx - q], o_send_sem.at[0], o_recv.at[1, nx - q], {**target, **partner}).start()
        else:
            remote(theirs, o_all.at[1, 0], o_send_sem.at[1], o_recv.at[1, 0], partner).start()
            o_all[0, 0] = o_send[0, own_rows]

    events = {n: [] for n in range(len(STEPS) + 1)}
    events[0] = [kv_relay_on, lambda: kv_row(1), lambda: kv_row(3), lambda: kv_side(0, 1), lambda: kv_side(0, 3),
                 lambda: kv_row(2), q_relay_on]
    events[1] = [lambda: kv_side(1, 1), lambda: kv_side(3, 1), lambda: kv_side(1, 3), lambda: kv_side(3, 3),
                 lambda: q_arrive(1)]
    events[2] = [lambda: q_arrive(3)]
    events[3] = [lambda: kv_side(2, 1), lambda: kv_side(2, 3), lambda: q_arrive(2)]
    events[7] = [lambda dx=dx: kv_side(dx, 2) for dx in range(nx)]
    events[12] = [o_relay_on]
    last_of = {q: max(n for n, s in enumerate(STEPS) if s[0] == q) for q in range(nx)}
    first_of = {dy: min(n for n, s in enumerate(STEPS) if s[1] == dy) for dy in range(ny)}

    for n in range(len(STEPS) + 1):
        for event in events[n]:
            event()
        if n < len(STEPS) and first_of[STEPS[n][1]] == n:
            dy = STEPS[n][1]
            v_t[dy] = jnp.transpose(kv_buf[dy].astype(jnp.float32), (1, 0))[head_dim:].astype(jnp.bfloat16)
        for t in range(tiles):
            if n:
                absorb(*STEPS[n - 1], t)
            if n < len(STEPS):
                score(*STEPS[n], t)
        if n and last_of[STEPS[n - 1][0]] == n - 1:
            finish(STEPS[n - 1][0])

    o_load.wait()
    for i, dx in enumerate((2, 1, 3, 0)):
        total = None
        for r in range(2):
            if dx or r:
                arrive(o_all.at[r, dx], o_recv.at[r, dx])
            first = ((core if r == 0 else other) * kv_local + head_at(dx)) * q_rows
            term = jnp.dot(o_all[r, dx], w_o[pl.ds(pl.multiple_of(first, q_rows), q_rows)],
                           preferred_element_type=jnp.float32)
            total = term if total is None else total + term
        if i == 0:
            y_acc[...] = total
        elif i < nx - 1:
            y_acc[...] += total
        else:
            y_ref[...] = (y_acc[...] + total).astype(jnp.bfloat16)

    for ref, sem in ((kv_buf, kv_send), (q_all, q_send), (o_all, o_send_sem.at[0]), (o_all.at[1, 0], o_send_sem.at[1])):
        remote(ref, ref, sem, x_sem.at[1], partner).wait_send()


def solution(mesh):
    nx, ny = mesh.shape["cx"], mesh.shape["cy"]
    seq_spec = P("dp", ("cy", "cx", "core"))

    def local_layer(x_loc, w_qkv, w_out):
        heads, head_dim, width = w_out.shape
        kv_heads = (w_qkv.shape[1] - heads) // 2
        tokens = x_loc.shape[1]
        kv_local = kv_heads // 2
        group = heads // kv_heads
        q_rows = group * head_dim
        feat = kv_local * q_rows
        rows = group * 2 * tokens
        dims = (nx, ny, heads, kv_heads, head_dim)
        w_rows = jnp.transpose(w_qkv, (1, 2, 0)).reshape(-1, width)
        hbm = pl.BlockSpec(memory_space=pl.ANY)
        half = jnp.bfloat16
        y = pl.pallas_call(
            functools.partial(kernel, dims),
            out_shape=jax.ShapeDtypeStruct((tokens, width), half),
            in_specs=[hbm] * 3,
            out_specs=pl.BlockSpec(memory_space=pltpu.VMEM),
            scratch_shapes=[
                pltpu.VMEM((TILE, width), half),
                pltpu.VMEM((2 * kv_local * head_dim, width), half),
                pltpu.VMEM((feat, width), half),
                pltpu.VMEM((heads * head_dim, width), half),
                pltpu.VMEM((kv_local, 2 * tokens, LANES), half),
                pltpu.VMEM((ny, nx * 2 * tokens, LANES), half),
                pltpu.VMEM((2, tokens, LANES), half),
                pltpu.VMEM((nx, head_dim, rows), half),
                pltpu.VMEM((nx, LANES, rows), half),
                pltpu.VMEM((2, head_dim // 2, rows), half),
                pltpu.VMEM((ny, head_dim, nx * 2 * tokens), half),
                pltpu.VMEM((rows // TILE, nx * 2 * tokens, TILE), jnp.float32),
                pltpu.VMEM((1, rows), jnp.float32),
                pltpu.VMEM((1, rows), jnp.float32),
                pltpu.VMEM((nx, 1, rows), jnp.float32),
                pltpu.VMEM((nx, 1, rows), jnp.float32),
                pltpu.VMEM((nx, head_dim, rows), jnp.float32),
                pltpu.VMEM((nx, 2 * tokens, q_rows), half),
                pltpu.VMEM((2, tokens, q_rows), half),
                pltpu.VMEM((2, nx, tokens, q_rows), half),
                pltpu.VMEM((tokens, width), jnp.float32),
                pltpu.SemaphoreType.DMA((3 + 2 * kv_local,)),
                pltpu.SemaphoreType.DMA((2,)),
                pltpu.SemaphoreType.DMA,
                pltpu.SemaphoreType.DMA((ny, nx)),
                pltpu.SemaphoreType.DMA((2,)),
                pltpu.SemaphoreType.DMA,
                pltpu.SemaphoreType.DMA((nx,)),
                pltpu.SemaphoreType.DMA((2,)),
                pltpu.SemaphoreType.DMA((2,)),
                pltpu.SemaphoreType.DMA((2, nx)),
                pltpu.SemaphoreType.DMA((2,)),
            ],
            compiler_params=pltpu.CompilerParams(
                collective_id=0, has_side_effects=True, vmem_limit_bytes=54000 * 1024),
        )(x_loc[0], w_rows, w_out.reshape(heads * head_dim, width))
        return y[None]

    return jax.shard_map(local_layer, mesh=mesh, in_specs=(seq_spec, P(), P()), out_specs=seq_spec, check_vma=False)
```

```python
import functools
import math

import jax
import jax.numpy as jnp
from jax import lax
from jax.experimental import pallas as pl
from jax.experimental.pallas import tpu as pltpu
from jax.sharding import PartitionSpec as P

MESH = pl.DeviceIdType.MESH
LANES = 128
TILE = 256
NT = (((1,), (1,)), ((), ()))

STEPS = (
    (1, 0), (3, 0), (1, 1), (3, 1), (2, 3), (2, 1), (2, 0), (3, 3),
    (2, 2), (3, 2), (1, 3), (1, 2), (0, 0), (0, 3), (0, 1), (0, 2),
)
FAR_FIRST = (2, 1, 3, 0)
O_ORDER = (3, 0, 1, 2)


def kernel(dims, x_hbm, wqkv_hbm, wout_hbm, y_ref,
           x_ext, w_kv, w_q, w_o, kv_all, kv_buf, q_all, q_t, q_relay,
           v_t, s_buf, m_cur, r_cur, m_run, l_run, acc, o_send, o_relay, o_all, y_acc,
           load_sem, x_sem, kv_send, kv_recv, q_send, q_recv, q_relay_sem,
           o_send_sem, o_recv, o_relay_sem):
    nx, ny, heads, kv_heads, head_dim = dims
    dev_tokens = x_hbm.shape[0]
    chip_tokens = 2 * dev_tokens
    row_keys = nx * chip_tokens
    kv_local = kv_heads // 2
    group = heads // kv_heads
    q_rows = group * head_dim
    feat = kv_local * q_rows
    rows = q_t.shape[2]
    tiles = rows // TILE
    main = LANES
    tail = chip_tokens - main
    cx, cy, core = lax.axis_index("cx"), lax.axis_index("cy"), lax.axis_index("core")
    other = 1 - core
    own_rows = pl.ds(pl.multiple_of(core * dev_tokens, 32), dev_tokens)
    other_rows = pl.ds(pl.multiple_of(other * dev_tokens, 32), dev_tokens)
    scale = head_dim ** -0.5 * math.log2(math.e)

    def head_at(dx):
        return lax.rem(cx + dx, nx)

    x_load = pltpu.make_async_copy(x_hbm, x_ext.at[own_rows], load_sem.at[0])
    x_load.start()
    kv_loads, q_loads = [], []
    for i, dx in enumerate(FAR_FIRST):
        for r in range(2):
            head = (core if r == 0 else other) * kv_local + head_at(dx)
            for part in range(2):
                src = pl.multiple_of((heads + part * kv_heads + head) * head_dim, head_dim)
                copy = pltpu.make_async_copy(
                    wqkv_hbm.at[pl.ds(src, head_dim)],
                    w_kv.at[pl.ds((4 * i + 2 * r + part) * head_dim, head_dim)],
                    load_sem.at[1 + 4 * i + 2 * r + part])
                copy.start()
                kv_loads.append(copy)
    for i, dx in enumerate(FAR_FIRST):
        src = pl.multiple_of(core * feat + head_at(dx) * q_rows, q_rows)
        copy = pltpu.make_async_copy(
            wqkv_hbm.at[pl.ds(src, q_rows)], w_q.at[pl.ds(i * q_rows, q_rows)], load_sem.at[1 + 4 * nx + i])
        copy.start()
        q_loads.append(copy)

    east = {"cx": lax.rem(cx + 1, nx)}
    west = {"cx": lax.rem(cx + nx - 1, nx)}
    north = {"cy": lax.rem(cy + 1, ny)}
    south = {"cy": lax.rem(cy + ny - 1, ny)}
    partner = {"core": other}
    across = {"cx": head_at(2)}
    by_dx = {0: {}, 1: east, 2: across, 3: west}
    targets = [partner, north, south]
    for dx in range(1, nx):
        targets += [by_dx[dx], {**by_dx[dx], **partner}]
    barrier = pltpu.get_barrier_semaphore()
    for target in targets:
        pl.semaphore_signal(barrier, inc=1, device_id=target, device_id_type=MESH)
    pl.semaphore_wait(barrier, len(targets))

    def remote(src, dst, send_sem, recv_sem, target):
        return pltpu.make_async_remote_copy(
            src_ref=src, dst_ref=dst, send_sem=send_sem, recv_sem=recv_sem, device_id=target, device_id_type=MESH)

    x_load.wait()
    x_copy = remote(x_ext.at[own_rows], x_ext.at[own_rows], x_sem.at[0], x_sem.at[1], partner)
    x_copy.start()
    q_t[:, head_dim:, :] = jnp.zeros((nx, LANES - head_dim, rows), jnp.bfloat16)
    acc[...] = jnp.zeros_like(acc)
    m_run[...] = jnp.full_like(m_run, -jnp.inf)
    l_run[...] = jnp.zeros_like(l_run)

    def kv_at(dx, dy):
        return dy * row_keys + dx * chip_tokens

    def kv_piece(dx, dy):
        return kv_buf.at[pl.ds(kv_at(dx, dy), chip_tokens)]

    def kv_half(dx, dy, r):
        return kv_buf.at[pl.ds(kv_at(dx, dy) + r * dev_tokens, dev_tokens)]

    def spread(src, dst_of, dx):
        remote(src, dst_of(3), kv_send.at[0], kv_recv.at[3, dx], north).start()
        remote(src, dst_of(1), kv_send.at[0], kv_recv.at[1, dx], south).start()

    for i in range(0, nx, 2):
        for copy in kv_loads[4 * i:4 * i + 8]:
            copy.wait()
        part = lax.dot_general(
            x_ext[own_rows], w_kv[4 * i * head_dim:(4 * i + 8) * head_dim], NT, preferred_element_type=jnp.float32)
        for k in range(4):
            kv_all[2 * i + k] = part[:, k * LANES:(k + 1) * LANES].astype(jnp.bfloat16)
        for k in range(4):
            dx, r = FAR_FIRST[i + k // 2], k % 2
            src = kv_all.at[2 * i + k]
            back = (nx - dx) % nx
            if dx:
                target = {**by_dx[dx], **partner} if r else by_dx[dx]
                remote(src, kv_half(back, 0, r), kv_send.at[0], kv_recv.at[0, back], target).start()
            elif r:
                remote(src, kv_half(0, 0, 1), kv_send.at[1], kv_recv.at[0, 0], partner).start()
            else:
                spread(src, lambda dy: kv_half(0, dy, 0), 0)
                kv_buf[kv_at(0, 0):kv_at(0, 0) + dev_tokens] = kv_all[2 * i + k]
    o_load = pltpu.make_async_copy(wout_hbm, w_o, load_sem.at[1 + 5 * nx])
    o_load.start()

    x_copy.wait()
    x_ext[chip_tokens:chip_tokens + tail] = x_ext[main:chip_tokens]
    lane = lax.broadcasted_iota(jnp.int32, (head_dim, LANES), 1)
    half_dim = head_dim // 2
    for i in range(0, nx, 2):
        results = []
        for k in (i, i + 1):
            q_loads[k].wait()
        for k in (i, i + 1):
            results.append(lax.dot_general(
                w_q[k * q_rows:(k + 1) * q_rows], x_ext[...], NT, preferred_element_type=jnp.float32))
        for k, res in zip((i, i + 1), results):
            dst = q_all.at[FAR_FIRST[k]] if FAR_FIRST[k] else q_t.at[0, pl.ds(0, head_dim)]
            for g in range(group):
                dst[:, g * LANES:(g + 1) * LANES] = res[g * head_dim:(g + 1) * head_dim, :main].astype(jnp.bfloat16)
            for pair in range(group // 2):
                lo = res[2 * pair * head_dim:(2 * pair + 1) * head_dim, main:]
                hi = res[(2 * pair + 1) * head_dim:(2 * pair + 2) * head_dim, main:]
                dst[:, (group + pair) * LANES:(group + pair + 1) * LANES] = (
                    jnp.where(lane < tail, lo, hi).astype(jnp.bfloat16))
        for k in (i, i + 1):
            dx = FAR_FIRST[k]
            if dx == 2:
                for half, target in ((0, east), (1, west)):
                    remote(q_all.at[2, pl.ds(half * half_dim, half_dim)], q_relay.at[half],
                           q_send, q_relay_sem.at[half], target).start()
            elif dx:
                remote(q_all.at[dx], q_t.at[nx - dx, pl.ds(0, head_dim)],
                       q_send, q_recv.at[nx - dx], by_dx[dx]).start()

    def arrive(ref, sem):
        remote(ref, ref, q_send, sem, partner).wait_recv()

    def kv_row(dx):
        if dx:
            arrive(kv_piece(dx, 0), kv_recv.at[0, dx])
            spread(kv_piece(dx, 0), lambda dy: kv_piece(dx, dy), dx)
        else:
            arrive(kv_half(0, 0, 1), kv_recv.at[0, 0])
            spread(kv_half(0, 0, 1), lambda dy: kv_half(0, dy, 1), 0)

    def kv_side(dx, dy):
        arrive(kv_piece(dx, dy), kv_recv.at[dy, dx])
        if dy == 3 and dx % 2 == 0:
            remote(kv_piece(dx, 3), kv_piece(dx, 2), kv_send.at[0], kv_recv.at[2, dx], north).start()
        if dy == 1 and dx % 2 == 1:
            remote(kv_piece(dx, 1), kv_piece(dx, 2), kv_send.at[0], kv_recv.at[2, dx], south).start()

    def q_relay_on():
        for half, target in ((0, east), (1, west)):
            arrive(q_relay.at[half], q_relay_sem.at[half])
            remote(q_relay.at[half], q_t.at[2, pl.ds(half * half_dim, half_dim)],
                   q_send, q_recv.at[2], target).start()

    def q_arrive(dx):
        arrive(q_t.at[dx, pl.ds(0, head_dim)], q_recv.at[dx])

    def o_relay_on():
        for half, target in ((0, east), (1, {**west, **partner})):
            arrive(o_relay.at[half], o_relay_sem.at[half])
            remote(o_relay.at[half], o_all.at[half, 2], o_send_sem.at[0], o_recv.at[half, 2], target).start()

    def keys(dy):
        return kv_buf[kv_at(0, dy):kv_at(0, dy) + row_keys]

    def score(q, dy, t):
        cols = slice(t * TILE, (t + 1) * TILE)
        scores = jnp.dot(keys(dy), q_t[q, :, cols], preferred_element_type=jnp.float32)
        old_max = m_run[q, :, cols]
        new_max = jnp.maximum(old_max, jnp.max(scores, axis=0, keepdims=True))
        m_run[q, :, cols] = new_max
        m_cur[:, cols] = new_max
        r_cur[:, cols] = jnp.exp2((old_max - new_max) * scale)
        s_buf[t] = scores

    def absorb(q, dy, t):
        cols = slice(t * TILE, (t + 1) * TILE)
        rescale = r_cur[:, cols]
        weights = jnp.exp2((s_buf[t] - m_cur[:, cols]) * scale)
        l_run[q, :, cols] = l_run[q, :, cols] * rescale + jnp.sum(weights, axis=0, keepdims=True)
        acc[q, :, cols] = acc[q, :, cols] * rescale + jnp.dot(
            v_t[dy], weights.astype(jnp.bfloat16), preferred_element_type=jnp.float32)

    def finish(q):
        out = acc[q] / l_run[q]
        dst = o_send.at[q]
        for pair in range(group // 2):
            cols = slice(pair * LANES, (pair + 1) * LANES)
            first = 2 * pair * LANES
            both = jnp.concatenate([out[:, first:first + LANES], out[:, first + LANES:first + 2 * LANES]], axis=0)
            dst[:main, cols] = jnp.transpose(both, (1, 0)).astype(jnp.bfloat16)
            ends = out[:, (group + pair) * LANES:(group + pair + 1) * LANES]
            both = jnp.concatenate([ends, pltpu.roll(ends, tail, 1)], axis=0)
            dst[main:, cols] = jnp.transpose(both, (1, 0))[:tail].astype(jnp.bfloat16)
        mine, theirs = o_send.at[q, own_rows], o_send.at[q, other_rows]
        if q == 2:
            remote(mine, o_relay.at[0], o_send_sem.at[0], o_relay_sem.at[0], east).start()
            remote(theirs, o_relay.at[1], o_send_sem.at[0], o_relay_sem.at[1], west).start()
        elif q:
            target = east if q == 1 else west
            remote(mine, o_all.at[0, nx - q], o_send_sem.at[0], o_recv.at[0, nx - q], target).start()
            remote(theirs, o_all.at[1, nx - q], o_send_sem.at[0], o_recv.at[1, nx - q], {**target, **partner}).start()
        else:
            remote(theirs, o_all.at[1, 0], o_send_sem.at[1], o_recv.at[1, 0], partner).start()
            o_all[0, 0] = o_send[0, own_rows]

    events = {n: [] for n in range(len(STEPS) + 1)}
    def row(*dxs):
        return [functools.partial(kv_row, dx) for dx in dxs]

    def side(*pieces):
        return [functools.partial(kv_side, dx, dy) for dx, dy in pieces]

    def query(dx):
        return [functools.partial(q_arrive, dx)]

    events[0] = row(0, 1, 2, 3) + [q_relay_on] + query(1)
    events[1] = side((0, 1), (1, 1)) + query(3) + side((1, 3), (2, 3))
    events[2] = side((0, 3), (2, 1), (3, 1))
    events[4] = query(2) + side((3, 3))
    events[5] = side((1, 2))
    events[8] = side((3, 2), (2, 2), (0, 2))
    events[15] = [o_relay_on]
    last_of = {q: max(n for n, s in enumerate(STEPS) if s[0] == q) for q in range(nx)}
    first_of = {dy: min(n for n, s in enumerate(STEPS) if s[1] == dy) for dy in range(ny)}

    for n in range(len(STEPS) + 1):
        for event in events[n]:
            event()
        if n < len(STEPS) and first_of[STEPS[n][1]] == n:
            dy = STEPS[n][1]
            v_t[dy] = jnp.transpose(keys(dy).astype(jnp.float32), (1, 0))[head_dim:].astype(jnp.bfloat16)
        for t in range(tiles):
            if n:
                absorb(*STEPS[n - 1], t)
            if n < len(STEPS):
                score(*STEPS[n], t)
        if n and last_of[STEPS[n - 1][0]] == n - 1:
            finish(STEPS[n - 1][0])

    o_load.wait()
    for i, dx in enumerate(O_ORDER):
        total = None
        for r in range(2):
            if dx or r:
                arrive(o_all.at[r, dx], o_recv.at[r, dx])
            first = ((core if r == 0 else other) * kv_local + head_at(dx)) * q_rows
            term = jnp.dot(o_all[r, dx], w_o[pl.ds(pl.multiple_of(first, q_rows), q_rows)],
                           preferred_element_type=jnp.float32)
            total = term if total is None else total + term
        if i == 0:
            y_acc[...] = total
        elif i < nx - 1:
            y_acc[...] += total
        else:
            y_ref[...] = (y_acc[...] + total).astype(jnp.bfloat16)

    for ref, sem in ((kv_buf.at[pl.ds(0, (nx * ny - 1) * chip_tokens)], kv_send.at[0]), (kv_all.at[0], kv_send.at[1]), (q_all, q_send), (o_all, o_send_sem.at[0]), (o_all.at[1, 0], o_send_sem.at[1])):
        remote(ref, ref, sem, x_sem.at[1], partner).wait_send()


def solution(mesh):
    nx, ny = mesh.shape["cx"], mesh.shape["cy"]
    seq_spec = P("dp", ("cy", "cx", "core"))

    def local_layer(x_loc, w_qkv, w_out):
        heads, head_dim, width = w_out.shape
        kv_heads = (w_qkv.shape[1] - heads) // 2
        tokens = x_loc.shape[1]
        kv_local = kv_heads // 2
        group = heads // kv_heads
        q_rows = group * head_dim
        feat = kv_local * q_rows
        rows = group * 2 * tokens
        dims = (nx, ny, heads, kv_heads, head_dim)
        w_rows = jnp.transpose(w_qkv, (1, 2, 0)).reshape(-1, width)
        hbm = pl.BlockSpec(memory_space=pl.ANY)
        half = jnp.bfloat16
        y = pl.pallas_call(
            functools.partial(kernel, dims),
            out_shape=jax.ShapeDtypeStruct((tokens, width), half),
            in_specs=[hbm] * 3,
            out_specs=pl.BlockSpec(memory_space=pltpu.VMEM),
            scratch_shapes=[
                pltpu.VMEM((TILE, width), half),
                pltpu.VMEM((2 * kv_heads * head_dim, width), half),
                pltpu.VMEM((feat, width), half),
                pltpu.VMEM((heads * head_dim, width), half),
                pltpu.VMEM((kv_heads, tokens, LANES), half),
                pltpu.VMEM((ny * nx * 2 * tokens, LANES), half),
                pltpu.VMEM((nx, head_dim, rows), half),
                pltpu.VMEM((nx, LANES, rows), half),
                pltpu.VMEM((2, head_dim // 2, rows), half),
                pltpu.VMEM((ny, head_dim, nx * 2 * tokens), half),
                pltpu.VMEM((rows // TILE, nx * 2 * tokens, TILE), jnp.float32),
                pltpu.VMEM((1, rows), jnp.float32),
                pltpu.VMEM((1, rows), jnp.float32),
                pltpu.VMEM((nx, 1, rows), jnp.float32),
                pltpu.VMEM((nx, 1, rows), jnp.float32),
                pltpu.VMEM((nx, head_dim, rows), jnp.float32),
                pltpu.VMEM((nx, 2 * tokens, q_rows), half),
                pltpu.VMEM((2, tokens, q_rows), half),
                pltpu.VMEM((2, nx, tokens, q_rows), half),
                pltpu.VMEM((tokens, width), jnp.float32),
                pltpu.SemaphoreType.DMA((2 + 5 * nx,)),
                pltpu.SemaphoreType.DMA((2,)),
                pltpu.SemaphoreType.DMA((2,)),
                pltpu.SemaphoreType.DMA((ny, nx)),
                pltpu.SemaphoreType.DMA,
                pltpu.SemaphoreType.DMA((nx,)),
                pltpu.SemaphoreType.DMA((2,)),
                pltpu.SemaphoreType.DMA((2,)),
                pltpu.SemaphoreType.DMA((2, nx)),
                pltpu.SemaphoreType.DMA((2,)),
            ],
            compiler_params=pltpu.CompilerParams(
                collective_id=0, has_side_effects=True, vmem_limit_bytes=54600 * 1024),
        )(x_loc[0], w_rows, w_out.reshape(heads * head_dim, width))
        return y[None]

    return jax.shard_map(local_layer, mesh=mesh, in_specs=(seq_spec, P(), P()), out_specs=seq_spec, check_vma=False)
```

```python
import functools
import math

import jax
import jax.numpy as jnp
from jax import lax
from jax.experimental import pallas as pl
from jax.experimental.pallas import tpu as pltpu
from jax.sharding import PartitionSpec as P

MESH = pl.DeviceIdType.MESH
LANES = 128
TILE = 256
NT = (((1,), (1,)), ((), ()))

STEPS = (
    (1, 0), (3, 0), (1, 1), (3, 1), (2, 3), (2, 1), (2, 0), (3, 3),
    (2, 2), (3, 2), (1, 3), (1, 2), (0, 0), (0, 3), (0, 1), (0, 2),
)
FAR_FIRST = (2, 1, 3, 0)
O_ORDER = (3, 0, 1, 2)


def kernel(dims, x_hbm, wqkv_hbm, wout_hbm, y_ref,
           x_ext, w_kv, w_q, w_o, kv_all, kv_buf, q_all, q_t, q_relay,
           v_t, s_buf, m_cur, r_cur, m_run, l_run, acc, o_send, o_relay, o_all, y_acc,
           load_sem, x_sem, kv_send, kv_recv, q_send, q_recv, q_relay_sem,
           o_send_sem, o_recv, o_relay_sem):
    nx, ny, heads, kv_heads, head_dim = dims
    dev_tokens = x_hbm.shape[0]
    chip_tokens = 2 * dev_tokens
    row_keys = nx * chip_tokens
    kv_local = kv_heads // 2
    group = heads // kv_heads
    q_rows = group * head_dim
    feat = kv_local * q_rows
    rows = q_t.shape[2]
    tiles = rows // TILE
    main = LANES
    tail = chip_tokens - main
    cx, cy, core = lax.axis_index("cx"), lax.axis_index("cy"), lax.axis_index("core")
    other = 1 - core
    own_rows = pl.ds(pl.multiple_of(core * dev_tokens, 32), dev_tokens)
    other_rows = pl.ds(pl.multiple_of(other * dev_tokens, 32), dev_tokens)
    scale = head_dim ** -0.5 * math.log2(math.e)

    def head_at(dx):
        return lax.rem(cx + dx, nx)

    x_load = pltpu.make_async_copy(x_hbm, x_ext.at[own_rows], load_sem.at[0])
    x_load.start()
    kv_loads, q_loads = [], []
    for i, dx in enumerate(FAR_FIRST):
        for r in range(2):
            head = (core if r == 0 else other) * kv_local + head_at(dx)
            for part in range(2):
                src = pl.multiple_of((heads + part * kv_heads + head) * head_dim, head_dim)
                copy = pltpu.make_async_copy(
                    wqkv_hbm.at[pl.ds(src, head_dim)],
                    w_kv.at[pl.ds((4 * i + 2 * r + part) * head_dim, head_dim)],
                    load_sem.at[1 + 4 * i + 2 * r + part])
                copy.start()
                kv_loads.append(copy)
    for i, dx in enumerate(FAR_FIRST):
        src = pl.multiple_of(core * feat + head_at(dx) * q_rows, q_rows)
        copy = pltpu.make_async_copy(
            wqkv_hbm.at[pl.ds(src, q_rows)], w_q.at[pl.ds(i * q_rows, q_rows)], load_sem.at[1 + 4 * nx + i])
        copy.start()
        q_loads.append(copy)

    east = {"cx": lax.rem(cx + 1, nx)}
    west = {"cx": lax.rem(cx + nx - 1, nx)}
    north = {"cy": lax.rem(cy + 1, ny)}
    south = {"cy": lax.rem(cy + ny - 1, ny)}
    partner = {"core": other}
    across = {"cx": head_at(2)}
    by_dx = {0: {}, 1: east, 2: across, 3: west}
    targets = [partner, north, south]
    for dx in range(1, nx):
        targets += [by_dx[dx], {**by_dx[dx], **partner}]
    barrier = pltpu.get_barrier_semaphore()
    for target in targets:
        pl.semaphore_signal(barrier, inc=1, device_id=target, device_id_type=MESH)
    pl.semaphore_wait(barrier, len(targets))

    def remote(src, dst, send_sem, recv_sem, target):
        return pltpu.make_async_remote_copy(
            src_ref=src, dst_ref=dst, send_sem=send_sem, recv_sem=recv_sem, device_id=target, device_id_type=MESH)

    x_load.wait()
    x_copy = remote(x_ext.at[own_rows], x_ext.at[own_rows], x_sem.at[0], x_sem.at[1], partner)
    x_copy.start()
    q_t[:, head_dim:, :] = jnp.zeros((nx, LANES - head_dim, rows), jnp.bfloat16)
    acc[...] = jnp.zeros_like(acc)
    m_run[...] = jnp.full_like(m_run, -jnp.inf)
    l_run[...] = jnp.zeros_like(l_run)

    def kv_at(dx, dy):
        return dy * row_keys + dx * chip_tokens

    def kv_piece(dx, dy):
        return kv_buf.at[pl.ds(kv_at(dx, dy), chip_tokens)]

    def kv_half(dx, dy, r):
        return kv_buf.at[pl.ds(kv_at(dx, dy) + r * dev_tokens, dev_tokens)]

    def spread(src, dst_of, dx):
        remote(src, dst_of(3), kv_send.at[0], kv_recv.at[3, dx], north).start()
        remote(src, dst_of(1), kv_send.at[0], kv_recv.at[1, dx], south).start()

    for i in range(0, nx, 2):
        for copy in kv_loads[4 * i:4 * i + 8]:
            copy.wait()
        part = lax.dot_general(
            x_ext[own_rows], w_kv[4 * i * head_dim:(4 * i + 8) * head_dim], NT, preferred_element_type=jnp.float32)
        for k in range(4):
            kv_all[2 * i + k] = part[:, k * LANES:(k + 1) * LANES].astype(jnp.bfloat16)
        for k in range(4):
            dx, r = FAR_FIRST[i + k // 2], k % 2
            src = kv_all.at[2 * i + k]
            back = (nx - dx) % nx
            if dx:
                target = {**by_dx[dx], **partner} if r else by_dx[dx]
                remote(src, kv_half(back, 0, r), kv_send.at[0], kv_recv.at[0, back], target).start()
            elif r:
                remote(src, kv_half(0, 0, 1), kv_send.at[1], kv_recv.at[0, 0], partner).start()
            else:
                spread(src, lambda dy: kv_half(0, dy, 0), 0)
                kv_buf[kv_at(0, 0):kv_at(0, 0) + dev_tokens] = kv_all[2 * i + k]
    o_load = pltpu.make_async_copy(wout_hbm, w_o, load_sem.at[1 + 5 * nx])
    o_load.start()

    x_copy.wait()
    x_ext[chip_tokens:chip_tokens + tail] = x_ext[main:chip_tokens]
    lane = lax.broadcasted_iota(jnp.int32, (head_dim, LANES), 1)
    half_dim = head_dim // 2
    for i in range(0, nx, 2):
        results = []
        for k in (i, i + 1):
            q_loads[k].wait()
        for k in (i, i + 1):
            results.append(lax.dot_general(
                w_q[k * q_rows:(k + 1) * q_rows], x_ext[...], NT, preferred_element_type=jnp.float32))
        for k, res in zip((i, i + 1), results):
            dst = q_all.at[FAR_FIRST[k]] if FAR_FIRST[k] else q_t.at[0, pl.ds(0, head_dim)]
            for g in range(group):
                dst[:, g * LANES:(g + 1) * LANES] = res[g * head_dim:(g + 1) * head_dim, :main].astype(jnp.bfloat16)
            for pair in range(group // 2):
                lo = res[2 * pair * head_dim:(2 * pair + 1) * head_dim, main:]
                hi = res[(2 * pair + 1) * head_dim:(2 * pair + 2) * head_dim, main:]
                dst[:, (group + pair) * LANES:(group + pair + 1) * LANES] = (
                    jnp.where(lane < tail, lo, hi).astype(jnp.bfloat16))
        for k in (i, i + 1):
            dx = FAR_FIRST[k]
            if dx == 2:
                for half, target in ((0, east), (1, west)):
                    remote(q_all.at[2, pl.ds(half * half_dim, half_dim)], q_relay.at[half],
                           q_send, q_relay_sem.at[half], target).start()
            elif dx:
                remote(q_all.at[dx], q_t.at[nx - dx, pl.ds(0, head_dim)],
                       q_send, q_recv.at[nx - dx], by_dx[dx]).start()

    def arrive(ref, sem):
        remote(ref, ref, q_send, sem, partner).wait_recv()

    def kv_row(dx):
        if dx:
            arrive(kv_piece(dx, 0), kv_recv.at[0, dx])
            spread(kv_piece(dx, 0), lambda dy: kv_piece(dx, dy), dx)
        else:
            arrive(kv_half(0, 0, 1), kv_recv.at[0, 0])
            spread(kv_half(0, 0, 1), lambda dy: kv_half(0, dy, 1), 0)

    def kv_side(dx, dy):
        arrive(kv_piece(dx, dy), kv_recv.at[dy, dx])
        if dy == 3 and dx % 2 == 0:
            remote(kv_piece(dx, 3), kv_piece(dx, 2), kv_send.at[0], kv_recv.at[2, dx], north).start()
        if dy == 1 and dx % 2 == 1:
            remote(kv_piece(dx, 1), kv_piece(dx, 2), kv_send.at[0], kv_recv.at[2, dx], south).start()

    def q_relay_on():
        for half, target in ((0, east), (1, west)):
            arrive(q_relay.at[half], q_relay_sem.at[half])
            remote(q_relay.at[half], q_t.at[2, pl.ds(half * half_dim, half_dim)],
                   q_send, q_recv.at[2], target).start()

    def q_arrive(dx):
        arrive(q_t.at[dx, pl.ds(0, head_dim)], q_recv.at[dx])

    def o_relay_on():
        for half, target in ((0, east), (1, {**west, **partner})):
            arrive(o_relay.at[half], o_relay_sem.at[half])
            remote(o_relay.at[half], o_all.at[half, 2], o_send_sem.at[0], o_recv.at[half, 2], target).start()

    def keys(dy):
        return kv_buf[kv_at(0, dy):kv_at(0, dy) + row_keys]

    def score(n, q, dy, t):
        cols = slice(t * TILE, (t + 1) * TILE)
        scores = jnp.dot(keys(dy), q_t[q, :, cols], preferred_element_type=jnp.float32)
        old_max = m_run[q, :, cols]
        new_max = jnp.maximum(old_max, jnp.max(scores, axis=0, keepdims=True))
        m_run[q, :, cols] = new_max
        m_cur[n % 2, :, cols] = new_max
        r_cur[n % 2, :, cols] = jnp.exp2((old_max - new_max) * scale)
        s_buf[n % 2, t] = scores

    def absorb(n, q, dy, t):
        cols = slice(t * TILE, (t + 1) * TILE)
        rescale = r_cur[n % 2, :, cols]
        weights = jnp.exp2((s_buf[n % 2, t] - m_cur[n % 2, :, cols]) * scale)
        l_run[q, :, cols] = l_run[q, :, cols] * rescale + jnp.sum(weights, axis=0, keepdims=True)
        acc[q, :, cols] = acc[q, :, cols] * rescale + jnp.dot(
            v_t[dy], weights.astype(jnp.bfloat16), preferred_element_type=jnp.float32)

    def finish(q):
        out = acc[q] / l_run[q]
        dst = o_send.at[q]
        for pair in range(group // 2):
            cols = slice(pair * LANES, (pair + 1) * LANES)
            first = 2 * pair * LANES
            both = jnp.concatenate([out[:, first:first + LANES], out[:, first + LANES:first + 2 * LANES]], axis=0)
            dst[:main, cols] = jnp.transpose(both, (1, 0)).astype(jnp.bfloat16)
            ends = out[:, (group + pair) * LANES:(group + pair + 1) * LANES]
            both = jnp.concatenate([ends, pltpu.roll(ends, tail, 1)], axis=0)
            dst[main:, cols] = jnp.transpose(both, (1, 0))[:tail].astype(jnp.bfloat16)
        mine, theirs = o_send.at[q, own_rows], o_send.at[q, other_rows]
        if q == 2:
            remote(mine, o_relay.at[0], o_send_sem.at[0], o_relay_sem.at[0], east).start()
            remote(theirs, o_relay.at[1], o_send_sem.at[0], o_relay_sem.at[1], west).start()
        elif q:
            target = east if q == 1 else west
            remote(mine, o_all.at[0, nx - q], o_send_sem.at[0], o_recv.at[0, nx - q], target).start()
            remote(theirs, o_all.at[1, nx - q], o_send_sem.at[0], o_recv.at[1, nx - q], {**target, **partner}).start()
        else:
            remote(theirs, o_all.at[1, 0], o_send_sem.at[1], o_recv.at[1, 0], partner).start()
            o_all[0, 0] = o_send[0, own_rows]

    events = {n: [] for n in range(len(STEPS) + 1)}
    def row(*dxs):
        return [functools.partial(kv_row, dx) for dx in dxs]

    def side(*pieces):
        return [functools.partial(kv_side, dx, dy) for dx, dy in pieces]

    def query(dx):
        return [functools.partial(q_arrive, dx)]

    events[0] = row(0, 1, 2, 3) + [q_relay_on] + query(1)
    events[1] = side((0, 1), (1, 1)) + query(3) + side((1, 3), (2, 3))
    events[2] = side((0, 3), (2, 1), (3, 1))
    events[4] = query(2) + side((3, 3))
    events[5] = side((1, 2))
    events[8] = side((3, 2), (2, 2), (0, 2))
    events[15] = [o_relay_on]
    last_of = {q: max(n for n, s in enumerate(STEPS) if s[0] == q) for q in range(nx)}
    first_of = {dy: min(n for n, s in enumerate(STEPS) if s[1] == dy) for dy in range(ny)}

    for n in range(len(STEPS) + 1):
        for event in events[n]:
            event()
        if n < len(STEPS) and first_of[STEPS[n][1]] == n:
            dy = STEPS[n][1]
            v_t[dy] = jnp.transpose(keys(dy).astype(jnp.float32), (1, 0))[head_dim:].astype(jnp.bfloat16)
        for t in range(tiles):
            if n < len(STEPS):
                score(n, *STEPS[n], t)
            if n:
                absorb(n - 1, *STEPS[n - 1], t)
        if n and last_of[STEPS[n - 1][0]] == n - 1:
            finish(STEPS[n - 1][0])

    o_load.wait()
    for i, dx in enumerate(O_ORDER):
        total = None
        for r in range(2):
            if dx or r:
                arrive(o_all.at[r, dx], o_recv.at[r, dx])
            first = ((core if r == 0 else other) * kv_local + head_at(dx)) * q_rows
            term = jnp.dot(o_all[r, dx], w_o[pl.ds(pl.multiple_of(first, q_rows), q_rows)],
                           preferred_element_type=jnp.float32)
            total = term if total is None else total + term
        if i == 0:
            y_acc[...] = total
        elif i < nx - 1:
            y_acc[...] += total
        else:
            y_ref[...] = (y_acc[...] + total).astype(jnp.bfloat16)

    for ref, sem in ((kv_buf.at[pl.ds(0, (nx * ny - 1) * chip_tokens)], kv_send.at[0]), (kv_all.at[0], kv_send.at[1]), (q_all, q_send), (o_all, o_send_sem.at[0]), (o_all.at[1, 0], o_send_sem.at[1])):
        remote(ref, ref, sem, x_sem.at[1], partner).wait_send()


def solution(mesh):
    nx, ny = mesh.shape["cx"], mesh.shape["cy"]
    seq_spec = P("dp", ("cy", "cx", "core"))

    def local_layer(x_loc, w_qkv, w_out):
        heads, head_dim, width = w_out.shape
        kv_heads = (w_qkv.shape[1] - heads) // 2
        tokens = x_loc.shape[1]
        kv_local = kv_heads // 2
        group = heads // kv_heads
        q_rows = group * head_dim
        feat = kv_local * q_rows
        rows = group * 2 * tokens
        dims = (nx, ny, heads, kv_heads, head_dim)
        w_rows = jnp.transpose(w_qkv, (1, 2, 0)).reshape(-1, width)
        hbm = pl.BlockSpec(memory_space=pl.ANY)
        half = jnp.bfloat16
        y = pl.pallas_call(
            functools.partial(kernel, dims),
            out_shape=jax.ShapeDtypeStruct((tokens, width), half),
            in_specs=[hbm] * 3,
            out_specs=pl.BlockSpec(memory_space=pltpu.VMEM),
            scratch_shapes=[
                pltpu.VMEM((TILE, width), half),
                pltpu.VMEM((2 * kv_heads * head_dim, width), half),
                pltpu.VMEM((feat, width), half),
                pltpu.VMEM((heads * head_dim, width), half),
                pltpu.VMEM((kv_heads, tokens, LANES), half),
                pltpu.VMEM((ny * nx * 2 * tokens, LANES), half),
                pltpu.VMEM((nx, head_dim, rows), half),
                pltpu.VMEM((nx, LANES, rows), half),
                pltpu.VMEM((2, head_dim // 2, rows), half),
                pltpu.VMEM((ny, head_dim, nx * 2 * tokens), half),
                pltpu.VMEM((2, rows // TILE, nx * 2 * tokens, TILE), jnp.float32),
                pltpu.VMEM((2, 1, rows), jnp.float32),
                pltpu.VMEM((2, 1, rows), jnp.float32),
                pltpu.VMEM((nx, 1, rows), jnp.float32),
                pltpu.VMEM((nx, 1, rows), jnp.float32),
                pltpu.VMEM((nx, head_dim, rows), jnp.float32),
                pltpu.VMEM((nx, 2 * tokens, q_rows), half),
                pltpu.VMEM((2, tokens, q_rows), half),
                pltpu.VMEM((2, nx, tokens, q_rows), half),
                pltpu.VMEM((tokens, width), jnp.float32),
                pltpu.SemaphoreType.DMA((2 + 5 * nx,)),
                pltpu.SemaphoreType.DMA((2,)),
                pltpu.SemaphoreType.DMA((2,)),
                pltpu.SemaphoreType.DMA((ny, nx)),
                pltpu.SemaphoreType.DMA,
                pltpu.SemaphoreType.DMA((nx,)),
                pltpu.SemaphoreType.DMA((2,)),
                pltpu.SemaphoreType.DMA((2,)),
                pltpu.SemaphoreType.DMA((2, nx)),
                pltpu.SemaphoreType.DMA((2,)),
            ],
            compiler_params=pltpu.CompilerParams(
                collective_id=0, has_side_effects=True, vmem_limit_bytes=54600 * 1024),
        )(x_loc[0], w_rows, w_out.reshape(heads * head_dim, width))
        return y[None]

    return jax.shard_map(local_layer, mesh=mesh, in_specs=(seq_spec, P(), P()), out_specs=seq_spec, check_vma=False)
```

```python
import functools
import math

import jax
import jax.numpy as jnp
from jax import lax
from jax.experimental import pallas as pl
from jax.experimental.pallas import tpu as pltpu
from jax.sharding import PartitionSpec as P

MESH = pl.DeviceIdType.MESH
LANES = 128
TILE = 256
NT = (((1,), (1,)), ((), ()))

STEPS = (
    (1, 0), (3, 0), (1, 1), (3, 1), (2, 3), (2, 1), (2, 0), (3, 3),
    (2, 2), (3, 2), (1, 3), (1, 2), (0, 0), (0, 3), (0, 1), (0, 2),
)
FAR_FIRST = (2, 1, 3, 0)
O_ORDER = (3, 0, 1, 2)


def kernel(dims, x_hbm, wqkv_hbm, wout_hbm, y_ref,
           x_ext, w_kv, w_q, w_o, kv_all, kv_buf, q_all, q_t, q_relay,
           v_t, s_buf, m_cur, r_cur, m_run, l_run, acc, o_send, o_all, y_acc,
           load_sem, x_sem, kv_send, kv_recv, q_send, q_recv, q_relay_sem,
           o_send_sem, o_recv):
    nx, ny, heads, kv_heads, head_dim = dims
    dev_tokens = x_hbm.shape[0]
    chip_tokens = 2 * dev_tokens
    row_keys = nx * chip_tokens
    kv_local = kv_heads // 2
    group = heads // kv_heads
    q_rows = group * head_dim
    feat = kv_local * q_rows
    rows = q_t.shape[2]
    tiles = rows // TILE
    main = LANES
    tail = chip_tokens - main
    cx, cy, core = lax.axis_index("cx"), lax.axis_index("cy"), lax.axis_index("core")
    other = 1 - core
    own_rows = pl.ds(pl.multiple_of(core * dev_tokens, 32), dev_tokens)
    other_rows = pl.ds(pl.multiple_of(other * dev_tokens, 32), dev_tokens)
    scale = head_dim ** -0.5 * math.log2(math.e)

    def head_at(dx):
        return lax.rem(cx + dx, nx)

    x_load = pltpu.make_async_copy(x_hbm, x_ext.at[own_rows], load_sem.at[0])
    x_load.start()
    kv_loads, q_loads = [], []
    for i, dx in enumerate(FAR_FIRST):
        for r in range(2):
            head = (core if r == 0 else other) * kv_local + head_at(dx)
            for part in range(2):
                src = pl.multiple_of((heads + part * kv_heads + head) * head_dim, head_dim)
                copy = pltpu.make_async_copy(
                    wqkv_hbm.at[pl.ds(src, head_dim)],
                    w_kv.at[pl.ds((4 * i + 2 * r + part) * head_dim, head_dim)],
                    load_sem.at[1 + 4 * i + 2 * r + part])
                copy.start()
                kv_loads.append(copy)
    for i, dx in enumerate(FAR_FIRST):
        src = pl.multiple_of(core * feat + head_at(dx) * q_rows, q_rows)
        copy = pltpu.make_async_copy(
            wqkv_hbm.at[pl.ds(src, q_rows)], w_q.at[pl.ds(i * q_rows, q_rows)], load_sem.at[1 + 4 * nx + i])
        copy.start()
        q_loads.append(copy)

    east = {"cx": lax.rem(cx + 1, nx)}
    west = {"cx": lax.rem(cx + nx - 1, nx)}
    north = {"cy": lax.rem(cy + 1, ny)}
    south = {"cy": lax.rem(cy + ny - 1, ny)}
    partner = {"core": other}
    across = {"cx": head_at(2)}
    by_dx = {0: {}, 1: east, 2: across, 3: west}
    targets = [partner, north, south]
    for dx in range(1, nx):
        targets += [by_dx[dx], {**by_dx[dx], **partner}]
    barrier = pltpu.get_barrier_semaphore()
    for target in targets:
        pl.semaphore_signal(barrier, inc=1, device_id=target, device_id_type=MESH)
    pl.semaphore_wait(barrier, len(targets))

    def remote(src, dst, send_sem, recv_sem, target):
        return pltpu.make_async_remote_copy(
            src_ref=src, dst_ref=dst, send_sem=send_sem, recv_sem=recv_sem, device_id=target, device_id_type=MESH)

    x_load.wait()
    x_copy = remote(x_ext.at[own_rows], x_ext.at[own_rows], x_sem.at[0], x_sem.at[1], partner)
    x_copy.start()
    q_t[:, head_dim:, :] = jnp.zeros((nx, LANES - head_dim, rows), jnp.bfloat16)
    acc[...] = jnp.zeros_like(acc)
    m_run[...] = jnp.full_like(m_run, -jnp.inf)
    l_run[...] = jnp.zeros_like(l_run)

    def kv_at(dx, dy):
        return dy * row_keys + dx * chip_tokens

    def kv_piece(dx, dy):
        return kv_buf.at[pl.ds(kv_at(dx, dy), chip_tokens)]

    def kv_half(dx, dy, r):
        return kv_buf.at[pl.ds(kv_at(dx, dy) + r * dev_tokens, dev_tokens)]

    def spread(src, dst_of, dx):
        remote(src, dst_of(3), kv_send.at[0], kv_recv.at[3, dx], north).start()
        remote(src, dst_of(1), kv_send.at[0], kv_recv.at[1, dx], south).start()

    for i in range(0, nx, 2):
        for copy in kv_loads[4 * i:4 * i + 8]:
            copy.wait()
        part = lax.dot_general(
            x_ext[own_rows], w_kv[4 * i * head_dim:(4 * i + 8) * head_dim], NT, preferred_element_type=jnp.float32)
        for k in range(4):
            kv_all[2 * i + k] = part[:, k * LANES:(k + 1) * LANES].astype(jnp.bfloat16)
        for k in range(4):
            dx, r = FAR_FIRST[i + k // 2], k % 2
            src = kv_all.at[2 * i + k]
            back = (nx - dx) % nx
            if dx:
                target = {**by_dx[dx], **partner} if r else by_dx[dx]
                remote(src, kv_half(back, 0, r), kv_send.at[0], kv_recv.at[0, back], target).start()
            elif r:
                remote(src, kv_half(0, 0, 1), kv_send.at[1], kv_recv.at[0, 0], partner).start()
            else:
                spread(src, lambda dy: kv_half(0, dy, 0), 0)
                kv_buf[kv_at(0, 0):kv_at(0, 0) + dev_tokens] = kv_all[2 * i + k]
    o_load = pltpu.make_async_copy(wout_hbm, w_o, load_sem.at[1 + 5 * nx])
    o_load.start()

    x_copy.wait()
    x_ext[chip_tokens:chip_tokens + tail] = x_ext[main:chip_tokens]
    lane = lax.broadcasted_iota(jnp.int32, (head_dim, LANES), 1)
    half_dim = head_dim // 2
    for i in range(0, nx, 2):
        results = []
        for k in (i, i + 1):
            q_loads[k].wait()
        for k in (i, i + 1):
            results.append(lax.dot_general(
                w_q[k * q_rows:(k + 1) * q_rows], x_ext[...], NT, preferred_element_type=jnp.float32))
        for k, res in zip((i, i + 1), results):
            dst = q_all.at[FAR_FIRST[k]] if FAR_FIRST[k] else q_t.at[0, pl.ds(0, head_dim)]
            for g in range(group):
                dst[:, g * LANES:(g + 1) * LANES] = res[g * head_dim:(g + 1) * head_dim, :main].astype(jnp.bfloat16)
            for pair in range(group // 2):
                lo = res[2 * pair * head_dim:(2 * pair + 1) * head_dim, main:]
                hi = res[(2 * pair + 1) * head_dim:(2 * pair + 2) * head_dim, main:]
                dst[:, (group + pair) * LANES:(group + pair + 1) * LANES] = (
                    jnp.where(lane < tail, lo, hi).astype(jnp.bfloat16))
        for k in (i, i + 1):
            dx = FAR_FIRST[k]
            if dx == 2:
                for half, target in ((0, east), (1, west)):
                    remote(q_all.at[2, pl.ds(half * half_dim, half_dim)], q_relay.at[half],
                           q_send, q_relay_sem.at[half], target).start()
            elif dx:
                remote(q_all.at[dx], q_t.at[nx - dx, pl.ds(0, head_dim)],
                       q_send, q_recv.at[nx - dx], by_dx[dx]).start()

    def arrive(ref, sem):
        remote(ref, ref, q_send, sem, partner).wait_recv()

    def kv_row(dx):
        if dx:
            arrive(kv_piece(dx, 0), kv_recv.at[0, dx])
            spread(kv_piece(dx, 0), lambda dy: kv_piece(dx, dy), dx)
        else:
            arrive(kv_half(0, 0, 1), kv_recv.at[0, 0])
            spread(kv_half(0, 0, 1), lambda dy: kv_half(0, dy, 1), 0)

    def kv_side(dx, dy):
        arrive(kv_piece(dx, dy), kv_recv.at[dy, dx])
        if dy == 3 and dx % 2 == 0:
            remote(kv_piece(dx, 3), kv_piece(dx, 2), kv_send.at[0], kv_recv.at[2, dx], north).start()
        if dy == 1 and dx % 2 == 1:
            remote(kv_piece(dx, 1), kv_piece(dx, 2), kv_send.at[0], kv_recv.at[2, dx], south).start()

    def q_relay_on():
        for half, target in ((0, east), (1, west)):
            arrive(q_relay.at[half], q_relay_sem.at[half])
            remote(q_relay.at[half], q_t.at[2, pl.ds(half * half_dim, half_dim)],
                   q_send, q_recv.at[2], target).start()

    def q_arrive(dx):
        arrive(q_t.at[dx, pl.ds(0, head_dim)], q_recv.at[dx])

    def keys(dy):
        return kv_buf[kv_at(0, dy):kv_at(0, dy) + row_keys]

    def score(n, q, dy, t):
        cols = slice(t * TILE, (t + 1) * TILE)
        scores = jnp.dot(keys(dy), q_t[q, :, cols], preferred_element_type=jnp.float32)
        old_max = m_run[q, :, cols]
        new_max = jnp.maximum(old_max, jnp.max(scores, axis=0, keepdims=True))
        m_run[q, :, cols] = new_max
        m_cur[n % 2, :, cols] = new_max
        r_cur[n % 2, :, cols] = jnp.exp2((old_max - new_max) * scale)
        s_buf[n % 2, t] = scores

    def absorb(n, q, dy, t):
        cols = slice(t * TILE, (t + 1) * TILE)
        rescale = r_cur[n % 2, :, cols]
        weights = jnp.exp2((s_buf[n % 2, t] - m_cur[n % 2, :, cols]) * scale)
        l_run[q, :, cols] = l_run[q, :, cols] * rescale + jnp.sum(weights, axis=0, keepdims=True)
        acc[q, :, cols] = acc[q, :, cols] * rescale + jnp.dot(
            v_t[dy], weights.astype(jnp.bfloat16), preferred_element_type=jnp.float32)

    def finish(q):
        out = acc[q] / l_run[q]
        dst = o_send.at[q]
        for pair in range(group // 2):
            cols = slice(pair * LANES, (pair + 1) * LANES)
            first = 2 * pair * LANES
            both = jnp.concatenate([out[:, first:first + LANES], out[:, first + LANES:first + 2 * LANES]], axis=0)
            dst[:main, cols] = jnp.transpose(both, (1, 0)).astype(jnp.bfloat16)
            ends = out[:, (group + pair) * LANES:(group + pair + 1) * LANES]
            both = jnp.concatenate([ends, pltpu.roll(ends, tail, 1)], axis=0)
            dst[main:, cols] = jnp.transpose(both, (1, 0))[:tail].astype(jnp.bfloat16)
        mine, theirs = o_send.at[q, own_rows], o_send.at[q, other_rows]
        if q:
            target = by_dx[q]
            remote(mine, o_all.at[0, nx - q], o_send_sem.at[0], o_recv.at[0, nx - q], target).start()
            remote(theirs, o_all.at[1, nx - q], o_send_sem.at[0], o_recv.at[1, nx - q], {**target, **partner}).start()
        else:
            remote(theirs, o_all.at[1, 0], o_send_sem.at[1], o_recv.at[1, 0], partner).start()
            o_all[0, 0] = o_send[0, own_rows]

    events = {n: [] for n in range(len(STEPS) + 1)}
    def row(*dxs):
        return [functools.partial(kv_row, dx) for dx in dxs]

    def side(*pieces):
        return [functools.partial(kv_side, dx, dy) for dx, dy in pieces]

    def query(dx):
        return [functools.partial(q_arrive, dx)]

    events[0] = row(0, 1, 2, 3) + [q_relay_on] + query(1)
    events[1] = side((0, 1), (1, 1)) + query(3) + side((1, 3), (2, 3))
    events[2] = side((0, 3), (2, 1), (3, 1))
    events[4] = query(2) + side((3, 3))
    events[5] = side((1, 2))
    events[8] = side((3, 2), (2, 2), (0, 2))
    last_of = {q: max(n for n, s in enumerate(STEPS) if s[0] == q) for q in range(nx)}
    first_of = {dy: min(n for n, s in enumerate(STEPS) if s[1] == dy) for dy in range(ny)}

    for n in range(len(STEPS) + 1):
        for event in events[n]:
            event()
        if n < len(STEPS) and first_of[STEPS[n][1]] == n:
            dy = STEPS[n][1]
            v_t[dy] = jnp.transpose(keys(dy).astype(jnp.float32), (1, 0))[head_dim:].astype(jnp.bfloat16)
        for t in range(tiles):
            if n < len(STEPS):
                score(n, *STEPS[n], t)
            if n:
                absorb(n - 1, *STEPS[n - 1], t)
        if n and last_of[STEPS[n - 1][0]] == n - 1:
            finish(STEPS[n - 1][0])

    o_load.wait()
    for i, dx in enumerate(O_ORDER):
        total = None
        for r in range(2):
            if dx or r:
                arrive(o_all.at[r, dx], o_recv.at[r, dx])
            first = ((core if r == 0 else other) * kv_local + head_at(dx)) * q_rows
            term = jnp.dot(o_all[r, dx], w_o[pl.ds(pl.multiple_of(first, q_rows), q_rows)],
                           preferred_element_type=jnp.float32)
            total = term if total is None else total + term
        if i == 0:
            y_acc[...] = total
        elif i < nx - 1:
            y_acc[...] += total
        else:
            y_ref[...] = (y_acc[...] + total).astype(jnp.bfloat16)

    for ref, sem in ((kv_buf.at[pl.ds(0, (nx * ny - 1) * chip_tokens)], kv_send.at[0]), (kv_all.at[0], kv_send.at[1]), (q_all, q_send), (o_all.at[:, pl.ds(0, nx - 1)], o_send_sem.at[0]), (o_all.at[1, 0], o_send_sem.at[1])):
        remote(ref, ref, sem, x_sem.at[1], partner).wait_send()


def solution(mesh):
    nx, ny = mesh.shape["cx"], mesh.shape["cy"]
    seq_spec = P("dp", ("cy", "cx", "core"))

    def local_layer(x_loc, w_qkv, w_out):
        heads, head_dim, width = w_out.shape
        kv_heads = (w_qkv.shape[1] - heads) // 2
        tokens = x_loc.shape[1]
        kv_local = kv_heads // 2
        group = heads // kv_heads
        q_rows = group * head_dim
        feat = kv_local * q_rows
        rows = group * 2 * tokens
        dims = (nx, ny, heads, kv_heads, head_dim)
        w_rows = jnp.transpose(w_qkv, (1, 2, 0)).reshape(-1, width)
        hbm = pl.BlockSpec(memory_space=pl.ANY)
        half = jnp.bfloat16
        y = pl.pallas_call(
            functools.partial(kernel, dims),
            out_shape=jax.ShapeDtypeStruct((tokens, width), half),
            in_specs=[hbm] * 3,
            out_specs=pl.BlockSpec(memory_space=pltpu.VMEM),
            scratch_shapes=[
                pltpu.VMEM((TILE, width), half),
                pltpu.VMEM((2 * kv_heads * head_dim, width), half),
                pltpu.VMEM((feat, width), half),
                pltpu.VMEM((heads * head_dim, width), half),
                pltpu.VMEM((kv_heads, tokens, LANES), half),
                pltpu.VMEM((ny * nx * 2 * tokens, LANES), half),
                pltpu.VMEM((nx, head_dim, rows), half),
                pltpu.VMEM((nx, LANES, rows), half),
                pltpu.VMEM((2, head_dim // 2, rows), half),
                pltpu.VMEM((ny, head_dim, nx * 2 * tokens), half),
                pltpu.VMEM((2, rows // TILE, nx * 2 * tokens, TILE), jnp.float32),
                pltpu.VMEM((2, 1, rows), jnp.float32),
                pltpu.VMEM((2, 1, rows), jnp.float32),
                pltpu.VMEM((nx, 1, rows), jnp.float32),
                pltpu.VMEM((nx, 1, rows), jnp.float32),
                pltpu.VMEM((nx, head_dim, rows), jnp.float32),
                pltpu.VMEM((nx, 2 * tokens, q_rows), half),
                pltpu.VMEM((2, nx, tokens, q_rows), half),
                pltpu.VMEM((tokens, width), jnp.float32),
                pltpu.SemaphoreType.DMA((2 + 5 * nx,)),
                pltpu.SemaphoreType.DMA((2,)),
                pltpu.SemaphoreType.DMA((2,)),
                pltpu.SemaphoreType.DMA((ny, nx)),
                pltpu.SemaphoreType.DMA,
                pltpu.SemaphoreType.DMA((nx,)),
                pltpu.SemaphoreType.DMA((2,)),
                pltpu.SemaphoreType.DMA((2,)),
                pltpu.SemaphoreType.DMA((2, nx)),
            ],
            compiler_params=pltpu.CompilerParams(
                collective_id=0, has_side_effects=True, vmem_limit_bytes=54600 * 1024),
        )(x_loc[0], w_rows, w_out.reshape(heads * head_dim, width))
        return y[None]

    return jax.shard_map(local_layer, mesh=mesh, in_specs=(seq_spec, P(), P()), out_specs=seq_spec, check_vma=False)
```

```python
import functools
import math

import jax
import jax.numpy as jnp
from jax import lax
from jax.experimental import pallas as pl
from jax.experimental.pallas import tpu as pltpu
from jax.sharding import PartitionSpec as P

MESH = pl.DeviceIdType.MESH
LANES = 128
TILE = 256
NT = (((1,), (1,)), ((), ()))

STEPS = (
    (0, 0), (1, 0), (3, 0), (1, 1), (2, 3), (2, 0), (1, 3), (2, 1),
    (2, 2), (3, 2), (1, 2), (3, 3), (3, 1), (0, 3), (0, 1), (0, 2),
)
FAR_FIRST = (2, 1, 3, 0)
Q_ORDER = (1, 3, 2, 0)
O_ORDER = (3, 0, 1, 2)


def kernel(dims, x_hbm, wqkv_hbm, wout_hbm, y_ref,
           x_ext, w_kv, w_q, w_o, kv_all, kv_buf, q_all, q_t,
           v_t, s_buf, m_cur, r_cur, m_run, l_run, acc, o_send, o_all, y_acc,
           load_sem, x_sem, kv_send, kv_recv, q_send, q_recv,
           o_send_sem, o_recv):
    nx, ny, heads, kv_heads, head_dim = dims
    dev_tokens = x_hbm.shape[0]
    chip_tokens = 2 * dev_tokens
    row_keys = nx * chip_tokens
    kv_local = kv_heads // 2
    group = heads // kv_heads
    q_rows = group * head_dim
    feat = kv_local * q_rows
    rows = q_t.shape[2]
    tiles = rows // TILE
    main = LANES
    tail = chip_tokens - main
    cx, cy, core = lax.axis_index("cx"), lax.axis_index("cy"), lax.axis_index("core")
    other = 1 - core
    own_rows = pl.ds(pl.multiple_of(core * dev_tokens, 32), dev_tokens)
    other_rows = pl.ds(pl.multiple_of(other * dev_tokens, 32), dev_tokens)
    scale = head_dim ** -0.5 * math.log2(math.e)

    def head_at(dx):
        return lax.rem(cx + dx, nx)

    x_load = pltpu.make_async_copy(x_hbm, x_ext.at[own_rows], load_sem.at[0])
    x_load.start()
    kv_loads, q_loads = [], []
    for i, dx in enumerate(FAR_FIRST):
        for r in range(2):
            head = (core if r == 0 else other) * kv_local + head_at(dx)
            for part in range(2):
                src = pl.multiple_of((heads + part * kv_heads + head) * head_dim, head_dim)
                copy = pltpu.make_async_copy(
                    wqkv_hbm.at[pl.ds(src, head_dim)],
                    w_kv.at[pl.ds((4 * i + 2 * r + part) * head_dim, head_dim)],
                    load_sem.at[1 + 4 * i + 2 * r + part])
                copy.start()
                kv_loads.append(copy)
    for i, dx in enumerate(Q_ORDER):
        src = pl.multiple_of(core * feat + head_at(dx) * q_rows, q_rows)
        copy = pltpu.make_async_copy(
            wqkv_hbm.at[pl.ds(src, q_rows)], w_q.at[pl.ds(i * q_rows, q_rows)], load_sem.at[1 + 4 * nx + i])
        copy.start()
        q_loads.append(copy)

    east = {"cx": lax.rem(cx + 1, nx)}
    west = {"cx": lax.rem(cx + nx - 1, nx)}
    north = {"cy": lax.rem(cy + 1, ny)}
    south = {"cy": lax.rem(cy + ny - 1, ny)}
    partner = {"core": other}
    across = {"cx": head_at(2)}
    by_dx = {0: {}, 1: east, 2: across, 3: west}
    targets = [partner, north, south]
    for dx in range(1, nx):
        targets += [by_dx[dx], {**by_dx[dx], **partner}]
    barrier = pltpu.get_barrier_semaphore()
    for target in targets:
        pl.semaphore_signal(barrier, inc=1, device_id=target, device_id_type=MESH)
    pl.semaphore_wait(barrier, len(targets))

    def remote(src, dst, send_sem, recv_sem, target):
        return pltpu.make_async_remote_copy(
            src_ref=src, dst_ref=dst, send_sem=send_sem, recv_sem=recv_sem, device_id=target, device_id_type=MESH)

    x_load.wait()
    x_copy = remote(x_ext.at[own_rows], x_ext.at[own_rows], x_sem.at[0], x_sem.at[1], partner)
    x_copy.start()
    q_t[:, head_dim:, :] = jnp.zeros((nx, LANES - head_dim, rows), jnp.bfloat16)
    acc[...] = jnp.zeros_like(acc)
    m_run[...] = jnp.full_like(m_run, -jnp.inf)
    l_run[...] = jnp.zeros_like(l_run)

    def kv_at(dx, dy):
        return dy * row_keys + dx * chip_tokens

    def kv_piece(dx, dy):
        return kv_buf.at[pl.ds(kv_at(dx, dy), chip_tokens)]

    def kv_half(dx, dy, r):
        return kv_buf.at[pl.ds(kv_at(dx, dy) + r * dev_tokens, dev_tokens)]

    def spread(src, dst_of, dx):
        remote(src, dst_of(3), kv_send.at[0], kv_recv.at[3, dx], north).start()
        remote(src, dst_of(1), kv_send.at[0], kv_recv.at[1, dx], south).start()

    for i in range(0, nx, 2):
        for copy in kv_loads[4 * i:4 * i + 8]:
            copy.wait()
        part = lax.dot_general(
            x_ext[own_rows], w_kv[4 * i * head_dim:(4 * i + 8) * head_dim], NT, preferred_element_type=jnp.float32)
        for k in range(4):
            kv_all[2 * i + k] = part[:, k * LANES:(k + 1) * LANES].astype(jnp.bfloat16)
        for k in range(4):
            dx, r = FAR_FIRST[i + k // 2], k % 2
            src = kv_all.at[2 * i + k]
            back = (nx - dx) % nx
            if dx:
                target = {**by_dx[dx], **partner} if r else by_dx[dx]
                remote(src, kv_half(back, 0, r), kv_send.at[0], kv_recv.at[0, back], target).start()
            elif r:
                remote(src, kv_half(0, 0, 1), kv_send.at[1], kv_recv.at[0, 0], partner).start()
            else:
                spread(src, lambda dy: kv_half(0, dy, 0), 0)
                kv_buf[kv_at(0, 0):kv_at(0, 0) + dev_tokens] = kv_all[2 * i + k]
    o_load = pltpu.make_async_copy(wout_hbm, w_o, load_sem.at[1 + 5 * nx])
    o_load.start()

    x_copy.wait()
    x_ext[chip_tokens:chip_tokens + tail] = x_ext[main:chip_tokens]
    lane = lax.broadcasted_iota(jnp.int32, (head_dim, LANES), 1)
    for i in range(0, nx, 2):
        results = []
        for k in (i, i + 1):
            q_loads[k].wait()
        for k in (i, i + 1):
            results.append(lax.dot_general(
                w_q[k * q_rows:(k + 1) * q_rows], x_ext[...], NT, preferred_element_type=jnp.float32))
        for k, res in zip((i, i + 1), results):
            dst = q_all.at[Q_ORDER[k]] if Q_ORDER[k] else q_t.at[0, pl.ds(0, head_dim)]
            for g in range(group):
                dst[:, g * LANES:(g + 1) * LANES] = res[g * head_dim:(g + 1) * head_dim, :main].astype(jnp.bfloat16)
            for pair in range(group // 2):
                lo = res[2 * pair * head_dim:(2 * pair + 1) * head_dim, main:]
                hi = res[(2 * pair + 1) * head_dim:(2 * pair + 2) * head_dim, main:]
                dst[:, (group + pair) * LANES:(group + pair + 1) * LANES] = (
                    jnp.where(lane < tail, lo, hi).astype(jnp.bfloat16))
        for k in (i, i + 1):
            dx = Q_ORDER[k]
            if dx:
                remote(q_all.at[dx], q_t.at[nx - dx, pl.ds(0, head_dim)],
                       q_send, q_recv.at[nx - dx], by_dx[dx]).start()

    def arrive(ref, sem):
        remote(ref, ref, q_send, sem, partner).wait_recv()

    def kv_row(dx):
        if dx:
            arrive(kv_piece(dx, 0), kv_recv.at[0, dx])
            spread(kv_piece(dx, 0), lambda dy: kv_piece(dx, dy), dx)
        else:
            arrive(kv_half(0, 0, 1), kv_recv.at[0, 0])
            spread(kv_half(0, 0, 1), lambda dy: kv_half(0, dy, 1), 0)

    def kv_side(dx, dy):
        arrive(kv_piece(dx, dy), kv_recv.at[dy, dx])
        if dy == 3 and dx % 2 == 0:
            remote(kv_piece(dx, 3), kv_piece(dx, 2), kv_send.at[0], kv_recv.at[2, dx], north).start()
        if dy == 1 and dx % 2 == 1:
            remote(kv_piece(dx, 1), kv_piece(dx, 2), kv_send.at[0], kv_recv.at[2, dx], south).start()

    def q_arrive(dx):
        arrive(q_t.at[dx, pl.ds(0, head_dim)], q_recv.at[dx])

    def keys(dy):
        return kv_buf[kv_at(0, dy):kv_at(0, dy) + row_keys]

    def score(n, q, dy, t):
        cols = slice(t * TILE, (t + 1) * TILE)
        scores = jnp.dot(keys(dy), q_t[q, :, cols], preferred_element_type=jnp.float32)
        old_max = m_run[q, :, cols]
        new_max = jnp.maximum(old_max, jnp.max(scores, axis=0, keepdims=True))
        m_run[q, :, cols] = new_max
        m_cur[n % 2, :, cols] = new_max
        r_cur[n % 2, :, cols] = jnp.exp2((old_max - new_max) * scale)
        s_buf[n % 2, t] = scores

    def absorb(n, q, dy, t):
        cols = slice(t * TILE, (t + 1) * TILE)
        rescale = r_cur[n % 2, :, cols]
        weights = jnp.exp2((s_buf[n % 2, t] - m_cur[n % 2, :, cols]) * scale)
        l_run[q, :, cols] = l_run[q, :, cols] * rescale + jnp.sum(weights, axis=0, keepdims=True)
        acc[q, :, cols] = acc[q, :, cols] * rescale + jnp.dot(
            v_t[dy], weights.astype(jnp.bfloat16), preferred_element_type=jnp.float32)

    def finish(q):
        out = acc[q] / l_run[q]
        dst = o_send.at[q]
        for pair in range(group // 2):
            cols = slice(pair * LANES, (pair + 1) * LANES)
            first = 2 * pair * LANES
            both = jnp.concatenate([out[:, first:first + LANES], out[:, first + LANES:first + 2 * LANES]], axis=0)
            dst[:main, cols] = jnp.transpose(both, (1, 0)).astype(jnp.bfloat16)
            ends = out[:, (group + pair) * LANES:(group + pair + 1) * LANES]
            both = jnp.concatenate([ends, pltpu.roll(ends, tail, 1)], axis=0)
            dst[main:, cols] = jnp.transpose(both, (1, 0))[:tail].astype(jnp.bfloat16)
        mine, theirs = o_send.at[q, own_rows], o_send.at[q, other_rows]
        if q:
            target = by_dx[q]
            remote(mine, o_all.at[0, nx - q], o_send_sem.at[0], o_recv.at[0, nx - q], target).start()
            remote(theirs, o_all.at[1, nx - q], o_send_sem.at[0], o_recv.at[1, nx - q], {**target, **partner}).start()
        else:
            remote(theirs, o_all.at[1, 0], o_send_sem.at[1], o_recv.at[1, 0], partner).start()
            o_all[0, 0] = o_send[0, own_rows]

    events = {n: [] for n in range(len(STEPS) + 1)}
    def row(*dxs):
        return [functools.partial(kv_row, dx) for dx in dxs]

    def side(*pieces):
        return [functools.partial(kv_side, dx, dy) for dx, dy in pieces]

    def query(dx):
        return [functools.partial(q_arrive, dx)]

    events[0] = row(0, 2, 1, 3)
    events[1] = side((0, 1)) + query(1)
    events[2] = side((2, 3)) + query(3)
    events[3] = side((1, 1), (2, 1), (0, 3), (3, 1))
    events[4] = side((3, 3), (1, 3)) + query(2)
    events[8] = side((0, 2), (1, 2), (2, 2), (3, 2))
    last_of = {q: max(n for n, s in enumerate(STEPS) if s[0] == q) for q in range(nx)}
    first_of = {dy: min(n for n, s in enumerate(STEPS) if s[1] == dy) for dy in range(ny)}

    for n in range(len(STEPS) + 1):
        for event in events[n]:
            event()
        if n < len(STEPS) and first_of[STEPS[n][1]] == n:
            dy = STEPS[n][1]
            v_t[dy] = jnp.transpose(keys(dy).astype(jnp.float32), (1, 0))[head_dim:].astype(jnp.bfloat16)
        for t in range(tiles):
            if n < len(STEPS):
                score(n, *STEPS[n], t)
            if n:
                absorb(n - 1, *STEPS[n - 1], t)
        if n and last_of[STEPS[n - 1][0]] == n - 1:
            finish(STEPS[n - 1][0])

    o_load.wait()
    for i, dx in enumerate(O_ORDER):
        total = None
        for r in range(2):
            if dx or r:
                arrive(o_all.at[r, dx], o_recv.at[r, dx])
            first = ((core if r == 0 else other) * kv_local + head_at(dx)) * q_rows
            term = jnp.dot(o_all[r, dx], w_o[pl.ds(pl.multiple_of(first, q_rows), q_rows)],
                           preferred_element_type=jnp.float32)
            total = term if total is None else total + term
        if i == 0:
            y_acc[...] = total
        elif i < nx - 1:
            y_acc[...] += total
        else:
            y_ref[...] = (y_acc[...] + total).astype(jnp.bfloat16)

    for ref, sem in ((kv_buf.at[pl.ds(0, (nx * ny - 1) * chip_tokens)], kv_send.at[0]), (kv_all.at[0], kv_send.at[1]), (q_all.at[pl.ds(0, nx - 1)], q_send), (o_all.at[:, pl.ds(0, nx - 1)], o_send_sem.at[0]), (o_all.at[1, 0], o_send_sem.at[1])):
        remote(ref, ref, sem, x_sem.at[1], partner).wait_send()


def solution(mesh):
    nx, ny = mesh.shape["cx"], mesh.shape["cy"]
    seq_spec = P("dp", ("cy", "cx", "core"))

    def local_layer(x_loc, w_qkv, w_out):
        heads, head_dim, width = w_out.shape
        kv_heads = (w_qkv.shape[1] - heads) // 2
        tokens = x_loc.shape[1]
        kv_local = kv_heads // 2
        group = heads // kv_heads
        q_rows = group * head_dim
        feat = kv_local * q_rows
        rows = group * 2 * tokens
        dims = (nx, ny, heads, kv_heads, head_dim)
        w_rows = jnp.transpose(w_qkv, (1, 2, 0)).reshape(-1, width)
        hbm = pl.BlockSpec(memory_space=pl.ANY)
        half = jnp.bfloat16
        y = pl.pallas_call(
            functools.partial(kernel, dims),
            out_shape=jax.ShapeDtypeStruct((tokens, width), half),
            in_specs=[hbm] * 3,
            out_specs=pl.BlockSpec(memory_space=pltpu.VMEM),
            scratch_shapes=[
                pltpu.VMEM((TILE, width), half),
                pltpu.VMEM((2 * kv_heads * head_dim, width), half),
                pltpu.VMEM((feat, width), half),
                pltpu.VMEM((heads * head_dim, width), half),
                pltpu.VMEM((kv_heads, tokens, LANES), half),
                pltpu.VMEM((ny * nx * 2 * tokens, LANES), half),
                pltpu.VMEM((nx, head_dim, rows), half),
                pltpu.VMEM((nx, LANES, rows), half),
                pltpu.VMEM((ny, head_dim, nx * 2 * tokens), half),
                pltpu.VMEM((2, rows // TILE, nx * 2 * tokens, TILE), jnp.float32),
                pltpu.VMEM((2, 1, rows), jnp.float32),
                pltpu.VMEM((2, 1, rows), jnp.float32),
                pltpu.VMEM((nx, 1, rows), jnp.float32),
                pltpu.VMEM((nx, 1, rows), jnp.float32),
                pltpu.VMEM((nx, head_dim, rows), jnp.float32),
                pltpu.VMEM((nx, 2 * tokens, q_rows), half),
                pltpu.VMEM((2, nx, tokens, q_rows), half),
                pltpu.VMEM((tokens, width), jnp.float32),
                pltpu.SemaphoreType.DMA((2 + 5 * nx,)),
                pltpu.SemaphoreType.DMA((2,)),
                pltpu.SemaphoreType.DMA((2,)),
                pltpu.SemaphoreType.DMA((ny, nx)),
                pltpu.SemaphoreType.DMA,
                pltpu.SemaphoreType.DMA((nx,)),
                pltpu.SemaphoreType.DMA((2,)),
                pltpu.SemaphoreType.DMA((2, nx)),
            ],
            compiler_params=pltpu.CompilerParams(
                collective_id=0, has_side_effects=True, vmem_limit_bytes=54600 * 1024),
        )(x_loc[0], w_rows, w_out.reshape(heads * head_dim, width))
        return y[None]

    return jax.shard_map(local_layer, mesh=mesh, in_specs=(seq_spec, P(), P()), out_specs=seq_spec, check_vma=False)
```

```python
import functools
import math

import jax
import jax.numpy as jnp
from jax import lax
from jax.experimental import pallas as pl
from jax.experimental.pallas import tpu as pltpu
from jax.sharding import PartitionSpec as P

MESH = pl.DeviceIdType.MESH
LANES = 128
TILE = 256
NT = (((1,), (1,)), ((), ()))

STEPS = (
    (0, 0), (1, 0), (3, 0), (1, 1), (2, 3), (2, 0), (1, 3), (2, 1),
    (2, 2), (3, 2), (1, 2), (3, 3), (3, 1), (0, 3), (0, 1), (0, 2),
)
FAR_FIRST = (2, 1, 3, 0)
Q_ORDER = (1, 3, 2, 0)
O_ORDER = (3, 0, 1, 2)


def kernel(dims, x_hbm, wqkv_hbm, wout_hbm, y_ref,
           x_ext, w_kv, w_q, w_o, kv_all, kv_buf, q_all, q_t,
           v_t, s_buf, m_cur, r_cur, m_run, l_run, acc, o_send, o_all, y_acc,
           load_sem, x_sem, kv_send, kv_recv, q_send, q_recv,
           o_send_sem, o_recv):
    nx, ny, heads, kv_heads, head_dim = dims
    dev_tokens = x_hbm.shape[0]
    chip_tokens = 2 * dev_tokens
    row_keys = nx * chip_tokens
    kv_local = kv_heads // 2
    group = heads // kv_heads
    q_rows = group * head_dim
    feat = kv_local * q_rows
    rows = q_t.shape[2]
    tiles = rows // TILE
    main = LANES
    tail = chip_tokens - main
    cx, cy, core = lax.axis_index("cx"), lax.axis_index("cy"), lax.axis_index("core")
    other = 1 - core
    own_rows = pl.ds(pl.multiple_of(core * dev_tokens, 32), dev_tokens)
    other_rows = pl.ds(pl.multiple_of(other * dev_tokens, 32), dev_tokens)
    scale = head_dim ** -0.5 * math.log2(math.e)

    def head_at(dx):
        return lax.rem(cx + dx, nx)

    x_load = pltpu.make_async_copy(x_hbm, x_ext.at[own_rows], load_sem.at[0])
    x_load.start()
    kv_loads, q_loads = [], []
    for i, dx in enumerate(FAR_FIRST):
        for r in range(2):
            head = (core if r == 0 else other) * kv_local + head_at(dx)
            for part in range(2):
                src = pl.multiple_of((heads + part * kv_heads + head) * head_dim, head_dim)
                copy = pltpu.make_async_copy(
                    wqkv_hbm.at[pl.ds(src, head_dim)],
                    w_kv.at[pl.ds((4 * i + 2 * r + part) * head_dim, head_dim)],
                    load_sem.at[1 + 4 * i + 2 * r + part])
                copy.start()
                kv_loads.append(copy)
    for i, dx in enumerate(Q_ORDER):
        src = pl.multiple_of(core * feat + head_at(dx) * q_rows, q_rows)
        copy = pltpu.make_async_copy(
            wqkv_hbm.at[pl.ds(src, q_rows)], w_q.at[pl.ds(i * q_rows, q_rows)], load_sem.at[1 + 4 * nx + i])
        q_loads.append(copy)

    east = {"cx": lax.rem(cx + 1, nx)}
    west = {"cx": lax.rem(cx + nx - 1, nx)}
    north = {"cy": lax.rem(cy + 1, ny)}
    south = {"cy": lax.rem(cy + ny - 1, ny)}
    partner = {"core": other}
    across = {"cx": head_at(2)}
    by_dx = {0: {}, 1: east, 2: across, 3: west}
    targets = [partner, north, south]
    for dx in range(1, nx):
        targets += [by_dx[dx], {**by_dx[dx], **partner}]
    barrier = pltpu.get_barrier_semaphore()
    for target in targets:
        pl.semaphore_signal(barrier, inc=1, device_id=target, device_id_type=MESH)
    pl.semaphore_wait(barrier, len(targets))

    def remote(src, dst, send_sem, recv_sem, target):
        return pltpu.make_async_remote_copy(
            src_ref=src, dst_ref=dst, send_sem=send_sem, recv_sem=recv_sem, device_id=target, device_id_type=MESH)

    x_load.wait()
    x_copy = remote(x_ext.at[own_rows], x_ext.at[own_rows], x_sem.at[0], x_sem.at[1], partner)
    x_copy.start()
    q_t[:, head_dim:, :] = jnp.zeros((nx, LANES - head_dim, rows), jnp.bfloat16)
    acc[...] = jnp.zeros_like(acc)
    m_run[...] = jnp.full_like(m_run, -jnp.inf)
    l_run[...] = jnp.zeros_like(l_run)

    def kv_at(dx, dy):
        return dy * row_keys + dx * chip_tokens

    def kv_piece(dx, dy):
        return kv_buf.at[pl.ds(kv_at(dx, dy), chip_tokens)]

    def kv_half(dx, dy, r):
        return kv_buf.at[pl.ds(kv_at(dx, dy) + r * dev_tokens, dev_tokens)]

    def spread(src, dst_of, dx):
        remote(src, dst_of(3), kv_send.at[0], kv_recv.at[3, dx], north).start()
        remote(src, dst_of(1), kv_send.at[0], kv_recv.at[1, dx], south).start()

    for i in range(0, nx, 2):
        for copy in kv_loads[4 * i:4 * i + 8]:
            copy.wait()
        for copy in q_loads[i:i + 2]:
            copy.start()
        part = lax.dot_general(
            x_ext[own_rows], w_kv[4 * i * head_dim:(4 * i + 8) * head_dim], NT, preferred_element_type=jnp.float32)
        for k in range(4):
            kv_all[2 * i + k] = part[:, k * LANES:(k + 1) * LANES].astype(jnp.bfloat16)
        for k in range(4):
            dx, r = FAR_FIRST[i + k // 2], k % 2
            src = kv_all.at[2 * i + k]
            back = (nx - dx) % nx
            if dx:
                target = {**by_dx[dx], **partner} if r else by_dx[dx]
                remote(src, kv_half(back, 0, r), kv_send.at[0], kv_recv.at[0, back], target).start()
            elif r:
                remote(src, kv_half(0, 0, 1), kv_send.at[1], kv_recv.at[0, 0], partner).start()
            else:
                spread(src, lambda dy: kv_half(0, dy, 0), 0)
                kv_buf[kv_at(0, 0):kv_at(0, 0) + dev_tokens] = kv_all[2 * i + k]
    o_load = pltpu.make_async_copy(wout_hbm, w_o, load_sem.at[1 + 5 * nx])
    o_load.start()

    x_copy.wait()
    x_ext[chip_tokens:chip_tokens + tail] = x_ext[main:chip_tokens]
    lane = lax.broadcasted_iota(jnp.int32, (head_dim, LANES), 1)
    for i in range(0, nx, 2):
        results = []
        for k in (i, i + 1):
            q_loads[k].wait()
        for k in (i, i + 1):
            results.append(lax.dot_general(
                w_q[k * q_rows:(k + 1) * q_rows], x_ext[...], NT, preferred_element_type=jnp.float32))
        for k, res in zip((i, i + 1), results):
            dst = q_all.at[Q_ORDER[k]] if Q_ORDER[k] else q_t.at[0, pl.ds(0, head_dim)]
            for g in range(group):
                dst[:, g * LANES:(g + 1) * LANES] = res[g * head_dim:(g + 1) * head_dim, :main].astype(jnp.bfloat16)
            for pair in range(group // 2):
                lo = res[2 * pair * head_dim:(2 * pair + 1) * head_dim, main:]
                hi = res[(2 * pair + 1) * head_dim:(2 * pair + 2) * head_dim, main:]
                dst[:, (group + pair) * LANES:(group + pair + 1) * LANES] = (
                    jnp.where(lane < tail, lo, hi).astype(jnp.bfloat16))
        for k in (i, i + 1):
            dx = Q_ORDER[k]
            if dx:
                remote(q_all.at[dx], q_t.at[nx - dx, pl.ds(0, head_dim)],
                       q_send, q_recv.at[nx - dx], by_dx[dx]).start()

    def arrive(ref, sem):
        remote(ref, ref, q_send, sem, partner).wait_recv()

    def kv_row(dx):
        if dx:
            arrive(kv_piece(dx, 0), kv_recv.at[0, dx])
            spread(kv_piece(dx, 0), lambda dy: kv_piece(dx, dy), dx)
        else:
            arrive(kv_half(0, 0, 1), kv_recv.at[0, 0])
            spread(kv_half(0, 0, 1), lambda dy: kv_half(0, dy, 1), 0)

    def kv_side(dx, dy):
        arrive(kv_piece(dx, dy), kv_recv.at[dy, dx])
        if dy == 3 and dx % 2 == 0:
            remote(kv_piece(dx, 3), kv_piece(dx, 2), kv_send.at[0], kv_recv.at[2, dx], north).start()
        if dy == 1 and dx % 2 == 1:
            remote(kv_piece(dx, 1), kv_piece(dx, 2), kv_send.at[0], kv_recv.at[2, dx], south).start()

    def q_arrive(dx):
        arrive(q_t.at[dx, pl.ds(0, head_dim)], q_recv.at[dx])

    def keys(dy):
        return kv_buf[kv_at(0, dy):kv_at(0, dy) + row_keys]

    def score(n, q, dy, t):
        cols = slice(t * TILE, (t + 1) * TILE)
        scores = jnp.dot(keys(dy), q_t[q, :, cols], preferred_element_type=jnp.float32)
        old_max = m_run[q, :, cols]
        new_max = jnp.maximum(old_max, jnp.max(scores, axis=0, keepdims=True))
        m_run[q, :, cols] = new_max
        m_cur[n % 2, :, cols] = new_max
        r_cur[n % 2, :, cols] = jnp.exp2((old_max - new_max) * scale)
        s_buf[n % 2, t] = scores

    def absorb(n, q, dy, t):
        cols = slice(t * TILE, (t + 1) * TILE)
        rescale = r_cur[n % 2, :, cols]
        weights = jnp.exp2((s_buf[n % 2, t] - m_cur[n % 2, :, cols]) * scale)
        l_run[q, :, cols] = l_run[q, :, cols] * rescale + jnp.sum(weights, axis=0, keepdims=True)
        acc[q, :, cols] = acc[q, :, cols] * rescale + jnp.dot(
            v_t[dy], weights.astype(jnp.bfloat16), preferred_element_type=jnp.float32)

    def finish(q):
        out = acc[q] / l_run[q]
        dst = o_send.at[q]
        for pair in range(group // 2):
            cols = slice(pair * LANES, (pair + 1) * LANES)
            first = 2 * pair * LANES
            both = jnp.concatenate([out[:, first:first + LANES], out[:, first + LANES:first + 2 * LANES]], axis=0)
            dst[:main, cols] = jnp.transpose(both, (1, 0)).astype(jnp.bfloat16)
            ends = out[:, (group + pair) * LANES:(group + pair + 1) * LANES]
            both = jnp.concatenate([ends, pltpu.roll(ends, tail, 1)], axis=0)
            dst[main:, cols] = jnp.transpose(both, (1, 0))[:tail].astype(jnp.bfloat16)
        mine, theirs = o_send.at[q, own_rows], o_send.at[q, other_rows]
        if q:
            target = by_dx[q]
            remote(mine, o_all.at[0, nx - q], o_send_sem.at[0], o_recv.at[0, nx - q], target).start()
            remote(theirs, o_all.at[1, nx - q], o_send_sem.at[0], o_recv.at[1, nx - q], {**target, **partner}).start()
        else:
            remote(theirs, o_all.at[1, 0], o_send_sem.at[1], o_recv.at[1, 0], partner).start()
            o_all[0, 0] = o_send[0, own_rows]

    events = {n: [] for n in range(len(STEPS) + 1)}
    def row(*dxs):
        return [functools.partial(kv_row, dx) for dx in dxs]

    def side(*pieces):
        return [functools.partial(kv_side, dx, dy) for dx, dy in pieces]

    def query(dx):
        return [functools.partial(q_arrive, dx)]

    events[0] = row(0, 2, 1, 3)
    events[1] = side((0, 1)) + query(1)
    events[2] = side((2, 3)) + query(3)
    events[3] = side((1, 1), (2, 1), (0, 3), (3, 1))
    events[4] = side((3, 3), (1, 3)) + query(2)
    events[8] = side((0, 2), (1, 2), (2, 2), (3, 2))
    last_of = {q: max(n for n, s in enumerate(STEPS) if s[0] == q) for q in range(nx)}
    first_of = {dy: min(n for n, s in enumerate(STEPS) if s[1] == dy) for dy in range(ny)}

    for n in range(len(STEPS) + 1):
        for event in events[n]:
            event()
        if n < len(STEPS) and first_of[STEPS[n][1]] == n:
            dy = STEPS[n][1]
            v_t[dy] = jnp.transpose(keys(dy).astype(jnp.float32), (1, 0))[head_dim:].astype(jnp.bfloat16)
        for t in range(tiles):
            if n < len(STEPS):
                score(n, *STEPS[n], t)
            if n:
                absorb(n - 1, *STEPS[n - 1], t)
        if n and last_of[STEPS[n - 1][0]] == n - 1:
            finish(STEPS[n - 1][0])

    o_load.wait()
    for i, dx in enumerate(O_ORDER):
        total = None
        for r in range(2):
            if dx or r:
                arrive(o_all.at[r, dx], o_recv.at[r, dx])
            first = ((core if r == 0 else other) * kv_local + head_at(dx)) * q_rows
            term = jnp.dot(o_all[r, dx], w_o[pl.ds(pl.multiple_of(first, q_rows), q_rows)],
                           preferred_element_type=jnp.float32)
            total = term if total is None else total + term
        if i == 0:
            y_acc[...] = total
        elif i < nx - 1:
            y_acc[...] += total
        else:
            y_ref[...] = (y_acc[...] + total).astype(jnp.bfloat16)

    for ref, sem in ((kv_buf.at[pl.ds(0, (nx * ny - 1) * chip_tokens)], kv_send.at[0]), (kv_all.at[0], kv_send.at[1]), (q_all.at[pl.ds(0, nx - 1)], q_send), (o_all.at[:, pl.ds(0, nx - 1)], o_send_sem.at[0]), (o_all.at[1, 0], o_send_sem.at[1])):
        remote(ref, ref, sem, x_sem.at[1], partner).wait_send()


def solution(mesh):
    nx, ny = mesh.shape["cx"], mesh.shape["cy"]
    seq_spec = P("dp", ("cy", "cx", "core"))

    def local_layer(x_loc, w_qkv, w_out):
        heads, head_dim, width = w_out.shape
        kv_heads = (w_qkv.shape[1] - heads) // 2
        tokens = x_loc.shape[1]
        kv_local = kv_heads // 2
        group = heads // kv_heads
        q_rows = group * head_dim
        feat = kv_local * q_rows
        rows = group * 2 * tokens
        dims = (nx, ny, heads, kv_heads, head_dim)
        w_rows = jnp.transpose(w_qkv, (1, 2, 0)).reshape(-1, width)
        hbm = pl.BlockSpec(memory_space=pl.ANY)
        half = jnp.bfloat16
        y = pl.pallas_call(
            functools.partial(kernel, dims),
            out_shape=jax.ShapeDtypeStruct((tokens, width), half),
            in_specs=[hbm] * 3,
            out_specs=pl.BlockSpec(memory_space=pltpu.VMEM),
            scratch_shapes=[
                pltpu.VMEM((TILE, width), half),
                pltpu.VMEM((2 * kv_heads * head_dim, width), half),
                pltpu.VMEM((feat, width), half),
                pltpu.VMEM((heads * head_dim, width), half),
                pltpu.VMEM((kv_heads, tokens, LANES), half),
                pltpu.VMEM((ny * nx * 2 * tokens, LANES), half),
                pltpu.VMEM((nx, head_dim, rows), half),
                pltpu.VMEM((nx, LANES, rows), half),
                pltpu.VMEM((ny, head_dim, nx * 2 * tokens), half),
                pltpu.VMEM((2, rows // TILE, nx * 2 * tokens, TILE), jnp.float32),
                pltpu.VMEM((2, 1, rows), jnp.float32),
                pltpu.VMEM((2, 1, rows), jnp.float32),
                pltpu.VMEM((nx, 1, rows), jnp.float32),
                pltpu.VMEM((nx, 1, rows), jnp.float32),
                pltpu.VMEM((nx, head_dim, rows), jnp.float32),
                pltpu.VMEM((nx, 2 * tokens, q_rows), half),
                pltpu.VMEM((2, nx, tokens, q_rows), half),
                pltpu.VMEM((tokens, width), jnp.float32),
                pltpu.SemaphoreType.DMA((2 + 5 * nx,)),
                pltpu.SemaphoreType.DMA((2,)),
                pltpu.SemaphoreType.DMA((2,)),
                pltpu.SemaphoreType.DMA((ny, nx)),
                pltpu.SemaphoreType.DMA,
                pltpu.SemaphoreType.DMA((nx,)),
                pltpu.SemaphoreType.DMA((2,)),
                pltpu.SemaphoreType.DMA((2, nx)),
            ],
            compiler_params=pltpu.CompilerParams(
                collective_id=0, has_side_effects=True, vmem_limit_bytes=54600 * 1024),
        )(x_loc[0], w_rows, w_out.reshape(heads * head_dim, width))
        return y[None]

    return jax.shard_map(local_layer, mesh=mesh, in_specs=(seq_spec, P(), P()), out_specs=seq_spec, check_vma=False)
```

```python
import functools
import math

import jax
import jax.numpy as jnp
from jax import lax
from jax.experimental import pallas as pl
from jax.experimental.pallas import tpu as pltpu
from jax.sharding import PartitionSpec as P

MESH = pl.DeviceIdType.MESH
LANES = 128
TILE = 256
NT = (((1,), (1,)), ((), ()))

STEPS = (
    (0, 0), (1, 0), (3, 0), (1, 1), (2, 3), (2, 0), (1, 3), (2, 1),
    (2, 2), (3, 2), (1, 2), (3, 3), (3, 1), (0, 3), (0, 1), (0, 2),
)
SLOTS = (("s", 0), ("a", 0), ("s", 1), ("a", 1), ("s", 2), ("a", 2))
END_SLOTS = (("s", 0), ("a", 0), ("a", 1), ("a", 2), ("s", 1), ("s", 2))
FAR_FIRST = (2, 1, 3, 0)
Q_ORDER = (1, 3, 2, 0)
O_ORDER = (3, 0, 1, 2)


def kernel(dims, x_hbm, wqkv_hbm, wout_hbm, y_ref,
           x_ext, w_kv, w_q, w_o, kv_all, kv_buf, q_all, q_t, q_wide, k_wide,
           v_t, s_buf, m_cur, r_cur, m_run, l_run, acc, o_send, o_all, y_acc,
           load_sem, x_sem, kv_send, kv_recv, q_send, q_recv,
           o_send_sem, o_recv):
    nx, ny, heads, kv_heads, head_dim = dims
    dev_tokens = x_hbm.shape[0]
    chip_tokens = 2 * dev_tokens
    row_keys = nx * chip_tokens
    kv_local = kv_heads // 2
    group = heads // kv_heads
    q_rows = group * head_dim
    feat = kv_local * q_rows
    rows = q_t.shape[2]
    tiles = rows // TILE
    main = LANES
    tail = chip_tokens - main
    cx, cy, core = lax.axis_index("cx"), lax.axis_index("cy"), lax.axis_index("core")
    other = 1 - core
    own_rows = pl.ds(pl.multiple_of(core * dev_tokens, 32), dev_tokens)
    other_rows = pl.ds(pl.multiple_of(other * dev_tokens, 32), dev_tokens)
    scale = head_dim ** -0.5 * math.log2(math.e)

    def head_at(dx):
        return lax.rem(cx + dx, nx)

    x_load = pltpu.make_async_copy(x_hbm, x_ext.at[own_rows], load_sem.at[0])
    x_load.start()
    kv_loads, q_loads = [], []
    for i, dx in enumerate(FAR_FIRST):
        for r in range(2):
            head = (core if r == 0 else other) * kv_local + head_at(dx)
            for part in range(2):
                src = pl.multiple_of((heads + part * kv_heads + head) * head_dim, head_dim)
                copy = pltpu.make_async_copy(
                    wqkv_hbm.at[pl.ds(src, head_dim)],
                    w_kv.at[pl.ds((4 * i + 2 * r + part) * head_dim, head_dim)],
                    load_sem.at[1 + 4 * i + 2 * r + part])
                copy.start()
                kv_loads.append(copy)
    for i, dx in enumerate(Q_ORDER):
        src = pl.multiple_of(core * feat + head_at(dx) * q_rows, q_rows)
        copy = pltpu.make_async_copy(
            wqkv_hbm.at[pl.ds(src, q_rows)], w_q.at[pl.ds(i * q_rows, q_rows)], load_sem.at[1 + 4 * nx + i])
        copy.start()
        q_loads.append(copy)

    east = {"cx": lax.rem(cx + 1, nx)}
    west = {"cx": lax.rem(cx + nx - 1, nx)}
    north = {"cy": lax.rem(cy + 1, ny)}
    south = {"cy": lax.rem(cy + ny - 1, ny)}
    partner = {"core": other}
    across = {"cx": head_at(2)}
    by_dx = {0: {}, 1: east, 2: across, 3: west}
    targets = [partner, north, south]
    for dx in range(1, nx):
        targets += [by_dx[dx], {**by_dx[dx], **partner}]
    barrier = pltpu.get_barrier_semaphore()
    for target in targets:
        pl.semaphore_signal(barrier, inc=1, device_id=target, device_id_type=MESH)
    pl.semaphore_wait(barrier, len(targets))

    def remote(src, dst, send_sem, recv_sem, target):
        return pltpu.make_async_remote_copy(
            src_ref=src, dst_ref=dst, send_sem=send_sem, recv_sem=recv_sem, device_id=target, device_id_type=MESH)

    x_load.wait()
    x_copy = remote(x_ext.at[own_rows], x_ext.at[own_rows], x_sem.at[0], x_sem.at[1], partner)
    x_copy.start()
    q_wide[:, head_dim:LANES, :] = jnp.zeros((nx, LANES - head_dim, rows), jnp.bfloat16)
    acc[...] = jnp.zeros_like(acc)
    m_run[...] = jnp.full_like(m_run, -jnp.inf)
    l_run[...] = jnp.zeros_like(l_run)

    def kv_at(dx, dy):
        return dy * row_keys + dx * chip_tokens

    def kv_piece(dx, dy):
        return kv_buf.at[pl.ds(kv_at(dx, dy), chip_tokens)]

    def kv_half(dx, dy, r):
        return kv_buf.at[pl.ds(kv_at(dx, dy) + r * dev_tokens, dev_tokens)]

    def spread(src, dst_of, dx):
        remote(src, dst_of(3), kv_send.at[0], kv_recv.at[3, dx], north).start()
        remote(src, dst_of(1), kv_send.at[0], kv_recv.at[1, dx], south).start()

    for i in range(0, nx, 2):
        for copy in kv_loads[4 * i:4 * i + 8]:
            copy.wait()
        part = lax.dot_general(
            x_ext[own_rows], w_kv[4 * i * head_dim:(4 * i + 8) * head_dim], NT, preferred_element_type=jnp.float32)
        for k in range(4):
            kv_all[2 * i + k] = part[:, k * LANES:(k + 1) * LANES].astype(jnp.bfloat16)
        for k in range(4):
            dx, r = FAR_FIRST[i + k // 2], k % 2
            src = kv_all.at[2 * i + k]
            back = (nx - dx) % nx
            if dx:
                target = {**by_dx[dx], **partner} if r else by_dx[dx]
                remote(src, kv_half(back, 0, r), kv_send.at[0], kv_recv.at[0, back], target).start()
            elif r:
                remote(src, kv_half(0, 0, 1), kv_send.at[1], kv_recv.at[0, 0], partner).start()
            else:
                spread(src, lambda dy: kv_half(0, dy, 0), 0)
                kv_buf[kv_at(0, 0):kv_at(0, 0) + dev_tokens] = kv_all[2 * i + k]
    o_load = pltpu.make_async_copy(wout_hbm, w_o, load_sem.at[1 + 5 * nx])
    o_load.start()

    x_copy.wait()
    x_ext[chip_tokens:chip_tokens + tail] = x_ext[main:chip_tokens]
    lane = lax.broadcasted_iota(jnp.int32, (head_dim, LANES), 1)
    for i in range(0, nx, 2):
        results = []
        for k in (i, i + 1):
            q_loads[k].wait()
        for k in (i, i + 1):
            results.append(lax.dot_general(
                w_q[k * q_rows:(k + 1) * q_rows], x_ext[...], NT, preferred_element_type=jnp.float32))
        for k, res in zip((i, i + 1), results):
            dst = q_all.at[Q_ORDER[k]] if Q_ORDER[k] else q_t.at[0]
            for g in range(group):
                dst[:, g * LANES:(g + 1) * LANES] = res[g * head_dim:(g + 1) * head_dim, :main].astype(jnp.bfloat16)
            for pair in range(group // 2):
                lo = res[2 * pair * head_dim:(2 * pair + 1) * head_dim, main:]
                hi = res[(2 * pair + 1) * head_dim:(2 * pair + 2) * head_dim, main:]
                dst[:, (group + pair) * LANES:(group + pair + 1) * LANES] = (
                    jnp.where(lane < tail, lo, hi).astype(jnp.bfloat16))
        for k in (i, i + 1):
            dx = Q_ORDER[k]
            if dx:
                remote(q_all.at[dx], q_t.at[nx - dx],
                       q_send, q_recv.at[nx - dx], by_dx[dx]).start()

    def arrive(ref, sem):
        remote(ref, ref, q_send, sem, partner).wait_recv()

    def kv_row(dx):
        if dx:
            arrive(kv_piece(dx, 0), kv_recv.at[0, dx])
            spread(kv_piece(dx, 0), lambda dy: kv_piece(dx, dy), dx)
        else:
            arrive(kv_half(0, 0, 1), kv_recv.at[0, 0])
            spread(kv_half(0, 0, 1), lambda dy: kv_half(0, dy, 1), 0)

    def kv_side(dx, dy):
        arrive(kv_piece(dx, dy), kv_recv.at[dy, dx])
        if dy == 3 and dx % 2 == 0:
            remote(kv_piece(dx, 3), kv_piece(dx, 2), kv_send.at[0], kv_recv.at[2, dx], north).start()
        if dy == 1 and dx % 2 == 1:
            remote(kv_piece(dx, 1), kv_piece(dx, 2), kv_send.at[0], kv_recv.at[2, dx], south).start()

    def q_arrive(dx):
        arrive(q_t.at[dx], q_recv.at[dx])

    def widen_queries(q):
        scaled = q_t[q].astype(jnp.float32) * scale
        high = scaled.astype(jnp.bfloat16)
        rest = scaled - high.astype(jnp.float32)
        middle = rest.astype(jnp.bfloat16)
        low = (rest - middle.astype(jnp.float32)).astype(jnp.bfloat16)
        q_wide[q, :head_dim] = high
        q_wide[q, LANES:LANES + head_dim] = middle
        q_wide[q, LANES + head_dim:] = low

    def widen_keys(dy):
        pair = kv_buf[kv_at(0, dy):kv_at(0, dy) + row_keys]
        wide = pair.astype(jnp.float32)
        first = lax.broadcasted_iota(jnp.int32, wide.shape, 1) < head_dim
        twice = jnp.where(first, wide, pltpu.roll(wide, head_dim, 1))
        k_wide[dy, :, :LANES] = pair
        k_wide[dy, :, LANES:] = twice.astype(jnp.bfloat16)
        v_t[dy] = jnp.transpose(wide, (1, 0))[head_dim:].astype(jnp.bfloat16)

    def score(n, q, dy, t):
        cols = slice(t * TILE, (t + 1) * TILE)
        scores = jnp.dot(k_wide[dy], q_wide[q, :, cols], preferred_element_type=jnp.float32)
        old_max = m_run[q, :, cols]
        new_max = jnp.maximum(old_max, jnp.max(scores, axis=0, keepdims=True))
        m_run[q, :, cols] = new_max
        m_cur[n % 2, :, cols] = new_max
        r_cur[n % 2, :, cols] = jnp.exp2(old_max - new_max)
        s_buf[n % 2, t] = scores

    def absorb(n, q, dy, t):
        cols = slice(t * TILE, (t + 1) * TILE)
        rescale = r_cur[n % 2, :, cols]
        weights = jnp.exp2(s_buf[n % 2, t] - m_cur[n % 2, :, cols])
        l_run[q, :, cols] = l_run[q, :, cols] * rescale + jnp.sum(weights, axis=0, keepdims=True)
        acc[q, :, cols] = acc[q, :, cols] * rescale + jnp.dot(
            v_t[dy], weights.astype(jnp.bfloat16), preferred_element_type=jnp.float32)

    def finish(q):
        out = acc[q] / l_run[q]
        dst = o_send.at[q]
        for pair in range(group // 2):
            cols = slice(pair * LANES, (pair + 1) * LANES)
            first = 2 * pair * LANES
            both = jnp.concatenate([out[:, first:first + LANES], out[:, first + LANES:first + 2 * LANES]], axis=0)
            dst[:main, cols] = jnp.transpose(both, (1, 0)).astype(jnp.bfloat16)
            ends = out[:, (group + pair) * LANES:(group + pair + 1) * LANES]
            both = jnp.concatenate([ends, pltpu.roll(ends, tail, 1)], axis=0)
            dst[main:, cols] = jnp.transpose(both, (1, 0))[:tail].astype(jnp.bfloat16)
        mine, theirs = o_send.at[q, own_rows], o_send.at[q, other_rows]
        if q:
            target = by_dx[q]
            remote(mine, o_all.at[0, nx - q], o_send_sem.at[0], o_recv.at[0, nx - q], target).start()
            remote(theirs, o_all.at[1, nx - q], o_send_sem.at[0], o_recv.at[1, nx - q], {**target, **partner}).start()
        else:
            remote(theirs, o_all.at[1, 0], o_send_sem.at[1], o_recv.at[1, 0], partner).start()
            o_all[0, 0] = o_send[0, own_rows]

    events = {n: [] for n in range(len(STEPS) + 1)}
    def row(*dxs):
        return [functools.partial(kv_row, dx) for dx in dxs]

    def side(*pieces):
        return [functools.partial(kv_side, dx, dy) for dx, dy in pieces]

    def query(dx):
        return [functools.partial(q_arrive, dx)]

    events[0] = row(0, 2, 1, 3)
    events[1] = side((0, 1)) + query(1)
    events[2] = side((2, 3)) + query(3)
    events[3] = side((1, 1), (2, 1), (0, 3), (3, 1))
    events[4] = side((3, 3), (1, 3)) + query(2)
    events[8] = side((0, 2), (1, 2), (2, 2), (3, 2))
    last_of = {q: max(n for n, s in enumerate(STEPS) if s[0] == q) for q in range(nx)}
    first_use = {q: min(n for n, s in enumerate(STEPS) if s[0] == q) for q in range(nx)}
    first_of = {dy: min(n for n, s in enumerate(STEPS) if s[1] == dy) for dy in range(ny)}

    for n in range(len(STEPS) + 1):
        for event in events[n]:
            event()
        if n < len(STEPS) and first_of[STEPS[n][1]] == n:
            dy = STEPS[n][1]
            widen_keys(dy)
        if n < len(STEPS) and first_use[STEPS[n][0]] == n:
            widen_queries(STEPS[n][0])
        ends = n and last_of[STEPS[n - 1][0]] == n - 1
        for work, t in (END_SLOTS if ends else SLOTS):
            if work == "s" and n < len(STEPS):
                score(n, *STEPS[n], t)
            if work == "a" and n:
                absorb(n - 1, *STEPS[n - 1], t)
        if ends:
            finish(STEPS[n - 1][0])

    o_load.wait()
    for i, dx in enumerate(O_ORDER):
        total = None
        for r in range(2):
            if dx or r:
                arrive(o_all.at[r, dx], o_recv.at[r, dx])
            first = ((core if r == 0 else other) * kv_local + head_at(dx)) * q_rows
            term = jnp.dot(o_all[r, dx], w_o[pl.ds(pl.multiple_of(first, q_rows), q_rows)],
                           preferred_element_type=jnp.float32)
            total = term if total is None else total + term
        if i == 0:
            y_acc[...] = total
        elif i < nx - 1:
            y_acc[...] += total
        else:
            y_ref[...] = (y_acc[...] + total).astype(jnp.bfloat16)

    for ref, sem in ((kv_buf.at[pl.ds(0, (nx * ny - 1) * chip_tokens)], kv_send.at[0]), (kv_all.at[0], kv_send.at[1]), (q_all.at[pl.ds(0, nx - 1)], q_send), (o_all.at[:, pl.ds(0, nx - 1)], o_send_sem.at[0]), (o_all.at[1, 0], o_send_sem.at[1])):
        remote(ref, ref, sem, x_sem.at[1], partner).wait_send()


def solution(mesh):
    nx, ny = mesh.shape["cx"], mesh.shape["cy"]
    seq_spec = P("dp", ("cy", "cx", "core"))

    def local_layer(x_loc, w_qkv, w_out):
        heads, head_dim, width = w_out.shape
        kv_heads = (w_qkv.shape[1] - heads) // 2
        tokens = x_loc.shape[1]
        kv_local = kv_heads // 2
        group = heads // kv_heads
        q_rows = group * head_dim
        feat = kv_local * q_rows
        rows = group * 2 * tokens
        dims = (nx, ny, heads, kv_heads, head_dim)
        w_rows = jnp.transpose(w_qkv, (1, 2, 0)).reshape(-1, width)
        hbm = pl.BlockSpec(memory_space=pl.ANY)
        half = jnp.bfloat16
        y = pl.pallas_call(
            functools.partial(kernel, dims),
            out_shape=jax.ShapeDtypeStruct((tokens, width), half),
            in_specs=[hbm] * 3,
            out_specs=pl.BlockSpec(memory_space=pltpu.VMEM),
            scratch_shapes=[
                pltpu.VMEM((TILE, width), half),
                pltpu.VMEM((2 * kv_heads * head_dim, width), half),
                pltpu.VMEM((feat, width), half),
                pltpu.VMEM((heads * head_dim, width), half),
                pltpu.VMEM((kv_heads, tokens, LANES), half),
                pltpu.VMEM((ny * nx * 2 * tokens, LANES), half),
                pltpu.VMEM((nx, head_dim, rows), half),
                pltpu.VMEM((nx, head_dim, rows), half),
                pltpu.VMEM((nx, 2 * LANES, rows), half),
                pltpu.VMEM((ny, nx * 2 * tokens, 2 * LANES), half),
                pltpu.VMEM((ny, head_dim, nx * 2 * tokens), half),
                pltpu.VMEM((2, rows // TILE, nx * 2 * tokens, TILE), jnp.float32),
                pltpu.VMEM((2, 1, rows), jnp.float32),
                pltpu.VMEM((2, 1, rows), jnp.float32),
                pltpu.VMEM((nx, 1, rows), jnp.float32),
                pltpu.VMEM((nx, 1, rows), jnp.float32),
                pltpu.VMEM((nx, head_dim, rows), jnp.float32),
                pltpu.VMEM((nx, 2 * tokens, q_rows), half),
                pltpu.VMEM((2, nx, tokens, q_rows), half),
                pltpu.VMEM((tokens, width), jnp.float32),
                pltpu.SemaphoreType.DMA((2 + 5 * nx,)),
                pltpu.SemaphoreType.DMA((2,)),
                pltpu.SemaphoreType.DMA((2,)),
                pltpu.SemaphoreType.DMA((ny, nx)),
                pltpu.SemaphoreType.DMA,
                pltpu.SemaphoreType.DMA((nx,)),
                pltpu.SemaphoreType.DMA((2,)),
                pltpu.SemaphoreType.DMA((2, nx)),
            ],
            compiler_params=pltpu.CompilerParams(
                collective_id=0, has_side_effects=True, vmem_limit_bytes=54600 * 1024),
        )(x_loc[0], w_rows, w_out.reshape(heads * head_dim, width))
        return y[None]

    return jax.shard_map(local_layer, mesh=mesh, in_specs=(seq_spec, P(), P()), out_specs=seq_spec, check_vma=False)
```

```python
import functools
import math

import jax
import jax.numpy as jnp
from jax import lax
from jax.experimental import pallas as pl
from jax.experimental.pallas import tpu as pltpu
from jax.sharding import PartitionSpec as P

MESH = pl.DeviceIdType.MESH
LANES = 128
TILE = 256
NT = (((1,), (1,)), ((), ()))

STEPS = (
    (0, 0), (1, 0), (3, 0), (1, 1), (2, 3), (2, 0), (1, 3), (2, 1),
    (2, 2), (3, 2), (1, 2), (3, 3), (3, 1), (0, 3), (0, 1), (0, 2),
)
SLOTS = (("s", 0), ("a", 0), ("s", 1), ("a", 1), ("s", 2), ("a", 2))
END_SLOTS = (("s", 0), ("a", 0), ("a", 1), ("s", 1), ("a", 2), ("s", 2))
FAR_FIRST = (2, 1, 3, 0)
Q_ORDER = (1, 3, 2, 0)
O_ORDER = (2, 0, 3, 1)


def kernel(dims, x_hbm, wqkv_hbm, wout_hbm, y_ref,
           x_ext, w_kv, w_q, w_o, kv_all, kv_buf, q_all, q_t,
           v_t, s_buf, m_cur, r_cur, m_run, l_run, acc, o_send, o_all, y_acc,
           load_sem, x_sem, kv_send, kv_recv, q_send, q_recv,
           o_send_sem, o_recv):
    nx, ny, heads, kv_heads, head_dim = dims
    dev_tokens = x_hbm.shape[0]
    chip_tokens = 2 * dev_tokens
    row_keys = nx * chip_tokens
    kv_local = kv_heads // 2
    group = heads // kv_heads
    q_rows = group * head_dim
    feat = kv_local * q_rows
    rows = q_t.shape[2]
    tiles = rows // TILE
    main = LANES
    tail = chip_tokens - main
    cx, cy, core = lax.axis_index("cx"), lax.axis_index("cy"), lax.axis_index("core")
    other = 1 - core
    own_rows = pl.ds(pl.multiple_of(core * dev_tokens, 32), dev_tokens)
    other_rows = pl.ds(pl.multiple_of(other * dev_tokens, 32), dev_tokens)
    scale = head_dim ** -0.5 * math.log2(math.e)

    def head_at(dx):
        return lax.rem(cx + dx, nx)

    x_load = pltpu.make_async_copy(x_hbm, x_ext.at[own_rows], load_sem.at[0])
    x_load.start()
    kv_loads, q_loads = [], []
    for i, dx in enumerate(FAR_FIRST):
        for r in range(2):
            head = (core if r == 0 else other) * kv_local + head_at(dx)
            for part in range(2):
                src = pl.multiple_of((heads + part * kv_heads + head) * head_dim, head_dim)
                copy = pltpu.make_async_copy(
                    wqkv_hbm.at[pl.ds(src, head_dim)],
                    w_kv.at[pl.ds((4 * i + 2 * r + part) * head_dim, head_dim)],
                    load_sem.at[1 + 4 * i + 2 * r + part])
                copy.start()
                kv_loads.append(copy)
    for i, dx in enumerate(Q_ORDER):
        src = pl.multiple_of(core * feat + head_at(dx) * q_rows, q_rows)
        copy = pltpu.make_async_copy(
            wqkv_hbm.at[pl.ds(src, q_rows)], w_q.at[pl.ds(i * q_rows, q_rows)], load_sem.at[1 + 4 * nx + i])
        copy.start()
        q_loads.append(copy)

    east = {"cx": lax.rem(cx + 1, nx)}
    west = {"cx": lax.rem(cx + nx - 1, nx)}
    north = {"cy": lax.rem(cy + 1, ny)}
    south = {"cy": lax.rem(cy + ny - 1, ny)}
    partner = {"core": other}
    across = {"cx": head_at(2)}
    by_dx = {0: {}, 1: east, 2: across, 3: west}
    targets = [partner, north, south]
    for dx in range(1, nx):
        targets += [by_dx[dx], {**by_dx[dx], **partner}]
    barrier = pltpu.get_barrier_semaphore()
    for target in targets:
        pl.semaphore_signal(barrier, inc=1, device_id=target, device_id_type=MESH)
    pl.semaphore_wait(barrier, len(targets))

    def remote(src, dst, send_sem, recv_sem, target):
        return pltpu.make_async_remote_copy(
            src_ref=src, dst_ref=dst, send_sem=send_sem, recv_sem=recv_sem, device_id=target, device_id_type=MESH)

    x_load.wait()
    x_copy = remote(x_ext.at[own_rows], x_ext.at[own_rows], x_sem.at[0], x_sem.at[1], partner)
    x_copy.start()
    q_t[:, head_dim:, :] = jnp.zeros((nx, LANES - head_dim, rows), jnp.bfloat16)
    acc[...] = jnp.zeros_like(acc)
    m_run[...] = jnp.full_like(m_run, -jnp.inf)
    l_run[...] = jnp.zeros_like(l_run)

    def kv_at(dx, dy):
        return dy * row_keys + dx * chip_tokens

    def kv_piece(dx, dy):
        return kv_buf.at[pl.ds(kv_at(dx, dy), chip_tokens)]

    def kv_half(dx, dy, r):
        return kv_buf.at[pl.ds(kv_at(dx, dy) + r * dev_tokens, dev_tokens)]

    def spread(src, dst_of, dx):
        remote(src, dst_of(3), kv_send.at[0], kv_recv.at[3, dx], north).start()
        remote(src, dst_of(1), kv_send.at[0], kv_recv.at[1, dx], south).start()

    for i in range(0, nx, 2):
        for copy in kv_loads[4 * i:4 * i + 8]:
            copy.wait()
        part = lax.dot_general(
            x_ext[own_rows], w_kv[4 * i * head_dim:(4 * i + 8) * head_dim], NT, preferred_element_type=jnp.float32)
        for k in range(4):
            kv_all[2 * i + k] = part[:, k * LANES:(k + 1) * LANES].astype(jnp.bfloat16)
        for k in range(4):
            dx, r = FAR_FIRST[i + k // 2], k % 2
            src = kv_all.at[2 * i + k]
            back = (nx - dx) % nx
            if dx:
                target = {**by_dx[dx], **partner} if r else by_dx[dx]
                remote(src, kv_half(back, 0, r), kv_send.at[0], kv_recv.at[0, back], target).start()
            elif r:
                remote(src, kv_half(0, 0, 1), kv_send.at[1], kv_recv.at[0, 0], partner).start()
            else:
                spread(src, lambda dy: kv_half(0, dy, 0), 0)
                kv_buf[kv_at(0, 0):kv_at(0, 0) + dev_tokens] = kv_all[2 * i + k]
    o_load = pltpu.make_async_copy(wout_hbm, w_o, load_sem.at[1 + 5 * nx])
    o_load.start()

    x_copy.wait()
    x_ext[chip_tokens:chip_tokens + tail] = x_ext[main:chip_tokens]
    lane = lax.broadcasted_iota(jnp.int32, (head_dim, LANES), 1)
    for i in range(0, nx, 2):
        results = []
        for k in (i, i + 1):
            q_loads[k].wait()
        for k in (i, i + 1):
            results.append(lax.dot_general(
                w_q[k * q_rows:(k + 1) * q_rows], x_ext[...], NT, preferred_element_type=jnp.float32))
        for k, res in zip((i, i + 1), results):
            dst = q_all.at[Q_ORDER[k]] if Q_ORDER[k] else q_t.at[0, pl.ds(0, head_dim)]
            for g in range(group):
                dst[:, g * LANES:(g + 1) * LANES] = res[g * head_dim:(g + 1) * head_dim, :main].astype(jnp.bfloat16)
            for pair in range(group // 2):
                lo = res[2 * pair * head_dim:(2 * pair + 1) * head_dim, main:]
                hi = res[(2 * pair + 1) * head_dim:(2 * pair + 2) * head_dim, main:]
                dst[:, (group + pair) * LANES:(group + pair + 1) * LANES] = (
                    jnp.where(lane < tail, lo, hi).astype(jnp.bfloat16))
        for k in (i, i + 1):
            dx = Q_ORDER[k]
            if dx:
                remote(q_all.at[dx], q_t.at[nx - dx, pl.ds(0, head_dim)],
                       q_send, q_recv.at[nx - dx], by_dx[dx]).start()

    def arrive(ref, sem):
        remote(ref, ref, q_send, sem, partner).wait_recv()

    def kv_row(dx):
        if dx:
            arrive(kv_piece(dx, 0), kv_recv.at[0, dx])
            spread(kv_piece(dx, 0), lambda dy: kv_piece(dx, dy), dx)
        else:
            arrive(kv_half(0, 0, 1), kv_recv.at[0, 0])
            spread(kv_half(0, 0, 1), lambda dy: kv_half(0, dy, 1), 0)

    def kv_side(dx, dy):
        arrive(kv_piece(dx, dy), kv_recv.at[dy, dx])
        if dy == 3 and dx % 2 == 0:
            remote(kv_piece(dx, 3), kv_piece(dx, 2), kv_send.at[0], kv_recv.at[2, dx], north).start()
        if dy == 1 and dx % 2 == 1:
            remote(kv_piece(dx, 1), kv_piece(dx, 2), kv_send.at[0], kv_recv.at[2, dx], south).start()

    def q_arrive(dx):
        arrive(q_t.at[dx, pl.ds(0, head_dim)], q_recv.at[dx])

    def keys(dy):
        return kv_buf[kv_at(0, dy):kv_at(0, dy) + row_keys]

    def score(n, q, dy, t):
        cols = slice(t * TILE, (t + 1) * TILE)
        scores = jnp.dot(keys(dy), q_t[q, :, cols], preferred_element_type=jnp.float32)
        old_max = m_run[q, :, cols]
        new_max = jnp.maximum(old_max, jnp.max(scores, axis=0, keepdims=True))
        m_run[q, :, cols] = new_max
        m_cur[n % 2, :, cols] = new_max
        r_cur[n % 2, :, cols] = jnp.exp2((old_max - new_max) * scale)
        s_buf[n % 2, t] = scores

    def absorb(n, q, dy, t):
        cols = slice(t * TILE, (t + 1) * TILE)
        rescale = r_cur[n % 2, :, cols]
        weights = jnp.exp2((s_buf[n % 2, t] - m_cur[n % 2, :, cols]) * scale)
        l_run[q, :, cols] = l_run[q, :, cols] * rescale + jnp.sum(weights, axis=0, keepdims=True)
        acc[q, :, cols] = acc[q, :, cols] * rescale + jnp.dot(
            v_t[dy], weights.astype(jnp.bfloat16), preferred_element_type=jnp.float32)

    def finish(q):
        out = acc[q] / l_run[q]
        dst = o_send.at[q]
        for pair in range(group // 2):
            cols = slice(pair * LANES, (pair + 1) * LANES)
            first = 2 * pair * LANES
            both = jnp.concatenate([out[:, first:first + LANES], out[:, first + LANES:first + 2 * LANES]], axis=0)
            dst[:main, cols] = jnp.transpose(both, (1, 0)).astype(jnp.bfloat16)
            ends = out[:, (group + pair) * LANES:(group + pair + 1) * LANES]
            both = jnp.concatenate([ends, pltpu.roll(ends, tail, 1)], axis=0)
            dst[main:, cols] = jnp.transpose(both, (1, 0))[:tail].astype(jnp.bfloat16)
        mine, theirs = o_send.at[q, own_rows], o_send.at[q, other_rows]
        if q:
            target = by_dx[q]
            remote(mine, o_all.at[0, nx - q], o_send_sem.at[0], o_recv.at[0, nx - q], target).start()
            remote(theirs, o_all.at[1, nx - q], o_send_sem.at[0], o_recv.at[1, nx - q], {**target, **partner}).start()
        else:
            remote(theirs, o_all.at[1, 0], o_send_sem.at[1], o_recv.at[1, 0], partner).start()
            o_all[0, 0] = o_send[0, own_rows]

    events = {n: [] for n in range(len(STEPS) + 1)}
    def row(*dxs):
        return [functools.partial(kv_row, dx) for dx in dxs]

    def side(*pieces):
        return [functools.partial(kv_side, dx, dy) for dx, dy in pieces]

    def query(dx):
        return [functools.partial(q_arrive, dx)]

    events[0] = row(0, 2, 1, 3)
    events[1] = side((0, 1)) + query(1)
    events[2] = side((2, 3)) + query(3)
    events[3] = side((1, 1), (2, 1), (0, 3), (3, 1))
    events[4] = side((3, 3), (1, 3)) + query(2)
    events[8] = side((0, 2), (1, 2), (2, 2), (3, 2))
    last_of = {q: max(n for n, s in enumerate(STEPS) if s[0] == q) for q in range(nx)}
    first_of = {dy: min(n for n, s in enumerate(STEPS) if s[1] == dy) for dy in range(ny)}

    for n in range(len(STEPS) + 1):
        for event in events[n]:
            event()
        if n < len(STEPS) and first_of[STEPS[n][1]] == n:
            dy = STEPS[n][1]
            v_t[dy] = jnp.transpose(keys(dy).astype(jnp.float32), (1, 0))[head_dim:].astype(jnp.bfloat16)
        ends = n and last_of[STEPS[n - 1][0]] == n - 1
        for work, t in (END_SLOTS if ends else SLOTS):
            if work == "s" and n < len(STEPS):
                score(n, *STEPS[n], t)
            if work == "a" and n:
                absorb(n - 1, *STEPS[n - 1], t)
        if ends:
            finish(STEPS[n - 1][0])

    o_load.wait()
    for i, dx in enumerate(O_ORDER):
        if i == nx - 1:
            for ref, sem in ((kv_buf.at[pl.ds(0, (nx * ny - 1) * chip_tokens)], kv_send.at[0]), (kv_all.at[0], kv_send.at[1]), (q_all.at[pl.ds(0, nx - 1)], q_send), (o_all.at[:, pl.ds(0, nx - 1)], o_send_sem.at[0]), (o_all.at[1, 0], o_send_sem.at[1])):
                remote(ref, ref, sem, x_sem.at[1], partner).wait_send()
        total = None
        for r in range(2):
            if dx or r:
                arrive(o_all.at[r, dx], o_recv.at[r, dx])
            first = ((core if r == 0 else other) * kv_local + head_at(dx)) * q_rows
            term = jnp.dot(o_all[r, dx], w_o[pl.ds(pl.multiple_of(first, q_rows), q_rows)],
                           preferred_element_type=jnp.float32)
            total = term if total is None else total + term
        if i == 0:
            y_acc[...] = total
        elif i < nx - 1:
            y_acc[...] += total
        else:
            y_ref[...] = (y_acc[...] + total).astype(jnp.bfloat16)


def solution(mesh):
    nx, ny = mesh.shape["cx"], mesh.shape["cy"]
    seq_spec = P("dp", ("cy", "cx", "core"))

    def local_layer(x_loc, w_qkv, w_out):
        heads, head_dim, width = w_out.shape
        kv_heads = (w_qkv.shape[1] - heads) // 2
        tokens = x_loc.shape[1]
        kv_local = kv_heads // 2
        group = heads // kv_heads
        q_rows = group * head_dim
        feat = kv_local * q_rows
        rows = group * 2 * tokens
        dims = (nx, ny, heads, kv_heads, head_dim)
        w_rows = jnp.transpose(w_qkv, (1, 2, 0)).reshape(-1, width)
        hbm = pl.BlockSpec(memory_space=pl.ANY)
        half = jnp.bfloat16
        y = pl.pallas_call(
            functools.partial(kernel, dims),
            out_shape=jax.ShapeDtypeStruct((tokens, width), half),
            in_specs=[hbm] * 3,
            out_specs=pl.BlockSpec(memory_space=pltpu.VMEM),
            scratch_shapes=[
                pltpu.VMEM((TILE, width), half),
                pltpu.VMEM((2 * kv_heads * head_dim, width), half),
                pltpu.VMEM((feat, width), half),
                pltpu.VMEM((heads * head_dim, width), half),
                pltpu.VMEM((kv_heads, tokens, LANES), half),
                pltpu.VMEM((ny * nx * 2 * tokens, LANES), half),
                pltpu.VMEM((nx, head_dim, rows), half),
                pltpu.VMEM((nx, LANES, rows), half),
                pltpu.VMEM((ny, head_dim, nx * 2 * tokens), half),
                pltpu.VMEM((2, rows // TILE, nx * 2 * tokens, TILE), jnp.float32),
                pltpu.VMEM((2, 1, rows), jnp.float32),
                pltpu.VMEM((2, 1, rows), jnp.float32),
                pltpu.VMEM((nx, 1, rows), jnp.float32),
                pltpu.VMEM((nx, 1, rows), jnp.float32),
                pltpu.VMEM((nx, head_dim, rows), jnp.float32),
                pltpu.VMEM((nx, 2 * tokens, q_rows), half),
                pltpu.VMEM((2, nx, tokens, q_rows), half),
                pltpu.VMEM((tokens, width), jnp.float32),
                pltpu.SemaphoreType.DMA((2 + 5 * nx,)),
                pltpu.SemaphoreType.DMA((2,)),
                pltpu.SemaphoreType.DMA((2,)),
                pltpu.SemaphoreType.DMA((ny, nx)),
                pltpu.SemaphoreType.DMA,
                pltpu.SemaphoreType.DMA((nx,)),
                pltpu.SemaphoreType.DMA((2,)),
                pltpu.SemaphoreType.DMA((2, nx)),
            ],
            compiler_params=pltpu.CompilerParams(
                collective_id=0, has_side_effects=True, vmem_limit_bytes=54600 * 1024),
        )(x_loc[0], w_rows, w_out.reshape(heads * head_dim, width))
        return y[None]

    return jax.shard_map(local_layer, mesh=mesh, in_specs=(seq_spec, P(), P()), out_specs=seq_spec, check_vma=False)
```

```python
import functools
import math

import jax
import jax.numpy as jnp
from jax import lax
from jax.experimental import pallas as pl
from jax.experimental.pallas import tpu as pltpu
from jax.sharding import PartitionSpec as P

MESH = pl.DeviceIdType.MESH
LANES = 128
TILE = 256
NT = (((1,), (1,)), ((), ()))

STEPS = (
    (0, 0), (3, 0), (1, 0), (2, 1), (3, 1), (2, 3), (3, 3), (1, 1),
    (2, 0), (2, 2), (1, 3), (3, 2), (1, 2), (0, 3), (0, 2), (0, 1),
)
SLOTS = (("s", 0), ("a", 0), ("s", 1), ("a", 1), ("s", 2), ("a", 2))
END_SLOTS = (("s", 0), ("a", 0), ("a", 1), ("s", 1), ("a", 2), ("s", 2))
FAR_FIRST = (2, 1, 3, 0)
Q_ORDER = (1, 3, 2, 0)
O_ORDER = (2, 0, 3, 1)


def kernel(dims, x_hbm, wqkv_hbm, wout_hbm, y_ref,
           x_ext, w_kv, w_q, w_o, kv_all, kv_buf, q_all, q_t,
           v_t, s_buf, m_cur, r_cur, m_run, l_run, acc, o_send, o_all, y_acc,
           load_sem, x_sem, kv_send, kv_recv, q_send, q_recv,
           o_send_sem, o_recv):
    nx, ny, heads, kv_heads, head_dim = dims
    dev_tokens = x_hbm.shape[0]
    chip_tokens = 2 * dev_tokens
    row_keys = nx * chip_tokens
    kv_local = kv_heads // 2
    group = heads // kv_heads
    q_rows = group * head_dim
    feat = kv_local * q_rows
    rows = q_t.shape[2]
    tiles = rows // TILE
    main = LANES
    tail = chip_tokens - main
    cx, cy, core = lax.axis_index("cx"), lax.axis_index("cy"), lax.axis_index("core")
    other = 1 - core
    own_rows = pl.ds(pl.multiple_of(core * dev_tokens, 32), dev_tokens)
    other_rows = pl.ds(pl.multiple_of(other * dev_tokens, 32), dev_tokens)
    scale = head_dim ** -0.5 * math.log2(math.e)

    def head_at(dx):
        return lax.rem(cx + dx, nx)

    x_load = pltpu.make_async_copy(x_hbm, x_ext.at[own_rows], load_sem.at[0])
    x_load.start()
    kv_loads, q_loads = [], []
    for i, dx in enumerate(FAR_FIRST):
        for r in range(2):
            head = (core if r == 0 else other) * kv_local + head_at(dx)
            for part in range(2):
                src = pl.multiple_of((heads + part * kv_heads + head) * head_dim, head_dim)
                copy = pltpu.make_async_copy(
                    wqkv_hbm.at[pl.ds(src, head_dim)],
                    w_kv.at[pl.ds((4 * i + 2 * r + part) * head_dim, head_dim)],
                    load_sem.at[1 + 4 * i + 2 * r + part])
                copy.start()
                kv_loads.append(copy)
    for i, dx in enumerate(Q_ORDER):
        src = pl.multiple_of(core * feat + head_at(dx) * q_rows, q_rows)
        copy = pltpu.make_async_copy(
            wqkv_hbm.at[pl.ds(src, q_rows)], w_q.at[pl.ds(i * q_rows, q_rows)], load_sem.at[1 + 4 * nx + i])
        copy.start()
        q_loads.append(copy)

    east = {"cx": lax.rem(cx + 1, nx)}
    west = {"cx": lax.rem(cx + nx - 1, nx)}
    north = {"cy": lax.rem(cy + 1, ny)}
    south = {"cy": lax.rem(cy + ny - 1, ny)}
    partner = {"core": other}
    across = {"cx": head_at(2)}
    by_dx = {0: {}, 1: east, 2: across, 3: west}
    targets = [partner, north, south]
    for dx in range(1, nx):
        targets += [by_dx[dx], {**by_dx[dx], **partner}]
    barrier = pltpu.get_barrier_semaphore()
    for target in targets:
        pl.semaphore_signal(barrier, inc=1, device_id=target, device_id_type=MESH)
    pl.semaphore_wait(barrier, len(targets))

    def remote(src, dst, send_sem, recv_sem, target):
        return pltpu.make_async_remote_copy(
            src_ref=src, dst_ref=dst, send_sem=send_sem, recv_sem=recv_sem, device_id=target, device_id_type=MESH)

    x_load.wait()
    x_copy = remote(x_ext.at[own_rows], x_ext.at[own_rows], x_sem.at[0], x_sem.at[1], partner)
    x_copy.start()
    q_t[:, head_dim:, :] = jnp.zeros((nx, LANES - head_dim, rows), jnp.bfloat16)
    acc[...] = jnp.zeros_like(acc)
    m_run[...] = jnp.full_like(m_run, -jnp.inf)
    l_run[...] = jnp.zeros_like(l_run)

    def kv_at(dx, dy):
        return dy * row_keys + dx * chip_tokens

    def kv_piece(dx, dy):
        return kv_buf.at[pl.ds(kv_at(dx, dy), chip_tokens)]

    def kv_half(dx, dy, r):
        return kv_buf.at[pl.ds(kv_at(dx, dy) + r * dev_tokens, dev_tokens)]

    def spread(src, dst_of, dx):
        remote(src, dst_of(3), kv_send.at[0], kv_recv.at[3, dx], north).start()
        remote(src, dst_of(1), kv_send.at[0], kv_recv.at[1, dx], south).start()

    for i in range(0, nx, 2):
        for copy in kv_loads[4 * i:4 * i + 8]:
            copy.wait()
        part = lax.dot_general(
            x_ext[own_rows], w_kv[4 * i * head_dim:(4 * i + 8) * head_dim], NT, preferred_element_type=jnp.float32)
        for k in range(4):
            kv_all[2 * i + k] = part[:, k * LANES:(k + 1) * LANES].astype(jnp.bfloat16)
        for k in range(4):
            dx, r = FAR_FIRST[i + k // 2], k % 2
            src = kv_all.at[2 * i + k]
            back = (nx - dx) % nx
            if dx:
                target = {**by_dx[dx], **partner} if r else by_dx[dx]
                remote(src, kv_half(back, 0, r), kv_send.at[0], kv_recv.at[0, back], target).start()
            elif r:
                remote(src, kv_half(0, 0, 1), kv_send.at[1], kv_recv.at[0, 0], partner).start()
            else:
                spread(src, lambda dy: kv_half(0, dy, 0), 0)
                kv_buf[kv_at(0, 0):kv_at(0, 0) + dev_tokens] = kv_all[2 * i + k]
    o_load = pltpu.make_async_copy(wout_hbm, w_o, load_sem.at[1 + 5 * nx])
    o_load.start()

    x_copy.wait()
    x_ext[chip_tokens:chip_tokens + tail] = x_ext[main:chip_tokens]
    lane = lax.broadcasted_iota(jnp.int32, (head_dim, LANES), 1)
    for i in range(0, nx, 2):
        results = []
        for k in (i, i + 1):
            q_loads[k].wait()
        for k in (i, i + 1):
            results.append(lax.dot_general(
                w_q[k * q_rows:(k + 1) * q_rows], x_ext[...], NT, preferred_element_type=jnp.float32))
        for k, res in zip((i, i + 1), results):
            dst = q_all.at[Q_ORDER[k]] if Q_ORDER[k] else q_t.at[0, pl.ds(0, head_dim)]
            for g in range(group):
                dst[:, g * LANES:(g + 1) * LANES] = res[g * head_dim:(g + 1) * head_dim, :main].astype(jnp.bfloat16)
            for pair in range(group // 2):
                lo = res[2 * pair * head_dim:(2 * pair + 1) * head_dim, main:]
                hi = res[(2 * pair + 1) * head_dim:(2 * pair + 2) * head_dim, main:]
                dst[:, (group + pair) * LANES:(group + pair + 1) * LANES] = (
                    jnp.where(lane < tail, lo, hi).astype(jnp.bfloat16))
        for k in (i, i + 1):
            dx = Q_ORDER[k]
            if dx:
                remote(q_all.at[dx], q_t.at[nx - dx, pl.ds(0, head_dim)],
                       q_send, q_recv.at[nx - dx], by_dx[dx]).start()

    def arrive(ref, sem):
        remote(ref, ref, q_send, sem, partner).wait_recv()

    def kv_row(dx):
        if dx:
            arrive(kv_piece(dx, 0), kv_recv.at[0, dx])
            spread(kv_piece(dx, 0), lambda dy: kv_piece(dx, dy), dx)
        else:
            arrive(kv_half(0, 0, 1), kv_recv.at[0, 0])
            spread(kv_half(0, 0, 1), lambda dy: kv_half(0, dy, 1), 0)

    def kv_side(dx, dy):
        arrive(kv_piece(dx, dy), kv_recv.at[dy, dx])
        if dy == 3 and dx % 2 == 0:
            remote(kv_piece(dx, 3), kv_piece(dx, 2), kv_send.at[0], kv_recv.at[2, dx], north).start()
        if dy == 1 and dx % 2 == 1:
            remote(kv_piece(dx, 1), kv_piece(dx, 2), kv_send.at[0], kv_recv.at[2, dx], south).start()

    def q_arrive(dx):
        arrive(q_t.at[dx, pl.ds(0, head_dim)], q_recv.at[dx])

    def keys(dy):
        return kv_buf[kv_at(0, dy):kv_at(0, dy) + row_keys]

    def score(n, q, dy, t):
        cols = slice(t * TILE, (t + 1) * TILE)
        scores = jnp.dot(keys(dy), q_t[q, :, cols], preferred_element_type=jnp.float32)
        old_max = m_run[q, :, cols]
        new_max = jnp.maximum(old_max, jnp.max(scores, axis=0, keepdims=True))
        m_run[q, :, cols] = new_max
        m_cur[n % 2, :, cols] = new_max
        r_cur[n % 2, :, cols] = jnp.exp2((old_max - new_max) * scale)
        s_buf[n % 2, t] = scores

    def absorb(n, q, dy, t):
        cols = slice(t * TILE, (t + 1) * TILE)
        rescale = r_cur[n % 2, :, cols]
        weights = jnp.exp2((s_buf[n % 2, t] - m_cur[n % 2, :, cols]) * scale)
        l_run[q, :, cols] = l_run[q, :, cols] * rescale + jnp.sum(weights, axis=0, keepdims=True)
        acc[q, :, cols] = acc[q, :, cols] * rescale + jnp.dot(
            v_t[dy], weights.astype(jnp.bfloat16), preferred_element_type=jnp.float32)

    def finish(q):
        out = acc[q] / l_run[q]
        dst = o_send.at[q]
        for pair in range(group // 2):
            cols = slice(pair * LANES, (pair + 1) * LANES)
            first = 2 * pair * LANES
            both = jnp.concatenate([out[:, first:first + LANES], out[:, first + LANES:first + 2 * LANES]], axis=0)
            dst[:main, cols] = jnp.transpose(both, (1, 0)).astype(jnp.bfloat16)
            ends = out[:, (group + pair) * LANES:(group + pair + 1) * LANES]
            both = jnp.concatenate([ends, pltpu.roll(ends, tail, 1)], axis=0)
            dst[main:, cols] = jnp.transpose(both, (1, 0))[:tail].astype(jnp.bfloat16)
        mine, theirs = o_send.at[q, own_rows], o_send.at[q, other_rows]
        if q:
            target = by_dx[q]
            remote(mine, o_all.at[0, nx - q], o_send_sem.at[0], o_recv.at[0, nx - q], target).start()
            remote(theirs, o_all.at[1, nx - q], o_send_sem.at[0], o_recv.at[1, nx - q], {**target, **partner}).start()
        else:
            remote(theirs, o_all.at[1, 0], o_send_sem.at[1], o_recv.at[1, 0], partner).start()
            o_all[0, 0] = o_send[0, own_rows]

    events = {n: [] for n in range(len(STEPS) + 1)}
    def row(*dxs):
        return [functools.partial(kv_row, dx) for dx in dxs]

    def side(*pieces):
        return [functools.partial(kv_side, dx, dy) for dx, dy in pieces]

    def query(dx):
        return [functools.partial(q_arrive, dx)]

    events[0] = row(0, 2, 1, 3) + side((0, 3))
    events[1] = query(3)
    events[2] = side((2, 3)) + query(1)
    events[3] = side((1, 1), (0, 1), (2, 1)) + query(2) + side((3, 1))
    events[5] = side((1, 3), (3, 3))
    events[9] = side((1, 2), (2, 2), (0, 2), (3, 2))
    last_of = {q: max(n for n, s in enumerate(STEPS) if s[0] == q) for q in range(nx)}
    first_of = {dy: min(n for n, s in enumerate(STEPS) if s[1] == dy) for dy in range(ny)}

    for n in range(len(STEPS) + 1):
        for event in events[n]:
            event()
        if n < len(STEPS) and first_of[STEPS[n][1]] == n:
            dy = STEPS[n][1]
            v_t[dy] = jnp.transpose(keys(dy).astype(jnp.float32), (1, 0))[head_dim:].astype(jnp.bfloat16)
        ends = n and last_of[STEPS[n - 1][0]] == n - 1
        for work, t in (END_SLOTS if ends else SLOTS):
            if work == "s" and n < len(STEPS):
                score(n, *STEPS[n], t)
            if work == "a" and n:
                absorb(n - 1, *STEPS[n - 1], t)
        if ends:
            finish(STEPS[n - 1][0])

    o_load.wait()
    for i, dx in enumerate(O_ORDER):
        if i == nx - 1:
            for ref, sem in ((kv_buf.at[pl.ds(0, (nx * ny - 1) * chip_tokens)], kv_send.at[0]), (kv_all.at[0], kv_send.at[1]), (q_all.at[pl.ds(0, nx - 1)], q_send), (o_all.at[:, pl.ds(0, nx - 1)], o_send_sem.at[0]), (o_all.at[1, 0], o_send_sem.at[1])):
                remote(ref, ref, sem, x_sem.at[1], partner).wait_send()
        total = None
        for r in range(2):
            if dx or r:
                arrive(o_all.at[r, dx], o_recv.at[r, dx])
            first = ((core if r == 0 else other) * kv_local + head_at(dx)) * q_rows
            term = jnp.dot(o_all[r, dx], w_o[pl.ds(pl.multiple_of(first, q_rows), q_rows)],
                           preferred_element_type=jnp.float32)
            total = term if total is None else total + term
        if i == 0:
            y_acc[...] = total
        elif i < nx - 1:
            y_acc[...] += total
        else:
            y_ref[...] = (y_acc[...] + total).astype(jnp.bfloat16)


def solution(mesh):
    nx, ny = mesh.shape["cx"], mesh.shape["cy"]
    seq_spec = P("dp", ("cy", "cx", "core"))

    def local_layer(x_loc, w_qkv, w_out):
        heads, head_dim, width = w_out.shape
        kv_heads = (w_qkv.shape[1] - heads) // 2
        tokens = x_loc.shape[1]
        kv_local = kv_heads // 2
        group = heads // kv_heads
        q_rows = group * head_dim
        feat = kv_local * q_rows
        rows = group * 2 * tokens
        dims = (nx, ny, heads, kv_heads, head_dim)
        w_rows = jnp.transpose(w_qkv, (1, 2, 0)).reshape(-1, width)
        hbm = pl.BlockSpec(memory_space=pl.ANY)
        half = jnp.bfloat16
        y = pl.pallas_call(
            functools.partial(kernel, dims),
            out_shape=jax.ShapeDtypeStruct((tokens, width), half),
            in_specs=[hbm] * 3,
            out_specs=pl.BlockSpec(memory_space=pltpu.VMEM),
            scratch_shapes=[
                pltpu.VMEM((TILE, width), half),
                pltpu.VMEM((2 * kv_heads * head_dim, width), half),
                pltpu.VMEM((feat, width), half),
                pltpu.VMEM((heads * head_dim, width), half),
                pltpu.VMEM((kv_heads, tokens, LANES), half),
                pltpu.VMEM((ny * nx * 2 * tokens, LANES), half),
                pltpu.VMEM((nx, head_dim, rows), half),
                pltpu.VMEM((nx, LANES, rows), half),
                pltpu.VMEM((ny, head_dim, nx * 2 * tokens), half),
                pltpu.VMEM((2, rows // TILE, nx * 2 * tokens, TILE), jnp.float32),
                pltpu.VMEM((2, 1, rows), jnp.float32),
                pltpu.VMEM((2, 1, rows), jnp.float32),
                pltpu.VMEM((nx, 1, rows), jnp.float32),
                pltpu.VMEM((nx, 1, rows), jnp.float32),
                pltpu.VMEM((nx, head_dim, rows), jnp.float32),
                pltpu.VMEM((nx, 2 * tokens, q_rows), half),
                pltpu.VMEM((2, nx, tokens, q_rows), half),
                pltpu.VMEM((tokens, width), jnp.float32),
                pltpu.SemaphoreType.DMA((2 + 5 * nx,)),
                pltpu.SemaphoreType.DMA((2,)),
                pltpu.SemaphoreType.DMA((2,)),
                pltpu.SemaphoreType.DMA((ny, nx)),
                pltpu.SemaphoreType.DMA,
                pltpu.SemaphoreType.DMA((nx,)),
                pltpu.SemaphoreType.DMA((2,)),
                pltpu.SemaphoreType.DMA((2, nx)),
            ],
            compiler_params=pltpu.CompilerParams(
                collective_id=0, has_side_effects=True, vmem_limit_bytes=54600 * 1024),
        )(x_loc[0], w_rows, w_out.reshape(heads * head_dim, width))
        return y[None]

    return jax.shard_map(local_layer, mesh=mesh, in_specs=(seq_spec, P(), P()), out_specs=seq_spec, check_vma=False)
```

```python
import functools
import math

import jax
import jax.numpy as jnp
from jax import lax
from jax.experimental import pallas as pl
from jax.experimental.pallas import tpu as pltpu
from jax.sharding import PartitionSpec as P

MESH = pl.DeviceIdType.MESH
LANES = 128
TILE = 256
NT = (((1,), (1,)), ((), ()))

STEPS = (
    (0, 0), (1, 0), (3, 0), (1, 1), (2, 3), (2, 0), (1, 3), (2, 1),
    (2, 2), (3, 2), (1, 2), (3, 3), (3, 1), (0, 3), (0, 1), (0, 2),
)
SLOTS = (("s", 0), ("a", 0), ("s", 1), ("a", 1), ("s", 2), ("a", 2))
END_SLOTS = (("s", 0), ("a", 0), ("a", 1), ("s", 1), ("a", 2), ("s", 2))
FAR_FIRST = (2, 1, 3, 0)
Q_ORDER = (1, 3, 2, 0)
O_ORDER = (2, 0, 3, 1)


def kernel(dims, x_hbm, wqkv_hbm, wout_hbm, y_ref,
           x_ext, w_kv, w_q, w_o, kv_all, kv_buf, q_all, q_t,
           v_t, s_buf, m_cur, r_cur, m_run, l_run, acc, o_send, o_all, y_acc,
           load_sem, x_sem, kv_send, kv_recv, q_send, q_recv,
           o_send_sem, o_recv):
    nx, ny, heads, kv_heads, head_dim = dims
    dev_tokens = x_hbm.shape[0]
    chip_tokens = 2 * dev_tokens
    row_keys = nx * chip_tokens
    kv_local = kv_heads // 2
    group = heads // kv_heads
    q_rows = group * head_dim
    feat = kv_local * q_rows
    rows = q_t.shape[2]
    tiles = rows // TILE
    main = LANES
    tail = chip_tokens - main
    cx, cy, core = lax.axis_index("cx"), lax.axis_index("cy"), lax.axis_index("core")
    other = 1 - core
    own_rows = pl.ds(pl.multiple_of(core * dev_tokens, 32), dev_tokens)
    other_rows = pl.ds(pl.multiple_of(other * dev_tokens, 32), dev_tokens)
    scale = head_dim ** -0.5 * math.log2(math.e)

    def head_at(dx):
        return lax.rem(cx + dx, nx)

    x_load = pltpu.make_async_copy(x_hbm, x_ext.at[own_rows], load_sem.at[0])
    x_load.start()
    kv_loads, q_loads = [], []
    for i, dx in enumerate(FAR_FIRST):
        for r in range(2):
            head = (core if r == 0 else other) * kv_local + head_at(dx)
            for part in range(2):
                src = pl.multiple_of((heads + part * kv_heads + head) * head_dim, head_dim)
                copy = pltpu.make_async_copy(
                    wqkv_hbm.at[pl.ds(src, head_dim)],
                    w_kv.at[pl.ds((4 * i + 2 * r + part) * head_dim, head_dim)],
                    load_sem.at[1 + 4 * i + 2 * r + part])
                copy.start()
                kv_loads.append(copy)
    for i, dx in enumerate(Q_ORDER):
        src = pl.multiple_of(core * feat + head_at(dx) * q_rows, q_rows)
        copy = pltpu.make_async_copy(
            wqkv_hbm.at[pl.ds(src, q_rows)], w_q.at[pl.ds(i * q_rows, q_rows)], load_sem.at[1 + 4 * nx + i])
        copy.start()
        q_loads.append(copy)

    east = {"cx": lax.rem(cx + 1, nx)}
    west = {"cx": lax.rem(cx + nx - 1, nx)}
    north = {"cy": lax.rem(cy + 1, ny)}
    south = {"cy": lax.rem(cy + ny - 1, ny)}
    partner = {"core": other}
    across = {"cx": head_at(2)}
    by_dx = {0: {}, 1: east, 2: across, 3: west}
    targets = [partner, north, south]
    for dx in range(1, nx):
        targets += [by_dx[dx], {**by_dx[dx], **partner}]
    barrier = pltpu.get_barrier_semaphore()
    for target in targets:
        pl.semaphore_signal(barrier, inc=1, device_id=target, device_id_type=MESH)
    pl.semaphore_wait(barrier, len(targets))

    def remote(src, dst, send_sem, recv_sem, target):
        return pltpu.make_async_remote_copy(
            src_ref=src, dst_ref=dst, send_sem=send_sem, recv_sem=recv_sem, device_id=target, device_id_type=MESH)

    x_load.wait()
    x_copy = remote(x_ext.at[own_rows], x_ext.at[own_rows], x_sem.at[0], x_sem.at[1], partner)
    x_copy.start()
    q_t[:, head_dim:, :] = jnp.zeros((nx, LANES - head_dim, rows), jnp.bfloat16)
    acc[...] = jnp.zeros_like(acc)
    m_run[...] = jnp.full_like(m_run, -jnp.inf)
    l_run[...] = jnp.zeros_like(l_run)

    def kv_at(dx, dy):
        return dy * row_keys + dx * chip_tokens

    def kv_piece(dx, dy):
        return kv_buf.at[pl.ds(kv_at(dx, dy), chip_tokens)]

    def kv_half(dx, dy, r):
        return kv_buf.at[pl.ds(kv_at(dx, dy) + r * dev_tokens, dev_tokens)]

    def spread(src, dst_of, dx):
        remote(src, dst_of(3), kv_send.at[0], kv_recv.at[3, dx], north).start()
        remote(src, dst_of(1), kv_send.at[0], kv_recv.at[1, dx], south).start()

    for i in range(0, nx, 2):
        for copy in kv_loads[4 * i:4 * i + 8]:
            copy.wait()
        part = lax.dot_general(
            x_ext[own_rows], w_kv[4 * i * head_dim:(4 * i + 8) * head_dim], NT, preferred_element_type=jnp.float32)
        for k in range(4):
            kv_all[2 * i + k] = part[:, k * LANES:(k + 1) * LANES].astype(jnp.bfloat16)
        for k in range(4):
            dx, r = FAR_FIRST[i + k // 2], k % 2
            src = kv_all.at[2 * i + k]
            back = (nx - dx) % nx
            if dx:
                target = {**by_dx[dx], **partner} if r else by_dx[dx]
                remote(src, kv_half(back, 0, r), kv_send.at[0], kv_recv.at[0, back], target).start()
            elif r:
                remote(src, kv_half(0, 0, 1), kv_send.at[1], kv_recv.at[0, 0], partner).start()
            else:
                spread(src, lambda dy: kv_half(0, dy, 0), 0)
                kv_buf[kv_at(0, 0):kv_at(0, 0) + dev_tokens] = kv_all[2 * i + k]
    o_loads = []
    for i, dx in enumerate(O_ORDER):
        for r in range(2):
            src = ((core if r == 0 else other) * kv_local + head_at(dx)) * q_rows
            copy = pltpu.make_async_copy(
                wout_hbm.at[pl.ds(pl.multiple_of(src, q_rows), q_rows)],
                w_o.at[pl.ds((2 * i + r) * q_rows, q_rows)], load_sem.at[1 + 5 * nx + 2 * i + r])
            copy.start()
            o_loads.append(copy)

    x_copy.wait()
    x_ext[chip_tokens:chip_tokens + tail] = x_ext[main:chip_tokens]
    lane = lax.broadcasted_iota(jnp.int32, (head_dim, LANES), 1)
    for i in range(0, nx, 2):
        results = []
        for k in (i, i + 1):
            q_loads[k].wait()
        for k in (i, i + 1):
            results.append(lax.dot_general(
                w_q[k * q_rows:(k + 1) * q_rows], x_ext[...], NT, preferred_element_type=jnp.float32))
        for k, res in zip((i, i + 1), results):
            dst = q_all.at[Q_ORDER[k]] if Q_ORDER[k] else q_t.at[0, pl.ds(0, head_dim)]
            for g in range(group):
                dst[:, g * LANES:(g + 1) * LANES] = res[g * head_dim:(g + 1) * head_dim, :main].astype(jnp.bfloat16)
            for pair in range(group // 2):
                lo = res[2 * pair * head_dim:(2 * pair + 1) * head_dim, main:]
                hi = res[(2 * pair + 1) * head_dim:(2 * pair + 2) * head_dim, main:]
                dst[:, (group + pair) * LANES:(group + pair + 1) * LANES] = (
                    jnp.where(lane < tail, lo, hi).astype(jnp.bfloat16))
        for k in (i, i + 1):
            dx = Q_ORDER[k]
            if dx:
                remote(q_all.at[dx], q_t.at[nx - dx, pl.ds(0, head_dim)],
                       q_send, q_recv.at[nx - dx], by_dx[dx]).start()

    def arrive(ref, sem):
        remote(ref, ref, q_send, sem, partner).wait_recv()

    def kv_row(dx):
        if dx:
            arrive(kv_piece(dx, 0), kv_recv.at[0, dx])
            spread(kv_piece(dx, 0), lambda dy: kv_piece(dx, dy), dx)
        else:
            arrive(kv_half(0, 0, 1), kv_recv.at[0, 0])
            spread(kv_half(0, 0, 1), lambda dy: kv_half(0, dy, 1), 0)

    def kv_side(dx, dy):
        arrive(kv_piece(dx, dy), kv_recv.at[dy, dx])
        if dy == 3 and dx % 2 == 0:
            remote(kv_piece(dx, 3), kv_piece(dx, 2), kv_send.at[0], kv_recv.at[2, dx], north).start()
        if dy == 1 and dx % 2 == 1:
            remote(kv_piece(dx, 1), kv_piece(dx, 2), kv_send.at[0], kv_recv.at[2, dx], south).start()

    def q_arrive(dx):
        arrive(q_t.at[dx, pl.ds(0, head_dim)], q_recv.at[dx])

    def keys(dy):
        return kv_buf[kv_at(0, dy):kv_at(0, dy) + row_keys]

    def score(n, q, dy, t):
        cols = slice(t * TILE, (t + 1) * TILE)
        scores = jnp.dot(keys(dy), q_t[q, :, cols], preferred_element_type=jnp.float32)
        old_max = m_run[q, :, cols]
        new_max = jnp.maximum(old_max, jnp.max(scores, axis=0, keepdims=True))
        m_run[q, :, cols] = new_max
        m_cur[n % 2, :, cols] = new_max
        r_cur[n % 2, :, cols] = jnp.exp2((old_max - new_max) * scale)
        s_buf[n % 2, t] = scores

    def absorb(n, q, dy, t):
        cols = slice(t * TILE, (t + 1) * TILE)
        rescale = r_cur[n % 2, :, cols]
        weights = jnp.exp2((s_buf[n % 2, t] - m_cur[n % 2, :, cols]) * scale)
        l_run[q, :, cols] = l_run[q, :, cols] * rescale + jnp.sum(weights, axis=0, keepdims=True)
        acc[q, :, cols] = acc[q, :, cols] * rescale + jnp.dot(
            v_t[dy], weights.astype(jnp.bfloat16), preferred_element_type=jnp.float32)

    def finish(q):
        out = acc[q] / l_run[q]
        dst = o_send.at[q]
        for pair in range(group // 2):
            cols = slice(pair * LANES, (pair + 1) * LANES)
            first = 2 * pair * LANES
            both = jnp.concatenate([out[:, first:first + LANES], out[:, first + LANES:first + 2 * LANES]], axis=0)
            dst[:main, cols] = jnp.transpose(both, (1, 0)).astype(jnp.bfloat16)
            ends = out[:, (group + pair) * LANES:(group + pair + 1) * LANES]
            both = jnp.concatenate([ends, pltpu.roll(ends, tail, 1)], axis=0)
            dst[main:, cols] = jnp.transpose(both, (1, 0))[:tail].astype(jnp.bfloat16)
        mine, theirs = o_send.at[q, own_rows], o_send.at[q, other_rows]
        if q:
            target = by_dx[q]
            remote(mine, o_all.at[0, nx - q], o_send_sem.at[0], o_recv.at[0, nx - q], target).start()
            remote(theirs, o_all.at[1, nx - q], o_send_sem.at[0], o_recv.at[1, nx - q], {**target, **partner}).start()
        else:
            remote(theirs, o_all.at[1, 0], o_send_sem.at[1], o_recv.at[1, 0], partner).start()
            o_all[0, 0] = o_send[0, own_rows]

    events = {n: [] for n in range(len(STEPS) + 1)}
    def row(*dxs):
        return [functools.partial(kv_row, dx) for dx in dxs]

    def side(*pieces):
        return [functools.partial(kv_side, dx, dy) for dx, dy in pieces]

    def query(dx):
        return [functools.partial(q_arrive, dx)]

    events[0] = row(0, 2, 1, 3)
    events[1] = side((0, 1)) + query(1)
    events[2] = side((2, 3)) + query(3)
    events[3] = side((1, 1), (2, 1), (0, 3), (3, 1))
    events[4] = side((3, 3), (1, 3)) + query(2)
    events[8] = side((0, 2), (1, 2), (2, 2), (3, 2))
    last_of = {q: max(n for n, s in enumerate(STEPS) if s[0] == q) for q in range(nx)}
    first_of = {dy: min(n for n, s in enumerate(STEPS) if s[1] == dy) for dy in range(ny)}

    for n in range(len(STEPS) + 1):
        for event in events[n]:
            event()
        if n < len(STEPS) and first_of[STEPS[n][1]] == n:
            dy = STEPS[n][1]
            v_t[dy] = jnp.transpose(keys(dy).astype(jnp.float32), (1, 0))[head_dim:].astype(jnp.bfloat16)
        ends = n and last_of[STEPS[n - 1][0]] == n - 1
        for work, t in (END_SLOTS if ends else SLOTS):
            if work == "s" and n < len(STEPS):
                score(n, *STEPS[n], t)
            if work == "a" and n:
                absorb(n - 1, *STEPS[n - 1], t)
        if ends:
            finish(STEPS[n - 1][0])

    for copy in o_loads:
        copy.wait()
    for i, dx in enumerate(O_ORDER):
        if i == nx - 1:
            for ref, sem in ((kv_buf.at[pl.ds(0, (nx * ny - 1) * chip_tokens)], kv_send.at[0]), (kv_all.at[0], kv_send.at[1]), (q_all.at[pl.ds(0, nx - 1)], q_send), (o_all.at[:, pl.ds(0, nx - 1)], o_send_sem.at[0]), (o_all.at[1, 0], o_send_sem.at[1])):
                remote(ref, ref, sem, x_sem.at[1], partner).wait_send()
        for r in range(2):
            if dx or r:
                arrive(o_all.at[r, dx], o_recv.at[r, dx])
        total = jnp.dot(
            jnp.concatenate([o_all[0, dx], o_all[1, dx]], axis=1), w_o[2 * i * q_rows:(2 * i + 2) * q_rows],
            preferred_element_type=jnp.float32)
        if i == 0:
            y_acc[...] = total
        elif i < nx - 1:
            y_acc[...] += total
        else:
            y_ref[...] = (y_acc[...] + total).astype(jnp.bfloat16)


def solution(mesh):
    nx, ny = mesh.shape["cx"], mesh.shape["cy"]
    seq_spec = P("dp", ("cy", "cx", "core"))

    def local_layer(x_loc, w_qkv, w_out):
        heads, head_dim, width = w_out.shape
        kv_heads = (w_qkv.shape[1] - heads) // 2
        tokens = x_loc.shape[1]
        kv_local = kv_heads // 2
        group = heads // kv_heads
        q_rows = group * head_dim
        feat = kv_local * q_rows
        rows = group * 2 * tokens
        dims = (nx, ny, heads, kv_heads, head_dim)
        w_rows = jnp.transpose(w_qkv, (1, 2, 0)).reshape(-1, width)
        hbm = pl.BlockSpec(memory_space=pl.ANY)
        half = jnp.bfloat16
        y = pl.pallas_call(
            functools.partial(kernel, dims),
            out_shape=jax.ShapeDtypeStruct((tokens, width), half),
            in_specs=[hbm] * 3,
            out_specs=pl.BlockSpec(memory_space=pltpu.VMEM),
            scratch_shapes=[
                pltpu.VMEM((TILE, width), half),
                pltpu.VMEM((2 * kv_heads * head_dim, width), half),
                pltpu.VMEM((feat, width), half),
                pltpu.VMEM((heads * head_dim, width), half),
                pltpu.VMEM((kv_heads, tokens, LANES), half),
                pltpu.VMEM((ny * nx * 2 * tokens, LANES), half),
                pltpu.VMEM((nx, head_dim, rows), half),
                pltpu.VMEM((nx, LANES, rows), half),
                pltpu.VMEM((ny, head_dim, nx * 2 * tokens), half),
                pltpu.VMEM((2, rows // TILE, nx * 2 * tokens, TILE), jnp.float32),
                pltpu.VMEM((2, 1, rows), jnp.float32),
                pltpu.VMEM((2, 1, rows), jnp.float32),
                pltpu.VMEM((nx, 1, rows), jnp.float32),
                pltpu.VMEM((nx, 1, rows), jnp.float32),
                pltpu.VMEM((nx, head_dim, rows), jnp.float32),
                pltpu.VMEM((nx, 2 * tokens, q_rows), half),
                pltpu.VMEM((2, nx, tokens, q_rows), half),
                pltpu.VMEM((tokens, width), jnp.float32),
                pltpu.SemaphoreType.DMA((1 + 7 * nx,)),
                pltpu.SemaphoreType.DMA((2,)),
                pltpu.SemaphoreType.DMA((2,)),
                pltpu.SemaphoreType.DMA((ny, nx)),
                pltpu.SemaphoreType.DMA,
                pltpu.SemaphoreType.DMA((nx,)),
                pltpu.SemaphoreType.DMA((2,)),
                pltpu.SemaphoreType.DMA((2, nx)),
            ],
            compiler_params=pltpu.CompilerParams(
                collective_id=0, has_side_effects=True, vmem_limit_bytes=54600 * 1024),
        )(x_loc[0], w_rows, w_out.reshape(heads * head_dim, width))
        return y[None]

    return jax.shard_map(local_layer, mesh=mesh, in_specs=(seq_spec, P(), P()), out_specs=seq_spec, check_vma=False)
```

```python
import functools
import math

import jax
import jax.numpy as jnp
from jax import lax
from jax.experimental import pallas as pl
from jax.experimental.pallas import tpu as pltpu
from jax.sharding import PartitionSpec as P

MESH = pl.DeviceIdType.MESH
LANES = 128
TILE = 256
NT = (((1,), (1,)), ((), ()))

STEPS = (
    (0, 0), (1, 0), (3, 0), (1, 1), (2, 3), (2, 0), (1, 3), (2, 1),
    (2, 2), (1, 2), (3, 2), (3, 3), (3, 1), (0, 3), (0, 1), (0, 2),
)
SLOTS = (("s", 0), ("a", 0), ("s", 1), ("a", 1), ("s", 2), ("a", 2))
END_SLOTS = (("s", 0), ("a", 0), ("a", 1), ("s", 1), ("a", 2), ("s", 2))
FAR_FIRST = (2, 1, 3, 0)
Q_ORDER = (1, 3, 2, 0)
O_ORDER = (2, 0, 3, 1)


def kernel(dims, x_hbm, wqkv_hbm, wout_hbm, y_ref,
           x_ext, w_kv, w_q, w_o, kv_all, kv_buf, q_all, q_t,
           v_t, s_buf, m_cur, r_cur, m_run, l_run, acc, o_send, o_all, y_acc,
           load_sem, x_sem, kv_send, kv_recv, q_send, q_recv,
           o_send_sem, o_recv):
    nx, ny, heads, kv_heads, head_dim = dims
    dev_tokens = x_hbm.shape[0]
    chip_tokens = 2 * dev_tokens
    row_keys = nx * chip_tokens
    kv_local = kv_heads // 2
    group = heads // kv_heads
    q_rows = group * head_dim
    feat = kv_local * q_rows
    rows = q_t.shape[2]
    tiles = rows // TILE
    main = LANES
    tail = chip_tokens - main
    cx, cy, core = lax.axis_index("cx"), lax.axis_index("cy"), lax.axis_index("core")
    other = 1 - core
    own_rows = pl.ds(pl.multiple_of(core * dev_tokens, 32), dev_tokens)
    other_rows = pl.ds(pl.multiple_of(other * dev_tokens, 32), dev_tokens)
    scale = head_dim ** -0.5 * math.log2(math.e)

    def head_at(dx):
        return lax.rem(cx + dx, nx)

    x_load = pltpu.make_async_copy(x_hbm, x_ext.at[own_rows], load_sem.at[0])
    x_load.start()
    kv_loads, q_loads = [], []
    for i, dx in enumerate(FAR_FIRST):
        for r in range(2):
            head = (core if r == 0 else other) * kv_local + head_at(dx)
            for part in range(2):
                src = pl.multiple_of((heads + part * kv_heads + head) * head_dim, head_dim)
                copy = pltpu.make_async_copy(
                    wqkv_hbm.at[pl.ds(src, head_dim)],
                    w_kv.at[pl.ds((4 * i + 2 * r + part) * head_dim, head_dim)],
                    load_sem.at[1 + 4 * i + 2 * r + part])
                copy.start()
                kv_loads.append(copy)
    for i, dx in enumerate(Q_ORDER):
        src = pl.multiple_of(core * feat + head_at(dx) * q_rows, q_rows)
        copy = pltpu.make_async_copy(
            wqkv_hbm.at[pl.ds(src, q_rows)], w_q.at[pl.ds(i * q_rows, q_rows)], load_sem.at[1 + 4 * nx + i])
        copy.start()
        q_loads.append(copy)

    east = {"cx": lax.rem(cx + 1, nx)}
    west = {"cx": lax.rem(cx + nx - 1, nx)}
    north = {"cy": lax.rem(cy + 1, ny)}
    south = {"cy": lax.rem(cy + ny - 1, ny)}
    partner = {"core": other}
    across = {"cx": head_at(2)}
    by_dx = {0: {}, 1: east, 2: across, 3: west}
    targets = [partner, north, south]
    for dx in range(1, nx):
        targets += [by_dx[dx], {**by_dx[dx], **partner}]
    barrier = pltpu.get_barrier_semaphore()
    for target in targets:
        pl.semaphore_signal(barrier, inc=1, device_id=target, device_id_type=MESH)
    pl.semaphore_wait(barrier, len(targets))

    def remote(src, dst, send_sem, recv_sem, target):
        return pltpu.make_async_remote_copy(
            src_ref=src, dst_ref=dst, send_sem=send_sem, recv_sem=recv_sem, device_id=target, device_id_type=MESH)

    x_load.wait()
    x_copy = remote(x_ext.at[own_rows], x_ext.at[own_rows], x_sem.at[0], x_sem.at[1], partner)
    x_copy.start()
    q_t[:, head_dim:, :] = jnp.zeros((nx, LANES - head_dim, rows), jnp.bfloat16)
    acc[...] = jnp.zeros_like(acc)
    m_run[...] = jnp.full_like(m_run, -jnp.inf)
    l_run[...] = jnp.zeros_like(l_run)

    def kv_at(dx, dy):
        return dy * row_keys + dx * chip_tokens

    def kv_piece(dx, dy):
        return kv_buf.at[pl.ds(kv_at(dx, dy), chip_tokens)]

    def kv_half(dx, dy, r):
        return kv_buf.at[pl.ds(kv_at(dx, dy) + r * dev_tokens, dev_tokens)]

    def spread(src, dst_of, dx):
        remote(src, dst_of(3), kv_send.at[0], kv_recv.at[3, dx], north).start()
        remote(src, dst_of(1), kv_send.at[0], kv_recv.at[1, dx], south).start()

    for i in range(0, nx, 2):
        for copy in kv_loads[4 * i:4 * i + 8]:
            copy.wait()
        part = lax.dot_general(
            x_ext[own_rows], w_kv[4 * i * head_dim:(4 * i + 8) * head_dim], NT, preferred_element_type=jnp.float32)
        for k in range(4):
            kv_all[2 * i + k] = part[:, k * LANES:(k + 1) * LANES].astype(jnp.bfloat16)
        for k in range(4):
            dx, r = FAR_FIRST[i + k // 2], k % 2
            src = kv_all.at[2 * i + k]
            back = (nx - dx) % nx
            if dx:
                target = {**by_dx[dx], **partner} if r else by_dx[dx]
                remote(src, kv_half(back, 0, r), kv_send.at[0], kv_recv.at[0, back], target).start()
            elif r:
                remote(src, kv_half(0, 0, 1), kv_send.at[1], kv_recv.at[0, 0], partner).start()
            else:
                spread(src, lambda dy: kv_half(0, dy, 0), 0)
                kv_buf[kv_at(0, 0):kv_at(0, 0) + dev_tokens] = kv_all[2 * i + k]
    o_loads = []
    for i, dx in enumerate(O_ORDER):
        for r in range(2):
            src = ((core if r == 0 else other) * kv_local + head_at(dx)) * q_rows
            copy = pltpu.make_async_copy(
                wout_hbm.at[pl.ds(pl.multiple_of(src, q_rows), q_rows)],
                w_o.at[pl.ds((2 * i + r) * q_rows, q_rows)], load_sem.at[1 + 5 * nx + 2 * i + r])
            copy.start()
            o_loads.append(copy)

    x_copy.wait()
    x_ext[chip_tokens:chip_tokens + tail] = x_ext[main:chip_tokens]
    lane = lax.broadcasted_iota(jnp.int32, (head_dim, LANES), 1)
    for i in range(0, nx, 2):
        results = []
        for k in (i, i + 1):
            q_loads[k].wait()
        for k in (i, i + 1):
            results.append(lax.dot_general(
                w_q[k * q_rows:(k + 1) * q_rows], x_ext[...], NT, preferred_element_type=jnp.float32))
        for k, res in zip((i, i + 1), results):
            dst = q_all.at[Q_ORDER[k]] if Q_ORDER[k] else q_t.at[0, pl.ds(0, head_dim)]
            for g in range(group):
                dst[:, g * LANES:(g + 1) * LANES] = res[g * head_dim:(g + 1) * head_dim, :main].astype(jnp.bfloat16)
            for pair in range(group // 2):
                lo = res[2 * pair * head_dim:(2 * pair + 1) * head_dim, main:]
                hi = res[(2 * pair + 1) * head_dim:(2 * pair + 2) * head_dim, main:]
                dst[:, (group + pair) * LANES:(group + pair + 1) * LANES] = (
                    jnp.where(lane < tail, lo, hi).astype(jnp.bfloat16))
        for k in (i, i + 1):
            dx = Q_ORDER[k]
            if dx:
                remote(q_all.at[dx], q_t.at[nx - dx, pl.ds(0, head_dim)],
                       q_send, q_recv.at[nx - dx], by_dx[dx]).start()

    def arrive(ref, sem):
        remote(ref, ref, q_send, sem, partner).wait_recv()

    def kv_row(dx):
        if dx:
            arrive(kv_piece(dx, 0), kv_recv.at[0, dx])
            spread(kv_piece(dx, 0), lambda dy: kv_piece(dx, dy), dx)
        else:
            arrive(kv_half(0, 0, 1), kv_recv.at[0, 0])
            spread(kv_half(0, 0, 1), lambda dy: kv_half(0, dy, 1), 0)

    def kv_side(dx, dy):
        arrive(kv_piece(dx, dy), kv_recv.at[dy, dx])
        if dy == 3 and dx % 2 == 0:
            remote(kv_piece(dx, 3), kv_piece(dx, 2), kv_send.at[0], kv_recv.at[2, dx], north).start()
        if dy == 1 and dx % 2 == 1:
            remote(kv_piece(dx, 1), kv_piece(dx, 2), kv_send.at[0], kv_recv.at[2, dx], south).start()

    def q_arrive(dx):
        arrive(q_t.at[dx, pl.ds(0, head_dim)], q_recv.at[dx])

    def keys(dy):
        return kv_buf[kv_at(0, dy):kv_at(0, dy) + row_keys]

    def score(n, q, dy, t):
        cols = slice(t * TILE, (t + 1) * TILE)
        scores = jnp.dot(keys(dy), q_t[q, :, cols], preferred_element_type=jnp.float32)
        old_max = m_run[q, :, cols]
        new_max = jnp.maximum(old_max, jnp.max(scores, axis=0, keepdims=True))
        m_run[q, :, cols] = new_max
        m_cur[n % 2, :, cols] = new_max
        r_cur[n % 2, :, cols] = jnp.exp2((old_max - new_max) * scale)
        s_buf[n % 2, t] = scores

    def absorb(n, q, dy, t):
        cols = slice(t * TILE, (t + 1) * TILE)
        rescale = r_cur[n % 2, :, cols]
        weights = jnp.exp2((s_buf[n % 2, t] - m_cur[n % 2, :, cols]) * scale)
        l_run[q, :, cols] = l_run[q, :, cols] * rescale + jnp.sum(weights, axis=0, keepdims=True)
        acc[q, :, cols] = acc[q, :, cols] * rescale + jnp.dot(
            v_t[dy], weights.astype(jnp.bfloat16), preferred_element_type=jnp.float32)

    def finish(q):
        out = acc[q] / l_run[q]
        dst = o_send.at[q]
        for pair in range(group // 2):
            cols = slice(pair * LANES, (pair + 1) * LANES)
            first = 2 * pair * LANES
            both = jnp.concatenate([out[:, first:first + LANES], out[:, first + LANES:first + 2 * LANES]], axis=0)
            dst[:main, cols] = jnp.transpose(both, (1, 0)).astype(jnp.bfloat16)
            ends = out[:, (group + pair) * LANES:(group + pair + 1) * LANES]
            both = jnp.concatenate([ends, pltpu.roll(ends, tail, 1)], axis=0)
            dst[main:, cols] = jnp.transpose(both, (1, 0))[:tail].astype(jnp.bfloat16)
        mine, theirs = o_send.at[q, own_rows], o_send.at[q, other_rows]
        if q:
            target = by_dx[q]
            remote(mine, o_all.at[0, nx - q], o_send_sem.at[0], o_recv.at[0, nx - q], target).start()
            remote(theirs, o_all.at[1, nx - q], o_send_sem.at[0], o_recv.at[1, nx - q], {**target, **partner}).start()
        else:
            remote(theirs, o_all.at[1, 0], o_send_sem.at[1], o_recv.at[1, 0], partner).start()
            o_all[0, 0] = o_send[0, own_rows]

    events = {n: [] for n in range(len(STEPS) + 1)}
    def row(*dxs):
        return [functools.partial(kv_row, dx) for dx in dxs]

    def side(*pieces):
        return [functools.partial(kv_side, dx, dy) for dx, dy in pieces]

    def query(dx):
        return [functools.partial(q_arrive, dx)]

    events[0] = row(0, 2, 1, 3)
    events[1] = side((0, 1)) + query(1)
    events[2] = side((2, 3)) + query(3)
    events[3] = side((1, 1), (2, 1), (0, 3), (3, 1))
    events[4] = side((3, 3), (1, 3)) + query(2)
    events[8] = side((0, 2), (1, 2), (2, 2), (3, 2))
    last_of = {q: max(n for n, s in enumerate(STEPS) if s[0] == q) for q in range(nx)}
    first_of = {dy: min(n for n, s in enumerate(STEPS) if s[1] == dy) for dy in range(ny)}

    for n in range(len(STEPS) + 1):
        for event in events[n]:
            event()
        if n < len(STEPS) and first_of[STEPS[n][1]] == n:
            dy = STEPS[n][1]
            v_t[dy] = jnp.transpose(keys(dy).astype(jnp.float32), (1, 0))[head_dim:].astype(jnp.bfloat16)
        ends = n and last_of[STEPS[n - 1][0]] == n - 1
        for work, t in (END_SLOTS if ends else SLOTS):
            if work == "s" and n < len(STEPS):
                score(n, *STEPS[n], t)
            if work == "a" and n:
                absorb(n - 1, *STEPS[n - 1], t)
        if ends:
            finish(STEPS[n - 1][0])

    for copy in o_loads:
        copy.wait()
    for i, dx in enumerate(O_ORDER):
        if i == nx - 1:
            for ref, sem in ((kv_buf.at[pl.ds(0, (nx * ny - 1) * chip_tokens)], kv_send.at[0]), (kv_all.at[0], kv_send.at[1]), (q_all.at[pl.ds(0, nx - 1)], q_send), (o_all.at[:, pl.ds(0, nx - 1)], o_send_sem.at[0]), (o_all.at[1, 0], o_send_sem.at[1])):
                remote(ref, ref, sem, x_sem.at[1], partner).wait_send()
        for r in range(2):
            if dx or r:
                arrive(o_all.at[r, dx], o_recv.at[r, dx])
        total = jnp.dot(
            jnp.concatenate([o_all[0, dx], o_all[1, dx]], axis=1), w_o[2 * i * q_rows:(2 * i + 2) * q_rows],
            preferred_element_type=jnp.float32)
        if i == 0:
            y_acc[...] = total
        elif i < nx - 1:
            y_acc[...] += total
        else:
            y_ref[...] = (y_acc[...] + total).astype(jnp.bfloat16)


def solution(mesh):
    nx, ny = mesh.shape["cx"], mesh.shape["cy"]
    seq_spec = P("dp", ("cy", "cx", "core"))

    def local_layer(x_loc, w_qkv, w_out):
        heads, head_dim, width = w_out.shape
        kv_heads = (w_qkv.shape[1] - heads) // 2
        tokens = x_loc.shape[1]
        kv_local = kv_heads // 2
        group = heads // kv_heads
        q_rows = group * head_dim
        feat = kv_local * q_rows
        rows = group * 2 * tokens
        dims = (nx, ny, heads, kv_heads, head_dim)
        w_rows = jnp.transpose(w_qkv, (1, 2, 0)).reshape(-1, width)
        hbm = pl.BlockSpec(memory_space=pl.ANY)
        half = jnp.bfloat16
        y = pl.pallas_call(
            functools.partial(kernel, dims),
            out_shape=jax.ShapeDtypeStruct((tokens, width), half),
            in_specs=[hbm] * 3,
            out_specs=pl.BlockSpec(memory_space=pltpu.VMEM),
            scratch_shapes=[
                pltpu.VMEM((TILE, width), half),
                pltpu.VMEM((2 * kv_heads * head_dim, width), half),
                pltpu.VMEM((feat, width), half),
                pltpu.VMEM((heads * head_dim, width), half),
                pltpu.VMEM((kv_heads, tokens, LANES), half),
                pltpu.VMEM((ny * nx * 2 * tokens, LANES), half),
                pltpu.VMEM((nx, head_dim, rows), half),
                pltpu.VMEM((nx, LANES, rows), half),
                pltpu.VMEM((ny, head_dim, nx * 2 * tokens), half),
                pltpu.VMEM((2, rows // TILE, nx * 2 * tokens, TILE), jnp.float32),
                pltpu.VMEM((2, 1, rows), jnp.float32),
                pltpu.VMEM((2, 1, rows), jnp.float32),
                pltpu.VMEM((nx, 1, rows), jnp.float32),
                pltpu.VMEM((nx, 1, rows), jnp.float32),
                pltpu.VMEM((nx, head_dim, rows), jnp.float32),
                pltpu.VMEM((nx, 2 * tokens, q_rows), half),
                pltpu.VMEM((2, nx, tokens, q_rows), half),
                pltpu.VMEM((tokens, width), jnp.float32),
                pltpu.SemaphoreType.DMA((1 + 7 * nx,)),
                pltpu.SemaphoreType.DMA((2,)),
                pltpu.SemaphoreType.DMA((2,)),
                pltpu.SemaphoreType.DMA((ny, nx)),
                pltpu.SemaphoreType.DMA,
                pltpu.SemaphoreType.DMA((nx,)),
                pltpu.SemaphoreType.DMA((2,)),
                pltpu.SemaphoreType.DMA((2, nx)),
            ],
            compiler_params=pltpu.CompilerParams(
                collective_id=0, has_side_effects=True, vmem_limit_bytes=54600 * 1024),
        )(x_loc[0], w_rows, w_out.reshape(heads * head_dim, width))
        return y[None]

    return jax.shard_map(local_layer, mesh=mesh, in_specs=(seq_spec, P(), P()), out_specs=seq_spec, check_vma=False)
```

```python
import functools
import math

import jax
import jax.numpy as jnp
from jax import lax
from jax.experimental import pallas as pl
from jax.experimental.pallas import tpu as pltpu
from jax.sharding import PartitionSpec as P

MESH = pl.DeviceIdType.MESH
LANES = 128
TILE = 256
NT = (((1,), (1,)), ((), ()))

STEPS = (
    (0, 0), (1, 0), (3, 0), (1, 1), (2, 3), (2, 0), (1, 3), (2, 1),
    (2, 2), (3, 2), (1, 2), (3, 3), (3, 1), (0, 3), (0, 1), (0, 2),
)
SLOTS = (("s", 0), ("a", 0), ("s", 1), ("a", 1), ("s", 2), ("a", 2))
END_SLOTS = (("s", 0), ("a", 0), ("a", 1), ("s", 1), ("a", 2), ("s", 2))
FAR_FIRST = (2, 1, 3, 0)
Q_ORDER = (1, 3, 2, 0)
O_ORDER = (2, 0, 3, 1)


def kernel(dims, x_hbm, wqkv_hbm, wout_hbm, y_ref,
           x_ext, w_kv, w_q, w_o, kv_all, kv_buf, q_all, q_t,
           v_t, s_buf, m_cur, r_cur, m_run, l_run, acc, o_send, o_all, y_acc,
           load_sem, x_sem, kv_send, kv_recv, q_send, q_recv,
           o_send_sem, o_recv):
    nx, ny, heads, kv_heads, head_dim = dims
    dev_tokens = x_hbm.shape[0]
    chip_tokens = 2 * dev_tokens
    row_keys = nx * chip_tokens
    kv_local = kv_heads // 2
    group = heads // kv_heads
    q_rows = group * head_dim
    feat = kv_local * q_rows
    rows = q_t.shape[2]
    tiles = rows // TILE
    main = LANES
    tail = chip_tokens - main
    cx, cy, core = lax.axis_index("cx"), lax.axis_index("cy"), lax.axis_index("core")
    other = 1 - core
    own_rows = pl.ds(pl.multiple_of(core * dev_tokens, 32), dev_tokens)
    other_rows = pl.ds(pl.multiple_of(other * dev_tokens, 32), dev_tokens)
    scale = head_dim ** -0.5 * math.log2(math.e)

    def head_at(dx):
        return lax.rem(cx + dx, nx)

    x_load = pltpu.make_async_copy(x_hbm, x_ext.at[own_rows], load_sem.at[0])
    x_load.start()
    kv_loads, q_loads = [], []
    for i, dx in enumerate(FAR_FIRST):
        for r in range(2):
            head = (core if r == 0 else other) * kv_local + head_at(dx)
            for part in range(2):
                src = pl.multiple_of((heads + part * kv_heads + head) * head_dim, head_dim)
                copy = pltpu.make_async_copy(
                    wqkv_hbm.at[pl.ds(src, head_dim)],
                    w_kv.at[pl.ds((4 * i + 2 * r + part) * head_dim, head_dim)],
                    load_sem.at[1 + 4 * i + 2 * r + part])
                copy.start()
                kv_loads.append(copy)
    for i, dx in enumerate(Q_ORDER):
        src = pl.multiple_of(core * feat + head_at(dx) * q_rows, q_rows)
        copy = pltpu.make_async_copy(
            wqkv_hbm.at[pl.ds(src, q_rows)], w_q.at[pl.ds(i * q_rows, q_rows)], load_sem.at[1 + 4 * nx + i])
        copy.start()
        q_loads.append(copy)

    east = {"cx": lax.rem(cx + 1, nx)}
    west = {"cx": lax.rem(cx + nx - 1, nx)}
    north = {"cy": lax.rem(cy + 1, ny)}
    south = {"cy": lax.rem(cy + ny - 1, ny)}
    partner = {"core": other}
    across = {"cx": head_at(2)}
    by_dx = {0: {}, 1: east, 2: across, 3: west}
    targets = [partner, north, south]
    for dx in range(1, nx):
        targets += [by_dx[dx], {**by_dx[dx], **partner}]
    barrier = pltpu.get_barrier_semaphore()
    for target in targets:
        pl.semaphore_signal(barrier, inc=1, device_id=target, device_id_type=MESH)
    pl.semaphore_wait(barrier, len(targets))

    def remote(src, dst, send_sem, recv_sem, target):
        return pltpu.make_async_remote_copy(
            src_ref=src, dst_ref=dst, send_sem=send_sem, recv_sem=recv_sem, device_id=target, device_id_type=MESH)

    x_load.wait()
    x_copy = remote(x_ext.at[own_rows], x_ext.at[own_rows], x_sem.at[0], x_sem.at[1], partner)
    x_copy.start()
    q_t[:, head_dim:, :] = jnp.zeros((nx, LANES - head_dim, rows), jnp.bfloat16)

    def kv_at(dx, dy):
        return dy * row_keys + dx * chip_tokens

    def kv_piece(dx, dy):
        return kv_buf.at[pl.ds(kv_at(dx, dy), chip_tokens)]

    def kv_half(dx, dy, r):
        return kv_buf.at[pl.ds(kv_at(dx, dy) + r * dev_tokens, dev_tokens)]

    def spread(src, dst_of, dx):
        remote(src, dst_of(3), kv_send.at[0], kv_recv.at[3, dx], north).start()
        remote(src, dst_of(1), kv_send.at[0], kv_recv.at[1, dx], south).start()

    for i in range(0, nx, 2):
        for copy in kv_loads[4 * i:4 * i + 8]:
            copy.wait()
        part = lax.dot_general(
            x_ext[own_rows], w_kv[4 * i * head_dim:(4 * i + 8) * head_dim], NT, preferred_element_type=jnp.float32)
        for k in range(4):
            kv_all[2 * i + k] = part[:, k * LANES:(k + 1) * LANES].astype(jnp.bfloat16)
        for k in range(4):
            dx, r = FAR_FIRST[i + k // 2], k % 2
            src = kv_all.at[2 * i + k]
            back = (nx - dx) % nx
            if dx:
                target = {**by_dx[dx], **partner} if r else by_dx[dx]
                remote(src, kv_half(back, 0, r), kv_send.at[0], kv_recv.at[0, back], target).start()
            elif r:
                remote(src, kv_half(0, 0, 1), kv_send.at[1], kv_recv.at[0, 0], partner).start()
            else:
                spread(src, lambda dy: kv_half(0, dy, 0), 0)
                kv_buf[kv_at(0, 0):kv_at(0, 0) + dev_tokens] = kv_all[2 * i + k]
    o_loads = []
    for i, dx in enumerate(O_ORDER):
        for r in range(2):
            src = ((core if r == 0 else other) * kv_local + head_at(dx)) * q_rows
            copy = pltpu.make_async_copy(
                wout_hbm.at[pl.ds(pl.multiple_of(src, q_rows), q_rows)],
                w_o.at[pl.ds((2 * i + r) * q_rows, q_rows)], load_sem.at[1 + 5 * nx + 2 * i + r])
            copy.start()
            o_loads.append(copy)

    x_copy.wait()
    x_ext[chip_tokens:chip_tokens + tail] = x_ext[main:chip_tokens]
    lane = lax.broadcasted_iota(jnp.int32, (head_dim, LANES), 1)
    for i in range(0, nx, 2):
        results = []
        for k in (i, i + 1):
            q_loads[k].wait()
        for k in (i, i + 1):
            results.append(lax.dot_general(
                w_q[k * q_rows:(k + 1) * q_rows], x_ext[...], NT, preferred_element_type=jnp.float32))
        for k, res in zip((i, i + 1), results):
            dst = q_all.at[Q_ORDER[k]] if Q_ORDER[k] else q_t.at[0, pl.ds(0, head_dim)]
            for g in range(group):
                dst[:, g * LANES:(g + 1) * LANES] = res[g * head_dim:(g + 1) * head_dim, :main].astype(jnp.bfloat16)
            for pair in range(group // 2):
                lo = res[2 * pair * head_dim:(2 * pair + 1) * head_dim, main:]
                hi = res[(2 * pair + 1) * head_dim:(2 * pair + 2) * head_dim, main:]
                dst[:, (group + pair) * LANES:(group + pair + 1) * LANES] = (
                    jnp.where(lane < tail, lo, hi).astype(jnp.bfloat16))
        for k in (i, i + 1):
            dx = Q_ORDER[k]
            if dx:
                remote(q_all.at[dx], q_t.at[nx - dx, pl.ds(0, head_dim)],
                       q_send, q_recv.at[nx - dx], by_dx[dx]).start()

    def arrive(ref, sem):
        remote(ref, ref, q_send, sem, partner).wait_recv()

    def kv_row(dx):
        if dx:
            arrive(kv_piece(dx, 0), kv_recv.at[0, dx])
            spread(kv_piece(dx, 0), lambda dy: kv_piece(dx, dy), dx)
        else:
            arrive(kv_half(0, 0, 1), kv_recv.at[0, 0])
            spread(kv_half(0, 0, 1), lambda dy: kv_half(0, dy, 1), 0)

    def kv_side(dx, dy):
        arrive(kv_piece(dx, dy), kv_recv.at[dy, dx])
        if dy == 3 and dx % 2 == 0:
            remote(kv_piece(dx, 3), kv_piece(dx, 2), kv_send.at[0], kv_recv.at[2, dx], north).start()
        if dy == 1 and dx % 2 == 1:
            remote(kv_piece(dx, 1), kv_piece(dx, 2), kv_send.at[0], kv_recv.at[2, dx], south).start()

    def q_arrive(dx):
        arrive(q_t.at[dx, pl.ds(0, head_dim)], q_recv.at[dx])

    def keys(dy):
        return kv_buf[kv_at(0, dy):kv_at(0, dy) + row_keys]

    def first_step(n):
        return all(step[0] != STEPS[n][0] for step in STEPS[:n])

    def score(n, q, dy, t):
        cols = slice(t * TILE, (t + 1) * TILE)
        scores = jnp.dot(keys(dy), q_t[q, :, cols], preferred_element_type=jnp.float32)
        new_max = jnp.max(scores, axis=0, keepdims=True)
        if not first_step(n):
            old_max = m_run[q, :, cols]
            new_max = jnp.maximum(old_max, new_max)
            r_cur[n % 2, :, cols] = jnp.exp2((old_max - new_max) * scale)
        m_run[q, :, cols] = new_max
        m_cur[n % 2, :, cols] = new_max
        s_buf[n % 2, t] = scores

    def absorb(n, q, dy, t):
        cols = slice(t * TILE, (t + 1) * TILE)
        weights = jnp.exp2((s_buf[n % 2, t] - m_cur[n % 2, :, cols]) * scale)
        sums = jnp.sum(weights, axis=0, keepdims=True)
        out = jnp.dot(v_t[dy], weights.astype(jnp.bfloat16), preferred_element_type=jnp.float32)
        if not first_step(n):
            rescale = r_cur[n % 2, :, cols]
            sums = l_run[q, :, cols] * rescale + sums
            out = acc[q, :, cols] * rescale + out
        l_run[q, :, cols] = sums
        acc[q, :, cols] = out

    def finish(q):
        out = acc[q] / l_run[q]
        dst = o_send.at[q]
        for pair in range(group // 2):
            cols = slice(pair * LANES, (pair + 1) * LANES)
            first = 2 * pair * LANES
            both = jnp.concatenate([out[:, first:first + LANES], out[:, first + LANES:first + 2 * LANES]], axis=0)
            dst[:main, cols] = jnp.transpose(both, (1, 0)).astype(jnp.bfloat16)
            ends = out[:, (group + pair) * LANES:(group + pair + 1) * LANES]
            both = jnp.concatenate([ends, pltpu.roll(ends, tail, 1)], axis=0)
            dst[main:, cols] = jnp.transpose(both, (1, 0))[:tail].astype(jnp.bfloat16)
        mine, theirs = o_send.at[q, own_rows], o_send.at[q, other_rows]
        if q:
            target = by_dx[q]
            remote(mine, o_all.at[0, nx - q], o_send_sem.at[0], o_recv.at[0, nx - q], target).start()
            remote(theirs, o_all.at[1, nx - q], o_send_sem.at[0], o_recv.at[1, nx - q], {**target, **partner}).start()
        else:
            remote(theirs, o_all.at[1, 0], o_send_sem.at[1], o_recv.at[1, 0], partner).start()
            o_all[0, 0] = o_send[0, own_rows]

    events = {n: [] for n in range(len(STEPS) + 1)}
    def row(*dxs):
        return [functools.partial(kv_row, dx) for dx in dxs]

    def side(*pieces):
        return [functools.partial(kv_side, dx, dy) for dx, dy in pieces]

    def query(dx):
        return [functools.partial(q_arrive, dx)]

    events[0] = row(0, 2, 1, 3)
    events[1] = side((0, 1)) + query(1)
    events[2] = side((2, 3)) + query(3)
    events[3] = side((1, 1), (2, 1), (0, 3), (3, 1))
    events[4] = side((3, 3), (1, 3)) + query(2)
    events[8] = side((0, 2), (1, 2), (2, 2), (3, 2))
    last_of = {q: max(n for n, s in enumerate(STEPS) if s[0] == q) for q in range(nx)}
    first_of = {dy: min(n for n, s in enumerate(STEPS) if s[1] == dy) for dy in range(ny)}

    for n in range(len(STEPS) + 1):
        for event in events[n]:
            event()
        if n < len(STEPS) and first_of[STEPS[n][1]] == n:
            dy = STEPS[n][1]
            v_t[dy] = jnp.transpose(keys(dy).astype(jnp.float32), (1, 0))[head_dim:].astype(jnp.bfloat16)
        ends = n and last_of[STEPS[n - 1][0]] == n - 1
        for work, t in (END_SLOTS if ends else SLOTS):
            if work == "s" and n < len(STEPS):
                score(n, *STEPS[n], t)
            if work == "a" and n:
                absorb(n - 1, *STEPS[n - 1], t)
        if ends:
            finish(STEPS[n - 1][0])

    for copy in o_loads:
        copy.wait()
    for i, dx in enumerate(O_ORDER):
        if i == nx - 1:
            for ref, sem in ((kv_buf.at[pl.ds(0, (nx * ny - 1) * chip_tokens)], kv_send.at[0]), (kv_all.at[0], kv_send.at[1]), (q_all.at[pl.ds(0, nx - 1)], q_send), (o_all.at[:, pl.ds(0, nx - 1)], o_send_sem.at[0]), (o_all.at[1, 0], o_send_sem.at[1])):
                remote(ref, ref, sem, x_sem.at[1], partner).wait_send()
        for r in range(2):
            if dx or r:
                arrive(o_all.at[r, dx], o_recv.at[r, dx])
        total = jnp.dot(
            jnp.concatenate([o_all[0, dx], o_all[1, dx]], axis=1), w_o[2 * i * q_rows:(2 * i + 2) * q_rows],
            preferred_element_type=jnp.float32)
        if i == 0:
            y_acc[...] = total
        elif i < nx - 1:
            y_acc[...] += total
        else:
            y_ref[...] = (y_acc[...] + total).astype(jnp.bfloat16)


def solution(mesh):
    nx, ny = mesh.shape["cx"], mesh.shape["cy"]
    seq_spec = P("dp", ("cy", "cx", "core"))

    def local_layer(x_loc, w_qkv, w_out):
        heads, head_dim, width = w_out.shape
        kv_heads = (w_qkv.shape[1] - heads) // 2
        tokens = x_loc.shape[1]
        kv_local = kv_heads // 2
        group = heads // kv_heads
        q_rows = group * head_dim
        feat = kv_local * q_rows
        rows = group * 2 * tokens
        dims = (nx, ny, heads, kv_heads, head_dim)
        w_rows = jnp.transpose(w_qkv, (1, 2, 0)).reshape(-1, width)
        hbm = pl.BlockSpec(memory_space=pl.ANY)
        half = jnp.bfloat16
        y = pl.pallas_call(
            functools.partial(kernel, dims),
            out_shape=jax.ShapeDtypeStruct((tokens, width), half),
            in_specs=[hbm] * 3,
            out_specs=pl.BlockSpec(memory_space=pltpu.VMEM),
            scratch_shapes=[
                pltpu.VMEM((TILE, width), half),
                pltpu.VMEM((2 * kv_heads * head_dim, width), half),
                pltpu.VMEM((feat, width), half),
                pltpu.VMEM((heads * head_dim, width), half),
                pltpu.VMEM((kv_heads, tokens, LANES), half),
                pltpu.VMEM((ny * nx * 2 * tokens, LANES), half),
                pltpu.VMEM((nx, head_dim, rows), half),
                pltpu.VMEM((nx, LANES, rows), half),
                pltpu.VMEM((ny, head_dim, nx * 2 * tokens), half),
                pltpu.VMEM((2, rows // TILE, nx * 2 * tokens, TILE), jnp.float32),
                pltpu.VMEM((2, 1, rows), jnp.float32),
                pltpu.VMEM((2, 1, rows), jnp.float32),
                pltpu.VMEM((nx, 1, rows), jnp.float32),
                pltpu.VMEM((nx, 1, rows), jnp.float32),
                pltpu.VMEM((nx, head_dim, rows), jnp.float32),
                pltpu.VMEM((nx, 2 * tokens, q_rows), half),
                pltpu.VMEM((2, nx, tokens, q_rows), half),
                pltpu.VMEM((tokens, width), jnp.float32),
                pltpu.SemaphoreType.DMA((1 + 7 * nx,)),
                pltpu.SemaphoreType.DMA((2,)),
                pltpu.SemaphoreType.DMA((2,)),
                pltpu.SemaphoreType.DMA((ny, nx)),
                pltpu.SemaphoreType.DMA,
                pltpu.SemaphoreType.DMA((nx,)),
                pltpu.SemaphoreType.DMA((2,)),
                pltpu.SemaphoreType.DMA((2, nx)),
            ],
            compiler_params=pltpu.CompilerParams(
                collective_id=0, has_side_effects=True, vmem_limit_bytes=54600 * 1024),
        )(x_loc[0], w_rows, w_out.reshape(heads * head_dim, width))
        return y[None]

    return jax.shard_map(local_layer, mesh=mesh, in_specs=(seq_spec, P(), P()), out_specs=seq_spec, check_vma=False)
```
